32 devices in a mesh: dp: 16 (over z, y, x), tensor: 2 (over core).
Axes of the slice: x: 2, y: 2, z: 4, core: 2. Of those that a mesh axis runs over, the one named last changes fastest.
Arguments:
- hidden_in: bfloat16 [16384, 1536], P(('dp', 'tensor')), may hold values from -6 to 6
- query_weight: bfloat16 [1536, 1536], P('dp', 'tensor'), may hold values from -0.15625 to 0.15625
- key_matrix: bfloat16 [1536, 768], P('dp', 'tensor'), may hold values from -0.15625 to 0.15625
- value_matrix: bfloat16 [1536, 768], P('dp', 'tensor'), may hold values from -0.15625 to 0.15625
- out_weight: bfloat16 [1536, 1536], P('tensor', 'dp'), may hold values from -1.25 to 1.25
- gate_weight: bfloat16 [1536, 4096], P('dp', 'tensor'), may hold values from -0.15625 to 0.15625
- up_weight: bfloat16 [1536, 4096], P('dp', 'tensor'), may hold values from -0.15625 to 0.15625
- down_weight: bfloat16 [4096, 1536], P('tensor', 'dp'), may hold values from -0.09375 to 0.09375
- attention_gain: bfloat16 [1536], P('dp'), may hold values from 0.099609375 to 1.8984375
- feedforward_gain: bfloat16 [1536], P('dp'), may hold values from 0.099609375 to 1.8984375
- cotangent: bfloat16 [16384, 1536], P(('dp', 'tensor')), may hold values from -6 to 6
Outputs:
- hidden_out: bfloat16 [16384, 1536], P(('dp', 'tensor'))
- grad_in: float32 [16384, 1536], P(('dp', 'tensor'))
- grad_query: float32 [1536, 1536], P('dp', 'tensor')
- grad_key: float32 [1536, 768], P('dp', 'tensor')
- grad_value: float32 [1536, 768], P('dp', 'tensor')
- grad_out: float32 [1536, 1536], P('tensor', 'dp')
- grad_gate: float32 [1536, 4096], P('dp', 'tensor')
- grad_up: float32 [1536, 4096], P('dp', 'tensor')
- grad_down: float32 [4096, 1536], P('tensor', 'dp')
- grad_attention_gain: float32 [1536], P('dp')
- grad_feedforward_gain: float32 [1536], P('dp')
The draws below stay inside these ranges and needn't reach their ends.
All inputs are finite; a program needn't handle non-finite values.
Results may differ from the reference program's by a relative error of at most 0.015.
Values may be sent and summed in bfloat16 or wider, within the bound.
A program may use at most 256 MiB of HBM per device.

```python
import math
import jax
import jax.numpy as jnp
from jax import lax

MODEL_WIDTH = 1536
QUERY_HEADS = 16
KEY_VALUE_HEADS = 8
HEAD_SIZE = 96
HIDDEN_UNITS = 4096
SEQUENCE_LENGTH = 512
TOKENS = 16384


def strengthened(array, rng, source, target, parts, factor):
    def block_of(dim):
        return (jnp.arange(array.shape[dim]) // (array.shape[dim] // parts)).reshape((-1,) + (1,) * (array.ndim - 1 - dim))

    one_side = jax.random.permutation(rng, parts)[block_of(target)]
    second = (block_of(target) + parts // 2) % parts
    return jnp.where((block_of(source) == one_side) | (block_of(source) == second), factor * array, array)


def shard_levels(own_key, shape, split, smallest, largest):
    loudness, own = 1.0, jax.random.fold_in(own_key, 6)
    for axis_at, shards_of in split:
        draws = jnp.exp(jax.random.uniform(jax.random.fold_in(own, axis_at), (shards_of,), jnp.float32, smallest / len(split), largest / len(split)))
        loudness = loudness * jnp.repeat(draws, shape[axis_at] // shards_of).reshape([-1 if axis == axis_at else 1 for axis in range(len(shape))])
    return loudness


def centred(own_key, dims, scale, reach, split=(), held_as=jnp.bfloat16):
    values = scale * jax.random.normal(own_key, dims, jnp.float32)
    if split:
        values = values * shard_levels(own_key, dims, split, -0.22, 0.18)
    return jnp.clip(values, -reach, reach).astype(held_as)


def gaussian_with(own_key, shape, scale, reach, cuts, heavy, held_as=jnp.bfloat16):
    result = scale * jax.random.normal(own_key, shape, jnp.float32)
    if cuts:
        result = result * shard_levels(own_key, shape, cuts, -0.22, 0.18)
    return jnp.clip(strengthened(result, jax.random.fold_in(own_key, 3), *heavy), -reach, reach).astype(held_as)


def setup_inputs(seed: int = 0) -> dict:
    key_list = jax.random.split(jax.random.key(seed), 12)
    hidden_in = centred(key_list[0], (TOKENS, MODEL_WIDTH), 1.0, 6.0, ((0, 32),))
    query_weight = centred(key_list[1], (MODEL_WIDTH, QUERY_HEADS * HEAD_SIZE), MODEL_WIDTH ** -0.5, 0.15625, ((0, 16), (1, 2)))
    key_matrix = centred(key_list[2], (MODEL_WIDTH, KEY_VALUE_HEADS * HEAD_SIZE), MODEL_WIDTH ** -0.5, 0.15625, ((0, 16), (1, 2)))
    value_matrix = centred(key_list[3], (MODEL_WIDTH, KEY_VALUE_HEADS * HEAD_SIZE), MODEL_WIDTH ** -0.5, 0.15625, ((0, 16), (1, 2)))
    out_weight = centred(key_list[4], (QUERY_HEADS * HEAD_SIZE, MODEL_WIDTH), (max(QUERY_HEADS * HEAD_SIZE // 64, 1)) ** -0.5, 1.25, ((0, 2), (1, 16)))
    gate_weight = centred(key_list[5], (MODEL_WIDTH, HIDDEN_UNITS), MODEL_WIDTH ** -0.5, 0.15625, ((0, 16), (1, 2)))
    up_weight = centred(key_list[6], (MODEL_WIDTH, HIDDEN_UNITS), MODEL_WIDTH ** -0.5, 0.15625, ((0, 16), (1, 2)))
    down_weight = centred(key_list[7], (HIDDEN_UNITS, MODEL_WIDTH), HIDDEN_UNITS ** -0.5, 0.09375, ((0, 2), (1, 16)))
    attention_gain = jnp.clip(1.0 + 0.18 * jax.random.normal(key_list[8], (MODEL_WIDTH,), jnp.float32), 0.099609375, 1.8984375).astype(jnp.bfloat16)
    feedforward_gain = jnp.clip(1.0 + 0.18 * jax.random.normal(key_list[9], (MODEL_WIDTH,), jnp.float32), 0.099609375, 1.8984375).astype(jnp.bfloat16)
    cotangent = gaussian_with(key_list[10], (TOKENS, MODEL_WIDTH), 1.0, 6.0, ((0, 32),), (0, 1, 32, 2.75))
    return dict(hidden_in=hidden_in, query_weight=query_weight, key_matrix=key_matrix, value_matrix=value_matrix, out_weight=out_weight, gate_weight=gate_weight, up_weight=up_weight, down_weight=down_weight, attention_gain=attention_gain, feedforward_gain=feedforward_gain, cotangent=cotangent)


EPSILON = 1e-05
THETA_BASE = 100000.0

def to_brain_float(tensor):
    return lax.optimization_barrier(tensor.astype(jnp.bfloat16))

def rope_tables(length, width):
    half_width = width // 2
    inverse = THETA_BASE ** (-(jnp.arange(half_width, dtype=jnp.float32) * 2.0 / width))
    position = jnp.arange(length, dtype=jnp.float32)
    angles = position[:, None] * inverse[None, :]
    return (jnp.cos(angles), jnp.sin(angles))

def apply_rotary(tensor, cosine_table, sine_table, direction):
    half_width = tensor.shape[-1] // 2
    first_half = tensor[..., :half_width]
    second_half = tensor[..., half_width:]
    cos_part = cosine_table[:, None, :]
    sin_part = direction * sine_table[:, None, :]
    return jnp.concatenate([first_half * cos_part - second_half * sin_part, second_half * cos_part + first_half * sin_part], axis=-1)

def causal_scores(query, keys):
    length = query.shape[0]
    score_scale = 1.0 / math.sqrt(query.shape[-1])
    scores = jnp.einsum('qkgd,tkd->kgqt', query.astype(jnp.float32), keys.astype(jnp.float32)) * score_scale
    earlier = jnp.arange(length)[:, None] >= jnp.arange(length)[None, :]
    return jnp.where(earlier, scores, -jnp.inf)

def attend(bundle):
    query, keys, values = bundle
    scores = causal_scores(query, keys)
    log_total = jnp.log(lax.optimization_barrier(jnp.sum(jnp.exp(scores), axis=-1)))
    soft_weights = to_brain_float(jnp.exp(scores - log_total[..., None]))
    mixture_output = to_brain_float(jnp.einsum('kgqt,tkd->qkgd', soft_weights.astype(jnp.float32), values.astype(jnp.float32)))
    return (mixture_output, log_total)

def attend_back(bundle):
    query, keys, values, mixture_gradient, row_products, log_total = bundle
    score_scale = 1.0 / math.sqrt(query.shape[-1])
    chances = jnp.exp(causal_scores(query, keys) - log_total[..., None])
    soft_weights = to_brain_float(chances).astype(jnp.float32)
    grad_wide = mixture_gradient.astype(jnp.float32)
    value_gradient = jnp.einsum('kgqt,qkgd->tkd', soft_weights, grad_wide)
    grad_weights = jnp.einsum('qkgd,tkd->kgqt', grad_wide, values.astype(jnp.float32))
    grad_scores = to_brain_float(chances * (grad_weights - row_products[..., None])).astype(jnp.float32)
    grad_query = jnp.einsum('kgqt,tkd->qkgd', grad_scores, keys.astype(jnp.float32)) * score_scale
    grad_keys = jnp.einsum('kgqt,qkgd->tkd', grad_scores, query.astype(jnp.float32)) * score_scale
    return (grad_query, grad_keys, value_gradient)

def matrix_multiply(left, right):
    return jnp.dot(left, right, preferred_element_type=jnp.float32)

def norm_back(grad_normed, unit_rows, inverse_rms, gain):
    scaled = grad_normed * gain
    inner = lax.optimization_barrier(jnp.mean(scaled * unit_rows, axis=1, keepdims=True))
    return (inverse_rms * (scaled - unit_rows * inner), lax.optimization_barrier(jnp.sum(grad_normed * unit_rows, axis=0)))

def reference(hidden_in, query_weight, key_matrix, value_matrix, out_weight, gate_weight, up_weight, down_weight, attention_gain, feedforward_gain, cotangent):
    heads_per_group = QUERY_HEADS // KEY_VALUE_HEADS
    cosine_table, sine_table = rope_tables(SEQUENCE_LENGTH, HEAD_SIZE)
    gain_first = attention_gain.astype(jnp.float32)
    gain_second = feedforward_gain.astype(jnp.float32)
    seq_total = TOKENS // SEQUENCE_LENGTH
    sequence_block = math.gcd(seq_total, 8)
    rows_per_block = sequence_block * SEQUENCE_LENGTH
    block_count = TOKENS // rows_per_block

    def one_block(carried, pair):
        input_block, cot_block = pair
        input_rows = input_block.astype(jnp.float32)
        inverse_one = lax.rsqrt(lax.optimization_barrier(jnp.mean(input_rows * input_rows, axis=1, keepdims=True)) + EPSILON)
        unit_one = input_rows * inverse_one
        first_normalized = to_brain_float(unit_one * gain_first)
        query_rows = apply_rotary(matrix_multiply(first_normalized, query_weight).reshape(sequence_block, SEQUENCE_LENGTH, QUERY_HEADS, HEAD_SIZE), cosine_table, sine_table, 1.0)
        query_rows = to_brain_float(query_rows).reshape(sequence_block, SEQUENCE_LENGTH, KEY_VALUE_HEADS, heads_per_group, HEAD_SIZE)
        every_key = to_brain_float(apply_rotary(matrix_multiply(first_normalized, key_matrix).reshape(sequence_block, SEQUENCE_LENGTH, KEY_VALUE_HEADS, HEAD_SIZE), cosine_table, sine_table, 1.0))
        every_value = to_brain_float(matrix_multiply(first_normalized, value_matrix)).reshape(sequence_block, SEQUENCE_LENGTH, KEY_VALUE_HEADS, HEAD_SIZE)
        mixture_output, log_totals = lax.map(attend, (query_rows, every_key, every_value))
        mixed_flat = mixture_output.reshape(rows_per_block, QUERY_HEADS * HEAD_SIZE)
        middle = input_rows + matrix_multiply(mixed_flat, out_weight)
        inverse_two = lax.rsqrt(lax.optimization_barrier(jnp.mean(middle * middle, axis=1, keepdims=True)) + EPSILON)
        unit_two = middle * inverse_two
        normed_two = to_brain_float(unit_two * gain_second)
        gate = matrix_multiply(normed_two, gate_weight)
        upward = matrix_multiply(normed_two, up_weight)
        sigma = jax.nn.sigmoid(gate)
        hidden = to_brain_float(gate * sigma * upward)
        out_block = (middle + matrix_multiply(hidden, down_weight)).astype(jnp.bfloat16)
        grad_down = matrix_multiply(hidden.T, cot_block)
        grad_hidden = matrix_multiply(cot_block, down_weight.T)
        grad_up_act = to_brain_float(grad_hidden * gate * sigma)
        grad_gate_act = to_brain_float(grad_hidden * upward * sigma * (1.0 + gate * (1.0 - sigma)))
        grad_gate = matrix_multiply(normed_two.T, grad_gate_act)
        grad_up = matrix_multiply(normed_two.T, grad_up_act)
        grad_normed_two = matrix_multiply(grad_gate_act, gate_weight.T) + matrix_multiply(grad_up_act, up_weight.T)
        middle_part, grad_second = norm_back(grad_normed_two, unit_two, inverse_two, gain_second)
        grad_middle = cot_block.astype(jnp.float32) + middle_part
        grad_middle_round = to_brain_float(grad_middle)
        grad_out = matrix_multiply(mixed_flat.T, grad_middle_round)
        mixture_gradient = matrix_multiply(grad_middle_round, out_weight.T)
        rounded_mixture_gradient = to_brain_float(mixture_gradient).reshape(sequence_block, SEQUENCE_LENGTH, KEY_VALUE_HEADS, heads_per_group, HEAD_SIZE)
        row_products = lax.optimization_barrier(jnp.sum(mixture_gradient.reshape(sequence_block, SEQUENCE_LENGTH, KEY_VALUE_HEADS, heads_per_group, HEAD_SIZE) * mixture_output.astype(jnp.float32), axis=-1))
        row_products = jnp.transpose(row_products, (0, 2, 3, 1))
        grad_queries_rot, rotated_key_gradient, value_gradient = lax.map(attend_back, (query_rows, every_key, every_value, rounded_mixture_gradient, row_products, log_totals))
        grad_queries_act = to_brain_float(apply_rotary(grad_queries_rot.reshape(sequence_block, SEQUENCE_LENGTH, QUERY_HEADS, HEAD_SIZE), cosine_table, sine_table, -1.0)).reshape(rows_per_block, QUERY_HEADS * HEAD_SIZE)
        key_activation_gradient = to_brain_float(apply_rotary(rotated_key_gradient, cosine_table, sine_table, -1.0)).reshape(rows_per_block, KEY_VALUE_HEADS * HEAD_SIZE)
        value_activation_gradient = to_brain_float(value_gradient).reshape(rows_per_block, KEY_VALUE_HEADS * HEAD_SIZE)
        grad_query = matrix_multiply(first_normalized.T, grad_queries_act)
        grad_key = matrix_multiply(first_normalized.T, key_activation_gradient)
        grad_value = matrix_multiply(first_normalized.T, value_activation_gradient)
        grad_normed_one = matrix_multiply(grad_queries_act, query_weight.T) + matrix_multiply(key_activation_gradient, key_matrix.T) + matrix_multiply(value_activation_gradient, value_matrix.T)
        first_part, grad_first = norm_back(grad_normed_one, unit_one, inverse_one, gain_first)
        grad_block = grad_middle + first_part
        fresh = (grad_query, grad_key, grad_value, grad_out, grad_gate, grad_up, grad_down, grad_first, grad_second)
        updated = tuple((older + newer for older, newer in zip(carried, fresh)))
        return (updated, (out_block, grad_block))
    start_offset = (jnp.zeros((MODEL_WIDTH, QUERY_HEADS * HEAD_SIZE), jnp.float32), jnp.zeros((MODEL_WIDTH, KEY_VALUE_HEADS * HEAD_SIZE), jnp.float32), jnp.zeros((MODEL_WIDTH, KEY_VALUE_HEADS * HEAD_SIZE), jnp.float32), jnp.zeros((QUERY_HEADS * HEAD_SIZE, MODEL_WIDTH), jnp.float32), jnp.zeros((MODEL_WIDTH, HIDDEN_UNITS), jnp.float32), jnp.zeros((MODEL_WIDTH, HIDDEN_UNITS), jnp.float32), jnp.zeros((HIDDEN_UNITS, MODEL_WIDTH), jnp.float32), jnp.zeros((MODEL_WIDTH,), jnp.float32), jnp.zeros((MODEL_WIDTH,), jnp.float32))
    totals, (out_blocks, grad_blocks) = lax.scan(one_block, start_offset, (hidden_in.reshape(block_count, rows_per_block, MODEL_WIDTH), cotangent.reshape(block_count, rows_per_block, MODEL_WIDTH)))
    return (out_blocks.reshape(TOKENS, MODEL_WIDTH), grad_blocks.reshape(TOKENS, MODEL_WIDTH), totals[0], totals[1], totals[2], totals[3], totals[4], totals[5], totals[6], totals[7], totals[8])
```

```python
import functools
import math

import jax
import jax.numpy as jnp
from jax import lax
from jax.experimental import pallas as pl
from jax.experimental.pallas import tpu as pltpu
from jax.sharding import PartitionSpec as P

QUERY_HEADS = 16
KEY_VALUE_HEADS = 8
HEAD_SIZE = 96
SEQUENCE_LENGTH = 512

EPSILON = 1e-05
THETA_BASE = 100000.0
MESH = pl.DeviceIdType.MESH


def place():
    d = lax.axis_index("dp")
    return lax.div(d, 4), lax.rem(lax.div(d, 2), 2), lax.rem(d, 2), lax.axis_index("tensor")

def dev(z, y, x, c):
    return (z * 4 + y * 2 + x, c)

def enter(line, pos):
    z, y, x, c = pos
    barrier = pltpu.get_barrier_semaphore()
    def greet(who):
        pl.semaphore_signal(barrier, inc=1, device_id=who, device_id_type=MESH)
    greet(dev(z, y, x, 1 - c)); greet(dev(z, y, 1 - x, c)); greet(dev(z, 1 - y, x, c))
    @pl.when(z > 0)
    def _(): greet(dev(z - 1, y, x, c))
    @pl.when(z < line - 1)
    def _(): greet(dev(z + 1, y, x, c))
    pl.semaphore_wait(barrier, 3 + (z > 0).astype(jnp.int32) + (z < line - 1).astype(jnp.int32))

class Gather:
    def __init__(self, line, pos, shards, fulls, chunks, send, recv, local):
        self.line, self.pos, self.shards, self.fulls, self.chunks = line, pos, shards, fulls, chunks
        self.send, self.recv, self.local = send, recv, local
        self.steps = line + 3
    def region(self, t, have, z=None):
        w, off, width, _ = self.chunks[t]
        pz, py, px, c = self.pos
        full = self.fulls[w]
        half = full.shape[-1] // 2
        cols = pl.ds(pl.multiple_of(c * half + off, 128), width)
        every = slice(None)
        zi = z if z is not None else (every if "z" in have else pz)
        return full.at[zi, every if "y" in have else py, every if "x" in have else px, :, cols]
    def own(self, t):
        w, off, width, _ = self.chunks[t]
        return self.shards[w].at[:, pl.ds(off, width)]
    def local_copy(self, t):
        return pltpu.make_async_copy(self.own(t), self.region(t, ""), self.local.at[t])
    def copy(self, t, slot, src, dst, who):
        return pltpu.make_async_remote_copy(src_ref=src, dst_ref=dst, send_sem=self.send.at[t, slot], recv_sem=self.recv.at[t, slot], device_id=who, device_id_type=MESH)
    def swap(self, t, axis, have):
        z, y, x, c = self.pos
        who = {"y": dev(z, 1 - y, x, c), "x": dev(z, y, 1 - x, c), "c": dev(z, y, x, 1 - c)}[axis]
        slot = 2 * (self.line - 1) + "yxc".index(axis)
        mine = self.region(t, have) if have else self.own(t)
        land = self.region(t, have)
        if axis == "y":
            w, off, width, _ = self.chunks[t]
        return self.copy(t, slot, mine, land, who)
    def hop(self, t, h, up, have, act):
        z, y, x, c = self.pos
        slot = (h - 1) * 2 + up
        if up:
            block, who, there, here = z - (h - 1), dev(z + 1, y, x, c), (z + 1 < self.line) & (z >= h - 1), z >= h
            incoming = z - h
        else:
            block, who, there, here = z + (h - 1), dev(z - 1, y, x, c), (z > 0) & (z + h - 1 < self.line), z + h < self.line
            incoming = z + h
        if act == "recv":
            @pl.when(here)
            def _():
                r = self.region(t, have, incoming)
                self.copy(t, slot, r, r, dev(z, y, x, 1 - c)).wait_recv()
        else:
            @pl.when(there)
            def _():
                r = self.region(t, have, block)
                src = self.own(t) if (h == 1 and not have) else r
                cp = self.copy(t, slot, src, r, who)
                if act == "start": cp.start()
                else: cp.wait_send()
    def plan(self, t):
        order, out, have = self.chunks[t][3], [], ""
        acts = []
        for axis in order:
            if axis == "z":
                for h in range(1, self.line): acts.append(("z", h, have))
            else: acts.append((axis, 0, have))
            have += axis
        acts.append(("c", 0, have))
        return acts
    def act(self, t, a, what):
        axis, h, have = a
        if axis == "z":
            for up in (1, 0): self.hop(t, h, up, have, what)
        else:
            cp = self.swap(t, axis, have)
            {"start": cp.start, "recv": cp.wait_recv, "sent": cp.wait_send}[what]()
    def step(self, t, s):
        acts = self.plan(t)
        if s > 0: self.act(t, acts[s - 1], "recv")
        if s == 1: self.local_copy(t).wait()
        if s < len(acts): self.act(t, acts[s], "start")
    def finish(self, t):
        for a in self.plan(t): self.act(t, a, "sent")

def gather_body(line, chunks, n, *refs):
    shards, fulls, (send, recv, local) = refs[:n], refs[n:2 * n], refs[2 * n:]
    pos = place()
    g = Gather(line, pos, shards, fulls, chunks, send, recv, local)
    for t in range(len(chunks)): g.local_copy(t).start()
    enter(line, pos)
    for p in range(len(chunks) + g.steps - 1):
        for s in range(g.steps):
            if 0 <= p - s < len(chunks): g.step(p - s, s)
    for t in range(len(chunks)): g.finish(t)

def gather(line, chunks, shards, cid):
    n = len(shards)
    slots = 2 * (line - 1) + 3
    return pl.pallas_call(
        functools.partial(gather_body, line, chunks, n),
        out_shape=[jax.ShapeDtypeStruct((line, 2, 2, s.shape[0], 2 * s.shape[1]), s.dtype) for s in shards],
        in_specs=[pl.BlockSpec(memory_space=pltpu.VMEM)] * n,
        out_specs=[pl.BlockSpec(memory_space=pl.ANY)] * n,
        scratch_shapes=[pltpu.SemaphoreType.DMA((len(chunks), slots)), pltpu.SemaphoreType.DMA((len(chunks), slots)), pltpu.SemaphoreType.DMA((len(chunks),))],
        compiler_params=pltpu.CompilerParams(collective_id=cid, has_side_effects=True),
        name="weight_gather",
    )(*shards)


class Scatter:
    def __init__(self, line, pos, grads, outs, chunks, bufs, send, recv, load):
        self.line, self.pos, self.grads, self.outs, self.chunks, self.bufs = line, pos, grads, outs, chunks, bufs
        self.send, self.recv, self.load = send, recv, load
    def copy(self, t, slot, src, dst, who):
        return pltpu.make_async_remote_copy(src_ref=src, dst_ref=dst, send_sem=self.send.at[t, slot], recv_sem=self.recv.at[t, slot], device_id=who, device_id_type=MESH)
    def pick(self, ref, dims, **at):
        return ref.at[tuple(at.get(d, slice(None)) for d in dims)]
    def source(self, t):
        w, off, width, _ = self.chunks[t]
        return self.grads[w].at[:, :, :, :, pl.ds(off, width)]
    def merge(self, dst, a, b, dims):
        def go(lead, rest):
            if not rest:
                dst[lead] = a[lead] + b[lead]
            elif rest[0] == "z":
                @pl.loop(0, self.line)
                def _(i): go(lead + (i,), rest[1:])
            else:
                for i in range(2): go(lead + (i,), rest[1:])
        go((), dims)
    def final(self, t, *parts):
        w, off, width, _ = self.chunks[t]
        total = parts[0].astype(jnp.float32)
        for p in parts[1:]: total = total + p.astype(jnp.float32)
        self.outs[w][:, pl.ds(off, width)] = total
    def steps(self, t):
        z, y, x, c = self.pos
        order = self.chunks[t][3]
        buf = self.bufs[t]
        todo, dims, cur, first, used = [], "zyx", self.source(t), True, 0
        pending = []
        line = self.line
        for n, axis in enumerate(order):
            last = n == 2
            rest = dims.replace(axis, "")
            if axis in "xy":
                me = {"x": x, "y": y}[axis]
                who = {"x": dev(z, y, 1 - x, c), "y": dev(z, 1 - y, x, c)}[axis]
                slot = 2 * (line - 1) + "yx".index(axis)
                land = buf[axis]
                give = self.pick(cur, dims, **{axis: 1 - me})
                keep = self.pick(cur, dims, **{axis: me})
                cp = self.copy(t, slot, give, land, who)
                if first:
                    ld = pltpu.make_async_copy(keep, buf["own"], self.load.at[t])
                    def begin(cp=cp, ld=ld): cp.start(); ld.start()
                    todo.append(begin)
                    have = buf["own"]
                else:
                    ld = None
                    have = keep
                    self_begin = cp.start
                    prev = todo.pop()
                    todo.append(lambda prev=prev, b=self_begin: (prev(), b()))
                def end(cp=cp, ld=ld, have=have, land=land, rest=rest, last=last):
                    if ld is not None: ld.wait()
                    cp.wait_recv()
                    if last: self.final(t, land[...], have[...])
                    else: self.merge(land, land, have, rest)
                todo.append(end)
                cur = land
                pending.append(cp.wait_send)
            else:
                up, dn = buf["up"], buf["dn"]
                if first:
                    ld = pltpu.make_async_copy(cur, buf["own"], self.load.at[t])
                    todo.append(ld.start)
                    cur = buf["own"]
                else: ld = None
                for j in range(line - 1):
                    def hop(j=j, cur=cur, ld=ld, rest=rest):
                        if j == 0 and ld is not None: ld.wait()
                        for way, ref, target, src_z, edge in ((0, up, line - 1 - j, z - 1, z == 0), (1, dn, j, z + 1, z == line - 1)):
                            slot = 2 * j + way
                            nxt = dev(z + 1, y, x, c) if way == 0 else dev(z - 1, y, x, c)
                            passes = (target > z) if way == 0 else (target < z)
                            @pl.when(passes & edge)
                            def _(): self.copy(t, slot, cur.at[target], ref.at[j], nxt).start()
                            @pl.when(passes & ~edge)
                            def _():
                                cp = self.copy(t, slot, ref.at[j], ref.at[j], nxt)
                                cp.wait_recv()
                                self.merge(ref.at[j], ref.at[j], cur.at[target], rest)
                                cp.start()
                    todo.append(hop)
                    for way in (0, 1):
                        def drain(j=j, way=way, cur=cur):
                            target = line - 1 - j if way == 0 else j
                            passes = (target > z) if way == 0 else (target < z)
                            @pl.when(passes)
                            def _(): self.copy(t, 2 * j + way, cur.at[target], (up if way == 0 else dn).at[j], dev(z, y, x, 1 - c)).wait_send()
                        pending.append(drain)
                def close(cur=cur, rest=rest, last=last):
                    ku, kd = line - 1 - z, z
                    def arrived(way, k):
                        ref = up if way == 0 else dn
                        self.copy(t, 2 * k + way, ref.at[k], ref.at[k], dev(z, y, x, 1 - c)).wait_recv()
                    mine = cur.at[z]
                    @pl.when(z == 0)
                    def _():
                        arrived(1, kd)
                        if last: self.final(t, mine[...], dn[kd])
                        else: self.merge(mine, mine, dn.at[kd], rest)
                    @pl.when(z == line - 1)
                    def _():
                        arrived(0, ku)
                        if last: self.final(t, mine[...], up[ku])
                        else: self.merge(mine, mine, up.at[ku], rest)
                    @pl.when((z > 0) & (z < line - 1))
                    def _():
                        arrived(0, ku)
                        arrived(1, kd)
                        if last: self.final(t, mine[...], up[ku], dn[kd])
                        else:
                            self.merge(mine, mine, up.at[ku], rest)
                            self.merge(mine, mine, dn.at[kd], rest)
                todo.append(close)
                cur = cur.at[z]
            dims, first = rest, False
        return todo, pending

def scatter_bufs(line, rows, width, order):
    size = {"z": line, "y": 2, "x": 2}
    dims, out = "zyx", {}
    for n, axis in enumerate(order):
        rest = dims.replace(axis, "")
        shape = tuple(size[d] for d in rest) + (rows, width)
        if axis == "z":
            if n == 0: out["own"] = (line,) + shape
            out["up"] = (line - 1,) + shape
            out["dn"] = (line - 1,) + shape
        else:
            if n == 0: out["own"] = shape
            out[axis] = shape
        dims = rest
    return out

def scatter_body(line, chunks, n, names, *refs):
    grads, outs, rest = refs[:n], refs[n:2 * n], list(refs[2 * n:])
    bufs = [{k: rest.pop(0) for k in ks} for ks in names]
    land, pair, send, recv, load = rest
    pos = place()
    s = Scatter(line, pos, grads, outs, chunks, bufs, send, recv, load)
    enter(line, pos)
    plans = [s.steps(t) for t in range(len(chunks))]
    depth = max(len(p[0]) for p in plans)
    for p in range(len(chunks) + depth - 1):
        for k in range(depth):
            t = p - k
            if 0 <= t < len(chunks) and k < len(plans[t][0]): plans[t][0][k]()
    for _, pending in plans:
        for f in pending: f()
    z, y, x, c = pos
    cp = pltpu.make_async_remote_copy(src_ref=outs[0], dst_ref=land, send_sem=pair.at[0], recv_sem=pair.at[1], device_id=dev(z, y, x, 1 - c), device_id_type=MESH)
    cp.start()
    cp.wait()
    outs[0][...] += land[...]

def scatter(line, chunks, grads, cid):
    n = len(grads)
    slots = 2 * (line - 1) + 2
    scratch, names = [], []
    for w, off, width, order in chunks:
        shapes = scatter_bufs(line, grads[w].shape[3], width, order)
        names.append(tuple(shapes))
        scratch += [pltpu.VMEM(s, grads[w].dtype) for s in shapes.values()]
    T = len(chunks)
    return pl.pallas_call(
        functools.partial(scatter_body, line, chunks, n, names),
        out_shape=[jax.ShapeDtypeStruct(g.shape[3:], jnp.float32) for g in grads],
        in_specs=[pl.BlockSpec(memory_space=pl.ANY)] * n,
        out_specs=[pl.BlockSpec(memory_space=pltpu.VMEM)] * n,
        scratch_shapes=scratch + [pltpu.VMEM(grads[0].shape[3:], jnp.float32), pltpu.SemaphoreType.DMA((2,)), pltpu.SemaphoreType.DMA((T, slots)), pltpu.SemaphoreType.DMA((T, slots)), pltpu.SemaphoreType.DMA((T,))],
        compiler_params=pltpu.CompilerParams(collective_id=cid, has_side_effects=True, vmem_limit_bytes=63 * 2**20),
        name="gradient_scatter",
    )(*grads)


def rope_tables(length, width):
    half_width = width // 2
    inverse = THETA_BASE ** (-(jnp.arange(half_width, dtype=jnp.float32) * 2.0 / width))
    angles = jnp.arange(length, dtype=jnp.float32)[:, None] * inverse[None, :]
    cosine, sine = jnp.cos(angles), jnp.sin(angles)
    return jnp.concatenate([cosine, cosine], axis=1), jnp.concatenate([-sine, sine], axis=1)


def turn(x, cosine, sine):
    half = x.shape[-1] // 2
    return x * cosine + jnp.concatenate([x[:, half:], x[:, :half]], axis=1) * sine


def dot_nt(a, b):
    return lax.dot_general(a, b, (((1,), (1,)), ((), ())), preferred_element_type=jnp.float32)


def dot_tn(a, b):
    return lax.dot_general(a, b, (((0,), (0,)), ((), ())), preferred_element_type=jnp.float32)


def dot_nn(a, b):
    return jnp.dot(a, b, preferred_element_type=jnp.float32)


BLOCK = 128


def causal_weights(q, k, b, heads):
    scores = dot_nt(q, k) * (1.0 / math.sqrt(HEAD_SIZE))
    n = scores.shape[1]
    row = lax.broadcasted_iota(jnp.int32, scores.shape, 0) % BLOCK + b * BLOCK
    keep = row >= lax.broadcasted_iota(jnp.int32, scores.shape, 1)
    scores = jnp.where(keep, scores, -jnp.inf)
    log_total = jnp.log(jnp.sum(jnp.exp(scores), axis=1, keepdims=True))
    return jnp.exp(scores - log_total)


def rows_of(ref, first, heads, rows):
    return jnp.concatenate([ref[first + i, rows] for i in range(heads)], axis=0)


def attend_kernel(heads, groups, qkv, cosine, sine, q_out, k_out, v_out, mixed_out, mixed):
    share = heads // groups
    blocks = qkv.shape[0] // BLOCK

    @pl.loop(0, blocks)
    def _(r):
        rows = pl.ds(pl.multiple_of(r * BLOCK, BLOCK), BLOCK)
        cos, sin = cosine[rows, :], sine[rows, :]
        for h in range(heads + 2 * groups):
            x = qkv[rows, h * HEAD_SIZE : (h + 1) * HEAD_SIZE]
            if h < heads:
                q_out[h, rows] = turn(x, cos, sin).astype(q_out.dtype)
            elif h < heads + groups:
                k_out[h - heads, rows] = turn(x, cos, sin).astype(k_out.dtype)
            else:
                v_out[h - heads - groups, rows] = x.astype(v_out.dtype)

    @pl.loop(0, groups)
    def _(g):
        for b in range(blocks):
            rows, n = pl.ds(b * BLOCK, BLOCK), (b + 1) * BLOCK
            q = rows_of(q_out, g * share, share, rows)
            w = causal_weights(q, k_out[g, :n], b, share).astype(v_out.dtype)
            m = dot_nn(w, v_out[g, :n]).astype(mixed.dtype)
            for i in range(share):
                mixed[g * share + i, rows] = m[i * BLOCK : (i + 1) * BLOCK]

    @pl.loop(0, blocks)
    def _(r):
        rows = pl.ds(pl.multiple_of(r * BLOCK, BLOCK), BLOCK)
        mixed_out[rows, :] = jnp.concatenate([mixed[h, rows] for h in range(heads)], axis=1)


def attend(qkv, cosine, sine, halves):
    tokens = qkv.shape[0]
    heads, groups = QUERY_HEADS // halves, KEY_VALUE_HEADS // halves
    width = qkv.shape[1] // halves
    head = lambda n: pl.BlockSpec((n, tokens, HEAD_SIZE), lambda c: (c, 0, 0))
    table = pl.BlockSpec((tokens, HEAD_SIZE), lambda c: (0, 0))
    bf16 = jnp.bfloat16
    return pl.pallas_call(
        functools.partial(attend_kernel, heads, groups),
        grid=(halves,),
        out_shape=[
            jax.ShapeDtypeStruct((QUERY_HEADS, tokens, HEAD_SIZE), bf16),
            jax.ShapeDtypeStruct((KEY_VALUE_HEADS, tokens, HEAD_SIZE), bf16),
            jax.ShapeDtypeStruct((KEY_VALUE_HEADS, tokens, HEAD_SIZE), bf16),
            jax.ShapeDtypeStruct((tokens, QUERY_HEADS * HEAD_SIZE), bf16),
        ],
        in_specs=[pl.BlockSpec((tokens, width), lambda c: (0, c)), table, table],
        out_specs=[head(heads), head(groups), head(groups), pl.BlockSpec((tokens, heads * HEAD_SIZE), lambda c: (0, c))],
        scratch_shapes=[pltpu.VMEM((heads, tokens, HEAD_SIZE), bf16)],
        compiler_params=pltpu.CompilerParams(vmem_limit_bytes=60 * 2**20),
        name="attend",
    )(qkv, cosine, sine)


def attend_back_kernel(heads, groups, q, k, v, mixed, grad_mixed, cosine, sine, out, gm, dots, dq, dk, dv):
    share = heads // groups
    blocks = out.shape[0] // BLOCK
    scale = 1.0 / math.sqrt(HEAD_SIZE)

    @pl.loop(0, blocks)
    def _(r):
        rows = pl.ds(pl.multiple_of(r * BLOCK, BLOCK), BLOCK)
        for h in range(heads):
            lanes = slice(h * HEAD_SIZE, (h + 1) * HEAD_SIZE)
            g = grad_mixed[rows, lanes]
            dots[h, rows] = jnp.sum(g * mixed[rows, lanes].astype(jnp.float32), axis=1, keepdims=True)
            gm[h, rows] = g.astype(gm.dtype)

    dk[...] = jnp.zeros_like(dk)
    dv[...] = jnp.zeros_like(dv)

    @pl.loop(0, groups)
    def _(g):
        for b in range(blocks):
            rows, n = pl.ds(b * BLOCK, BLOCK), (b + 1) * BLOCK
            qb, gb, db = (rows_of(ref, g * share, share, rows) for ref in (q, gm, dots))
            kb, vb = k[g, :n], v[g, :n]
            p = causal_weights(qb, kb, b, share)
            ds = (p * (dot_nt(gb, vb) - db)).astype(qb.dtype)
            dv[g, :n] += dot_tn(p.astype(qb.dtype), gb)
            dk[g, :n] += dot_tn(ds, qb)
            d = dot_nn(ds, kb) * scale
            for i in range(share):
                dq[g * share + i, rows] = d[i * BLOCK : (i + 1) * BLOCK]

    @pl.loop(0, blocks)
    def _(r):
        rows = pl.ds(pl.multiple_of(r * BLOCK, BLOCK), BLOCK)
        cos, sin = cosine[rows, :], -sine[rows, :]
        parts = [turn(dq[h, rows], cos, sin) for h in range(heads)]
        parts += [turn(dk[g, rows] * scale, cos, sin) for g in range(groups)]
        parts += [dv[g, rows] for g in range(groups)]
        out[rows, :] = jnp.concatenate([part.astype(out.dtype) for part in parts], axis=1)


def attend_back(q, k, v, mixed, grad_mixed, cosine, sine, halves):
    tokens = q.shape[1]
    heads, groups = QUERY_HEADS // halves, KEY_VALUE_HEADS // halves
    width = (heads + 2 * groups) * HEAD_SIZE
    head = lambda n: pl.BlockSpec((n, tokens, HEAD_SIZE), lambda c: (c, 0, 0))
    table = pl.BlockSpec((tokens, HEAD_SIZE), lambda c: (0, 0))
    flat = pl.BlockSpec((tokens, heads * HEAD_SIZE), lambda c: (0, c))
    return pl.pallas_call(
        functools.partial(attend_back_kernel, heads, groups),
        grid=(halves,),
        out_shape=jax.ShapeDtypeStruct((tokens, width * halves), jnp.bfloat16),
        in_specs=[head(heads), head(groups), head(groups), flat, flat, table, table],
        out_specs=pl.BlockSpec((tokens, width), lambda c: (0, c)),
        scratch_shapes=[
            pltpu.VMEM((heads, tokens, HEAD_SIZE), jnp.bfloat16),
            pltpu.VMEM((heads, tokens, 1), jnp.float32),
            pltpu.VMEM((heads, tokens, HEAD_SIZE), jnp.float32),
            pltpu.VMEM((groups, tokens, HEAD_SIZE), jnp.float32),
            pltpu.VMEM((groups, tokens, HEAD_SIZE), jnp.float32),
        ],
        compiler_params=pltpu.CompilerParams(vmem_limit_bytes=60 * 2**20),
        name="attend_back",
    )(q, k, v, mixed, grad_mixed, cosine, sine)


def norm_back(grad_normed, unit_rows, inverse_rms, gain):
    scaled = grad_normed * gain
    inner = jnp.mean(scaled * unit_rows, axis=1, keepdims=True)
    return (inverse_rms * (scaled - unit_rows * inner), jnp.sum(grad_normed * unit_rows, axis=0))


def cut(halves, width, mix):
    chunks, k = [], 0
    for w, half in enumerate(halves):
        pieces = -(-half // width)
        while half % (pieces * 128):
            pieces += 1
        for i in range(pieces):
            chunks.append((w, i * (half // pieces), half // pieces, mix[k % len(mix)]))
            k += 1
    return tuple(chunks)


GATHER_MIX = ("xyz", "zyx", "zxy", "yxz", "zyx", "zxy", "zyx", "zxy")
SCATTER_MIX = ("xyz", "yxz")


def layer(n_dp, n_tensor, hidden_in, query_weight, key_matrix, value_matrix, out_weight, gate_weight, up_weight, down_weight, attention_gain, feedforward_gain, cotangent):
    line = n_dp // 4
    rows = attention_gain.shape[0]
    width = rows * n_dp
    bf16, f32 = jnp.bfloat16, jnp.float32
    side = lax.axis_index("tensor")

    gains = jnp.zeros((8, 128), bf16).at[0, :rows].set(attention_gain).at[1, :rows].set(feedforward_gain)
    shards = [gains, jnp.concatenate([query_weight, key_matrix, value_matrix], axis=1), out_weight.T, gate_weight, up_weight, down_weight.T]
    fulls = gather(line, cut([s.shape[1] for s in shards], 512, GATHER_MIX), shards, 0)
    all_gains = fulls[0].reshape(n_dp, 8, -1)
    gain_first = all_gains[:, 0, :rows].reshape(1, width).astype(f32)
    gain_second = all_gains[:, 1, :rows].reshape(1, width).astype(f32)
    w_qkv, w_out, w_gate, w_up, w_down = (f.reshape(width, f.shape[-1]) for f in fulls[1:])

    cosine, sine = rope_tables(SEQUENCE_LENGTH, HEAD_SIZE)
    x = hidden_in.astype(f32)
    inverse_one = lax.rsqrt(jnp.mean(x * x, axis=1, keepdims=True) + EPSILON)
    unit_one = x * inverse_one
    normed_one = (unit_one * gain_first).astype(bf16)
    q, k, v, mixed = attend(dot_nn(normed_one, w_qkv), cosine, sine, n_tensor)
    middle = x + dot_nt(mixed, w_out)
    inverse_two = lax.rsqrt(jnp.mean(middle * middle, axis=1, keepdims=True) + EPSILON)
    unit_two = middle * inverse_two
    normed_two = (unit_two * gain_second).astype(bf16)
    gate = dot_nn(normed_two, w_gate)
    up = dot_nn(normed_two, w_up)
    sigma = jax.nn.sigmoid(gate)
    hidden = (gate * sigma * up).astype(bf16)
    hidden_out = (middle + dot_nt(hidden, w_down)).astype(bf16)
    grad_hidden = dot_nn(cotangent, w_down)
    grad_up_act = (grad_hidden * gate * sigma).astype(bf16)
    grad_gate_act = (grad_hidden * up * sigma * (1.0 + gate * (1.0 - sigma))).astype(bf16)
    grad_normed_two = dot_nt(grad_gate_act, w_gate) + dot_nt(grad_up_act, w_up)
    middle_part, second_part = norm_back(grad_normed_two, unit_two, inverse_two, gain_second)
    grad_middle = cotangent.astype(f32) + middle_part
    grad_middle_round = grad_middle.astype(bf16)
    grad_mixed = dot_nn(grad_middle_round, w_out)
    grad_qkv_act = attend_back(q, k, v, mixed, grad_mixed, cosine, sine, n_tensor)
    grad_normed_one = dot_nt(grad_qkv_act, w_qkv)
    first_part, first_gain = norm_back(grad_normed_one, unit_one, inverse_one, gain_first)
    grad_in = grad_middle + first_part

    swap = [(i, i ^ 1) for i in range(n_tensor)]
    other = lambda a: lax.ppermute(a, "tensor", swap)

    def of_half(a, which):
        size = a.shape[1] // n_tensor
        return lax.dynamic_slice_in_dim(a, which * size, size, axis=1)

    both = lambda a: jnp.concatenate([a, other(a)], axis=0)
    both_half = lambda a: jnp.concatenate([of_half(a, side), other(of_half(a, 1 - side))], axis=0)
    n1, n2, ct, gm = both(normed_one), both(normed_two), both(cotangent), both(grad_middle_round)
    weight_grad = lambda a, b: dot_tn(a, both_half(b)).astype(bf16)
    grads = [
        weight_grad(ct, hidden),
        weight_grad(n2, grad_gate_act),
        weight_grad(n2, grad_up_act),
        weight_grad(gm, mixed),
        weight_grad(n1, grad_qkv_act),
    ]
    parts = jnp.stack([first_gain, second_part]).reshape(2, n_dp, rows).transpose(1, 0, 2)
    parts = jnp.pad(parts, ((0, 0), (0, 6), (0, 128 - rows))).astype(bf16)
    grads = [parts.reshape(line, 2, 2, 8, 128)] + [g.reshape(line, 2, 2, rows, g.shape[1]) for g in grads]
    g_gains, g_down, g_gate, g_up, g_out, g_qkv = scatter(line, cut([g.shape[-1] for g in grads], 512, SCATTER_MIX), grads, 1)
    nq, nk = query_weight.shape[1], key_matrix.shape[1]
    return (
        hidden_out,
        grad_in,
        g_qkv[:, :nq],
        g_qkv[:, nq : nq + nk],
        g_qkv[:, nq + nk :],
        g_out.T,
        g_gate,
        g_up,
        g_down.T,
        g_gains[0, :rows],
        g_gains[1, :rows],
    )


def solution(mesh):
    split = P(("dp", "tensor"), None)
    row, column, gain = P("dp", "tensor"), P("tensor", "dp"), P("dp")
    return jax.shard_map(
        functools.partial(layer, mesh.shape["dp"], mesh.shape["tensor"]),
        mesh=mesh,
        in_specs=(split, row, row, row, column, row, row, column, gain, gain, split),
        out_specs=(split, split, row, row, row, column, row, row, column, gain, gain),
        check_vma=False,
    )
```

```python
import functools
import math

import jax
import jax.numpy as jnp
from jax import lax
from jax.experimental import pallas as pl
from jax.experimental.pallas import tpu as pltpu
from jax.sharding import PartitionSpec as P

QUERY_HEADS = 16
KEY_VALUE_HEADS = 8
HEAD_SIZE = 96
SEQUENCE_LENGTH = 512

EPSILON = 1e-05
THETA_BASE = 100000.0
MESH = pl.DeviceIdType.MESH


def place():
    d = lax.axis_index("dp")
    return lax.div(d, 4), lax.rem(lax.div(d, 2), 2), lax.rem(d, 2), lax.axis_index("tensor")


def dev(z, y, x, c):
    return (z * 4 + y * 2 + x, c)


def enter(line, pos):
    z, y, x, c = pos
    barrier = pltpu.get_barrier_semaphore()

    def greet(who):
        pl.semaphore_signal(barrier, inc=1, device_id=who, device_id_type=MESH)

    greet(dev(z, y, x, 1 - c))
    greet(dev(z, y, 1 - x, c))
    greet(dev(z, 1 - y, x, c))

    @pl.when(z > 0)
    def _():
        greet(dev(z - 1, y, x, c))

    @pl.when(z < line - 1)
    def _():
        greet(dev(z + 1, y, x, c))

    pl.semaphore_wait(barrier, 3 + (z > 0).astype(jnp.int32) + (z < line - 1).astype(jnp.int32))


def remote(src, dst, send, recv, who):
    return pltpu.make_async_remote_copy(src_ref=src, dst_ref=dst, send_sem=send, recv_sem=recv, device_id=who, device_id_type=MESH)


class Gather:
    def __init__(self, line, pos, shard, full, width, orders, paired, send, recv):
        self.line, self.pos, self.shard, self.full, self.width = line, pos, shard, full, width
        self.orders, self.paired, self.send, self.recv = orders, paired, send, recv
        self.count = shard.shape[-1] // width
        self.depth = line + 1 + paired

    def columns(self, t, sub):
        part = self.width // len(self.orders[0])
        return t * self.width + sub * part, part

    def region(self, t, sub, have, z=None):
        first, part = self.columns(t, sub)
        pz, py, px, c = self.pos
        if self.paired:
            first = first + c * self.shard.shape[-1]
        every = slice(None)
        zi = z if z is not None else (every if "z" in have else pz)
        cols = pl.ds(pl.multiple_of(first, 128), part)
        return self.full.at[zi, every if "y" in have else py, every if "x" in have else px, :, cols]

    def own(self, t, sub):
        first, part = self.columns(t, sub)
        return self.shard.at[:, pl.ds(pl.multiple_of(first, 128), part)]

    def copy(self, t, sub, slot, src, dst, who):
        return remote(src, dst, self.send.at[t, sub, slot], self.recv.at[t, sub, slot], who)

    def hop(self, t, sub, h, up, have, what):
        z, y, x, c = self.pos
        slot = (h - 1) * 2 + up
        if up:
            block, incoming, who = z - (h - 1), z - h, dev(z + 1, y, x, c)
            there, here = (z + 1 < self.line) & (z >= h - 1), z >= h
        else:
            block, incoming, who = z + (h - 1), z + h, dev(z - 1, y, x, c)
            there, here = (z > 0) & (z + h - 1 < self.line), z + h < self.line

        @pl.when(here if what == "recv" else there)
        def _():
            if what == "recv":
                r = self.region(t, sub, have, incoming)
                self.copy(t, sub, slot, r, r, dev(z, y, x, 1 - c)).wait_recv()
                return
            r = self.region(t, sub, have, block)
            cp = self.copy(t, sub, slot, self.own(t, sub) if h == 1 and not have else r, r, who)
            cp.start() if what == "start" else cp.wait_send()

    def act(self, t, sub, order, i, what):
        z, y, x, c = self.pos
        moves, have = [], ""
        for axis in order:
            moves += [(axis, h, have) for h in (range(1, self.line) if axis == "z" else (0,))]
            have += axis
        if self.paired:
            moves.append(("c", 0, have))
        axis, h, have = moves[i]
        if axis == "z":
            for up in (1, 0):
                self.hop(t, sub, h, up, have, what)
            return
        who = {"y": dev(z, 1 - y, x, c), "x": dev(z, y, 1 - x, c), "c": dev(z, y, x, 1 - c)}[axis]
        land = self.region(t, sub, have)
        cp = self.copy(t, sub, 2 * (self.line - 1) + "yxc".index(axis), land if have else self.own(t, sub), land, who)
        {"start": cp.start, "recv": cp.wait_recv, "sent": cp.wait_send}[what]()

    def each(self, t, fn):
        there = (t >= 0) & (t < self.count)
        for v, orders in enumerate(self.orders):
            turn_of = there if len(self.orders) == 1 else there & ((lax.rem(t + 4, 4) == 0) == (v == 1))

            @pl.when(turn_of)
            def _():
                for sub, order in enumerate(orders):
                    fn(sub, order)

    def step(self, t, s):
        def go(sub, order):
            if s > 0:
                self.act(t, sub, order, s - 1, "recv")
            if s < self.depth:
                self.act(t, sub, order, s, "start")

        self.each(t, go)

    def advance(self, p):
        for s in range(self.depth + 1):
            self.step(p - s, s)

    def finish(self):
        @pl.loop(0, self.count)
        def _(t):
            self.each(t, lambda sub, order: [self.act(t, sub, order, i, "sent") for i in range(self.depth)])


def own_copy(g, sem):
    z, y, x, c = g.pos
    first = c * g.shard.shape[-1] if g.paired else 0
    return pltpu.make_async_copy(g.shard, g.full.at[z, y, x, :, pl.ds(pl.multiple_of(first, 128), g.shard.shape[-1])], sem)


class Scatter:
    def __init__(self, line, pos, grads, outs, chunks, bufs, send, recv, load):
        self.line, self.pos, self.grads, self.outs, self.chunks, self.bufs = line, pos, grads, outs, chunks, bufs
        self.send, self.recv, self.load = send, recv, load
    def copy(self, t, slot, src, dst, who):
        return pltpu.make_async_remote_copy(src_ref=src, dst_ref=dst, send_sem=self.send.at[t, slot], recv_sem=self.recv.at[t, slot], device_id=who, device_id_type=MESH)
    def pick(self, ref, dims, **at):
        return ref.at[tuple(at.get(d, slice(None)) for d in dims)]
    def source(self, t):
        w, off, width, _ = self.chunks[t]
        return self.grads[w].at[:, :, :, :, pl.ds(off, width)]
    def merge(self, dst, a, b, dims):
        def go(lead, rest):
            if not rest:
                dst[lead] = a[lead] + b[lead]
            elif rest[0] == "z":
                @pl.loop(0, self.line)
                def _(i): go(lead + (i,), rest[1:])
            else:
                for i in range(2): go(lead + (i,), rest[1:])
        go((), dims)
    def final(self, t, *parts):
        w, off, width, _ = self.chunks[t]
        total = parts[0].astype(jnp.float32)
        for p in parts[1:]: total = total + p.astype(jnp.float32)
        self.outs[w][:, pl.ds(off, width)] = total
    def steps(self, t):
        z, y, x, c = self.pos
        order = self.chunks[t][3]
        buf = self.bufs[t]
        todo, dims, cur, first, used = [], "zyx", self.source(t), True, 0
        pending = []
        line = self.line
        for n, axis in enumerate(order):
            last = n == 2
            rest = dims.replace(axis, "")
            if axis in "xy":
                me = {"x": x, "y": y}[axis]
                who = {"x": dev(z, y, 1 - x, c), "y": dev(z, 1 - y, x, c)}[axis]
                slot = 2 * (line - 1) + "yx".index(axis)
                land = buf[axis]
                give = self.pick(cur, dims, **{axis: 1 - me})
                keep = self.pick(cur, dims, **{axis: me})
                cp = self.copy(t, slot, give, land, who)
                if first:
                    ld = pltpu.make_async_copy(keep, buf["own"], self.load.at[t])
                    def begin(cp=cp, ld=ld): cp.start(); ld.start()
                    todo.append(begin)
                    have = buf["own"]
                else:
                    ld = None
                    have = keep
                    self_begin = cp.start
                    prev = todo.pop()
                    todo.append(lambda prev=prev, b=self_begin: (prev(), b()))
                def end(cp=cp, ld=ld, have=have, land=land, rest=rest, last=last):
                    if ld is not None: ld.wait()
                    cp.wait_recv()
                    if last: self.final(t, land[...], have[...])
                    else: self.merge(land, land, have, rest)
                todo.append(end)
                cur = land
                pending.append(cp.wait_send)
            else:
                up, dn = buf["up"], buf["dn"]
                if first:
                    ld = pltpu.make_async_copy(cur, buf["own"], self.load.at[t])
                    todo.append(ld.start)
                    cur = buf["own"]
                else: ld = None
                for j in range(line - 1):
                    def hop(j=j, cur=cur, ld=ld, rest=rest):
                        if j == 0 and ld is not None: ld.wait()
                        for way, ref, target, src_z, edge in ((0, up, line - 1 - j, z - 1, z == 0), (1, dn, j, z + 1, z == line - 1)):
                            slot = 2 * j + way
                            nxt = dev(z + 1, y, x, c) if way == 0 else dev(z - 1, y, x, c)
                            passes = (target > z) if way == 0 else (target < z)
                            @pl.when(passes & edge)
                            def _(): self.copy(t, slot, cur.at[target], ref.at[j], nxt).start()
                            @pl.when(passes & ~edge)
                            def _():
                                cp = self.copy(t, slot, ref.at[j], ref.at[j], nxt)
                                cp.wait_recv()
                                self.merge(ref.at[j], ref.at[j], cur.at[target], rest)
                                cp.start()
                    todo.append(hop)
                    for way in (0, 1):
                        def drain(j=j, way=way, cur=cur):
                            target = line - 1 - j if way == 0 else j
                            passes = (target > z) if way == 0 else (target < z)
                            @pl.when(passes)
                            def _(): self.copy(t, 2 * j + way, cur.at[target], (up if way == 0 else dn).at[j], dev(z, y, x, 1 - c)).wait_send()
                        pending.append(drain)
                def close(cur=cur, rest=rest, last=last):
                    ku, kd = line - 1 - z, z
                    def arrived(way, k):
                        ref = up if way == 0 else dn
                        self.copy(t, 2 * k + way, ref.at[k], ref.at[k], dev(z, y, x, 1 - c)).wait_recv()
                    mine = cur.at[z]
                    @pl.when(z == 0)
                    def _():
                        arrived(1, kd)
                        if last: self.final(t, mine[...], dn[kd])
                        else: self.merge(mine, mine, dn.at[kd], rest)
                    @pl.when(z == line - 1)
                    def _():
                        arrived(0, ku)
                        if last: self.final(t, mine[...], up[ku])
                        else: self.merge(mine, mine, up.at[ku], rest)
                    @pl.when((z > 0) & (z < line - 1))
                    def _():
                        arrived(0, ku)
                        arrived(1, kd)
                        if last: self.final(t, mine[...], up[ku], dn[kd])
                        else:
                            self.merge(mine, mine, up.at[ku], rest)
                            self.merge(mine, mine, dn.at[kd], rest)
                todo.append(close)
                cur = cur.at[z]
            dims, first = rest, False
        return todo, pending

def scatter_bufs(line, rows, width, order):
    size = {"z": line, "y": 2, "x": 2}
    dims, out = "zyx", {}
    for n, axis in enumerate(order):
        rest = dims.replace(axis, "")
        shape = tuple(size[d] for d in rest) + (rows, width)
        if axis == "z":
            if n == 0: out["own"] = (line,) + shape
            out["up"] = (line - 1,) + shape
            out["dn"] = (line - 1,) + shape
        else:
            if n == 0: out["own"] = shape
            out[axis] = shape
        dims = rest
    return out

def scatter_body(line, chunks, n, names, *refs):
    grads, outs, rest = refs[:n], refs[n:2 * n], list(refs[2 * n:])
    bufs = [{k: rest.pop(0) for k in ks} for ks in names]
    land, pair, send, recv, load = rest
    pos = place()
    s = Scatter(line, pos, grads, outs, chunks, bufs, send, recv, load)
    enter(line, pos)
    plans = [s.steps(t) for t in range(len(chunks))]
    depth = max(len(p[0]) for p in plans)
    for p in range(len(chunks) + depth - 1):
        for k in range(depth):
            t = p - k
            if 0 <= t < len(chunks) and k < len(plans[t][0]): plans[t][0][k]()
    for _, pending in plans:
        for f in pending: f()
    z, y, x, c = pos
    cp = pltpu.make_async_remote_copy(src_ref=outs[0], dst_ref=land, send_sem=pair.at[0], recv_sem=pair.at[1], device_id=dev(z, y, x, 1 - c), device_id_type=MESH)
    cp.start()
    cp.wait()
    outs[0][...] += land[...]

def scatter(line, chunks, grads, cid):
    n = len(grads)
    slots = 2 * (line - 1) + 2
    scratch, names = [], []
    for w, off, width, order in chunks:
        shapes = scatter_bufs(line, grads[w].shape[3], width, order)
        names.append(tuple(shapes))
        scratch += [pltpu.VMEM(s, grads[w].dtype) for s in shapes.values()]
    T = len(chunks)
    return pl.pallas_call(
        functools.partial(scatter_body, line, chunks, n, names),
        out_shape=[jax.ShapeDtypeStruct(g.shape[3:], jnp.float32) for g in grads],
        in_specs=[pl.BlockSpec(memory_space=pl.ANY)] * n,
        out_specs=[pl.BlockSpec(memory_space=pltpu.VMEM)] * n,
        scratch_shapes=scratch + [pltpu.VMEM(grads[0].shape[3:], jnp.float32), pltpu.SemaphoreType.DMA((2,)), pltpu.SemaphoreType.DMA((T, slots)), pltpu.SemaphoreType.DMA((T, slots)), pltpu.SemaphoreType.DMA((T,))],
        compiler_params=pltpu.CompilerParams(collective_id=cid, has_side_effects=True, vmem_limit_bytes=63 * 2**20),
        name="gradient_scatter",
    )(*grads)


def rope_tables(length, width):
    half_width = width // 2
    inverse = THETA_BASE ** (-(jnp.arange(half_width, dtype=jnp.float32) * 2.0 / width))
    angles = jnp.arange(length, dtype=jnp.float32)[:, None] * inverse[None, :]
    cosine, sine = jnp.cos(angles), jnp.sin(angles)
    return jnp.concatenate([cosine, cosine], axis=1), jnp.concatenate([-sine, sine], axis=1)


def turn(x, cosine, sine):
    half = x.shape[-1] // 2
    return x * cosine + jnp.concatenate([x[:, half:], x[:, :half]], axis=1) * sine


def dot_nt(a, b):
    return lax.dot_general(a, b, (((1,), (1,)), ((), ())), preferred_element_type=jnp.float32)


def dot_tn(a, b):
    return lax.dot_general(a, b, (((0,), (0,)), ((), ())), preferred_element_type=jnp.float32)


def dot_nn(a, b):
    return jnp.dot(a, b, preferred_element_type=jnp.float32)


BLOCK = 128


def causal_weights(q, k, b, heads):
    scores = dot_nt(q, k) * (1.0 / math.sqrt(HEAD_SIZE))
    n = scores.shape[1]
    row = lax.broadcasted_iota(jnp.int32, scores.shape, 0) % BLOCK + b * BLOCK
    keep = row >= lax.broadcasted_iota(jnp.int32, scores.shape, 1)
    scores = jnp.where(keep, scores, -jnp.inf)
    log_total = jnp.log(jnp.sum(jnp.exp(scores), axis=1, keepdims=True))
    return jnp.exp(scores - log_total)


def rows_of(ref, first, heads, rows):
    return jnp.concatenate([ref[first + i, rows] for i in range(heads)], axis=0)


def attend_kernel(heads, groups, qkv, cosine, sine, q_out, k_out, v_out, mixed_out, mixed):
    share = heads // groups
    blocks = qkv.shape[0] // BLOCK

    @pl.loop(0, blocks)
    def _(r):
        rows = pl.ds(pl.multiple_of(r * BLOCK, BLOCK), BLOCK)
        cos, sin = cosine[rows, :], sine[rows, :]
        for h in range(heads + 2 * groups):
            x = qkv[rows, h * HEAD_SIZE : (h + 1) * HEAD_SIZE]
            if h < heads:
                q_out[h, rows] = turn(x, cos, sin).astype(q_out.dtype)
            elif h < heads + groups:
                k_out[h - heads, rows] = turn(x, cos, sin).astype(k_out.dtype)
            else:
                v_out[h - heads - groups, rows] = x.astype(v_out.dtype)

    @pl.loop(0, groups)
    def _(g):
        for b in range(blocks):
            rows, n = pl.ds(b * BLOCK, BLOCK), (b + 1) * BLOCK
            q = rows_of(q_out, g * share, share, rows)
            w = causal_weights(q, k_out[g, :n], b, share).astype(v_out.dtype)
            m = dot_nn(w, v_out[g, :n]).astype(mixed.dtype)
            for i in range(share):
                mixed[g * share + i, rows] = m[i * BLOCK : (i + 1) * BLOCK]

    @pl.loop(0, blocks)
    def _(r):
        rows = pl.ds(pl.multiple_of(r * BLOCK, BLOCK), BLOCK)
        mixed_out[rows, :] = jnp.concatenate([mixed[h, rows] for h in range(heads)], axis=1)


def attend(qkv, cosine, sine, halves):
    tokens = qkv.shape[0]
    heads, groups = QUERY_HEADS // halves, KEY_VALUE_HEADS // halves
    width = qkv.shape[1] // halves
    head = lambda n: pl.BlockSpec((n, tokens, HEAD_SIZE), lambda c: (c, 0, 0))
    table = pl.BlockSpec((tokens, HEAD_SIZE), lambda c: (0, 0))
    bf16 = jnp.bfloat16
    return pl.pallas_call(
        functools.partial(attend_kernel, heads, groups),
        grid=(halves,),
        out_shape=[
            jax.ShapeDtypeStruct((QUERY_HEADS, tokens, HEAD_SIZE), bf16),
            jax.ShapeDtypeStruct((KEY_VALUE_HEADS, tokens, HEAD_SIZE), bf16),
            jax.ShapeDtypeStruct((KEY_VALUE_HEADS, tokens, HEAD_SIZE), bf16),
            jax.ShapeDtypeStruct((tokens, QUERY_HEADS * HEAD_SIZE), bf16),
        ],
        in_specs=[pl.BlockSpec((tokens, width), lambda c: (0, c)), table, table],
        out_specs=[head(heads), head(groups), head(groups), pl.BlockSpec((tokens, heads * HEAD_SIZE), lambda c: (0, c))],
        scratch_shapes=[pltpu.VMEM((heads, tokens, HEAD_SIZE), bf16)],
        compiler_params=pltpu.CompilerParams(vmem_limit_bytes=60 * 2**20),
        name="attend",
    )(qkv, cosine, sine)


def attend_back_kernel(heads, groups, q, k, v, mixed, grad_mixed, cosine, sine, out, gm, dots, dq, dk, dv):
    share = heads // groups
    blocks = out.shape[0] // BLOCK
    scale = 1.0 / math.sqrt(HEAD_SIZE)

    @pl.loop(0, blocks)
    def _(r):
        rows = pl.ds(pl.multiple_of(r * BLOCK, BLOCK), BLOCK)
        for h in range(heads):
            lanes = slice(h * HEAD_SIZE, (h + 1) * HEAD_SIZE)
            g = grad_mixed[rows, lanes]
            dots[h, rows] = jnp.sum(g * mixed[rows, lanes].astype(jnp.float32), axis=1, keepdims=True)
            gm[h, rows] = g.astype(gm.dtype)

    dk[...] = jnp.zeros_like(dk)
    dv[...] = jnp.zeros_like(dv)

    @pl.loop(0, groups)
    def _(g):
        for b in range(blocks):
            rows, n = pl.ds(b * BLOCK, BLOCK), (b + 1) * BLOCK
            qb, gb, db = (rows_of(ref, g * share, share, rows) for ref in (q, gm, dots))
            kb, vb = k[g, :n], v[g, :n]
            p = causal_weights(qb, kb, b, share)
            ds = (p * (dot_nt(gb, vb) - db)).astype(qb.dtype)
            dv[g, :n] += dot_tn(p.astype(qb.dtype), gb)
            dk[g, :n] += dot_tn(ds, qb)
            d = dot_nn(ds, kb) * scale
            for i in range(share):
                dq[g * share + i, rows] = d[i * BLOCK : (i + 1) * BLOCK]

    @pl.loop(0, blocks)
    def _(r):
        rows = pl.ds(pl.multiple_of(r * BLOCK, BLOCK), BLOCK)
        cos, sin = cosine[rows, :], -sine[rows, :]
        parts = [turn(dq[h, rows], cos, sin) for h in range(heads)]
        parts += [turn(dk[g, rows] * scale, cos, sin) for g in range(groups)]
        parts += [dv[g, rows] for g in range(groups)]
        out[rows, :] = jnp.concatenate([part.astype(out.dtype) for part in parts], axis=1)


def attend_back(q, k, v, mixed, grad_mixed, cosine, sine, halves):
    tokens = q.shape[1]
    heads, groups = QUERY_HEADS // halves, KEY_VALUE_HEADS // halves
    width = (heads + 2 * groups) * HEAD_SIZE
    head = lambda n: pl.BlockSpec((n, tokens, HEAD_SIZE), lambda c: (c, 0, 0))
    table = pl.BlockSpec((tokens, HEAD_SIZE), lambda c: (0, 0))
    flat = pl.BlockSpec((tokens, heads * HEAD_SIZE), lambda c: (0, c))
    return pl.pallas_call(
        functools.partial(attend_back_kernel, heads, groups),
        grid=(halves,),
        out_shape=jax.ShapeDtypeStruct((tokens, width * halves), jnp.bfloat16),
        in_specs=[head(heads), head(groups), head(groups), flat, flat, table, table],
        out_specs=pl.BlockSpec((tokens, width), lambda c: (0, c)),
        scratch_shapes=[
            pltpu.VMEM((heads, tokens, HEAD_SIZE), jnp.bfloat16),
            pltpu.VMEM((heads, tokens, 1), jnp.float32),
            pltpu.VMEM((heads, tokens, HEAD_SIZE), jnp.float32),
            pltpu.VMEM((groups, tokens, HEAD_SIZE), jnp.float32),
            pltpu.VMEM((groups, tokens, HEAD_SIZE), jnp.float32),
        ],
        compiler_params=pltpu.CompilerParams(vmem_limit_bytes=60 * 2**20),
        name="attend_back",
    )(q, k, v, mixed, grad_mixed, cosine, sine)


ROWS = 128


def each_rows(tokens, step, fn):
    @pl.loop(0, tokens // step)
    def _(r):
        fn(pl.ds(pl.multiple_of(r * step, step), step))


def forward_kernel(line, width, block, *refs):
    refs = list(refs)
    take = lambda n: [refs.pop(0) for _ in range(n)]
    shard, gains, hid, ct, cosine, sine = take(6)
    full, gains_full, q_out, k_out, v_out, mixed_out, n1_pair, n2_pair, ct_pair, mixed_pair, gm_pair = take(11)
    tile_pairs = take(3)
    hidden_out, grad_middle, grad_mixed, gain_sum = take(4)
    wbuf, gain_buf, gain, n1, n2, flat, qh, kh, vh, mh, mixed, middle, acc, grad_n2, act, tiles = take(16)
    send, recv, gsend, grecv, own_sem, load_sem, gain_sem, local_sem, pair_send, pair_recv, tile_local, tile_send, tile_recv = take(13)

    pos = place()
    z, y, x, c = pos
    tokens, d_model = hid.shape
    half = shard.shape[-1]
    heads, groups = qh.shape[0] // 2, kh.shape[0] // 2
    sibling = dev(z, y, x, 1 - c)
    bf16, f32 = jnp.bfloat16, jnp.float32

    g = Gather(line, pos, shard, full, width, (("zyx", "zxy"), ("xyz", "yxz")), 1, send, recv)
    gg = Gather(line, pos, gains, gains_full, gains.shape[-1], (("zyx",),), 0, gsend, grecv)
    g_own, gg_own = own_copy(g, own_sem.at[0]), own_copy(gg, own_sem.at[1])
    g_own.start()
    gg_own.start()
    enter(line, pos)

    def load(t, hh, slot):
        cols = pl.ds(pl.multiple_of(hh * half + t * width, 128), width)
        return pltpu.make_async_copy(full.at[:, :, :, :, cols], wbuf.at[slot, hh], load_sem.at[slot, hh])

    def weight(slot, hh):
        return wbuf[slot, hh].reshape(d_model, width)

    def share(i, own_src, own_dst, other_src, other_dst):
        return pltpu.make_async_copy(own_src, own_dst, local_sem.at[i]), remote(other_src, other_dst, pair_send.at[i], pair_recv.at[i], sibling)

    shares = [share(i, src, pair.at[0], src, pair.at[1]) for i, (src, pair) in enumerate(((ct, ct_pair), (n1, n1_pair), (n2, n2_pair), (n1, gm_pair)))]
    hw = mixed.shape[1] // 2
    side = lambda ref, s, w: ref.at[:, pl.ds(pl.multiple_of(s * w, 128), w)]
    shares.append(share(4, side(mixed, c, hw), mixed_pair.at[0], side(mixed, 1 - c, hw), mixed_pair.at[1]))
    keeps = [pltpu.make_async_copy(src, dst, local_sem.at[5 + i]) for i, (src, dst) in enumerate(((qh, q_out), (kh, k_out), (vh, v_out), (mixed, mixed_out)))]

    def begin(i):
        for cp in shares[i]:
            cp.start()

    def end(i):
        for cp in shares[i]:
            cp.wait()

    def tile_copies(j, hh):
        slot = lax.rem(j, 2)
        cols = pl.ds(pl.multiple_of(j * block, 128), block)
        own = [pltpu.make_async_copy(tiles.at[slot, hh, i], pair.at[0, :, cols], tile_local.at[j, i]) for i, pair in enumerate(tile_pairs)]
        out = [remote(tiles.at[slot, hh, i], pair.at[1, :, cols], tile_send.at[j, i], tile_recv.at[j, i], sibling) for i, pair in enumerate(tile_pairs)]
        return own, out

    def drain_tiles(j):
        for cp in tile_copies(j, 0)[0]:
            cp.wait()
        for cp in tile_copies(j, 0)[1]:
            cp.wait_send()

    def normalize():
        loaded = pltpu.make_async_copy(gains_full, gain_buf, gain_sem)
        loaded.start()
        loaded.wait()
        n = d_model // (gain_buf.shape[0] * 4)
        table = gain_buf[...].astype(f32)
        for i in range(2):
            gain[i : i + 1, :] = jnp.concatenate([table[a, b, e, i : i + 1, :n] for a in range(gain_buf.shape[0]) for b in range(2) for e in range(2)], axis=1)

        def rows_of_norm(rows):
            v = hid[rows, :].astype(f32)
            v = v * lax.rsqrt(jnp.mean(v * v, axis=1, keepdims=True) + EPSILON)
            n1[rows, :] = (v * gain[0:1, :]).astype(bf16)

        each_rows(tokens, ROWS, rows_of_norm)
        begin(1)

    def project(slot, outs):
        @pl.loop(0, 2)
        def _(hh):
            flat[...] = dot_nn(n1[...], weight(slot, hh))

            def to_heads(rows):
                cos, sin = cosine[rows, :], sine[rows, :]
                first = 0
                for n, target, turned in outs:
                    for h in range(n):
                        v = flat[rows, (first + h) * HEAD_SIZE : (first + h + 1) * HEAD_SIZE]
                        target[hh * n + h, rows] = (turn(v, cos, sin) if turned else v).astype(bf16)
                    first += n

            each_rows(tokens, ROWS, to_heads)

    def attend_half(hh):
        per = heads // groups
        blocks = tokens // BLOCK

        @pl.loop(0, groups)
        def _(i):
            kv = hh * groups + i
            for b in range(blocks):
                rows, n = pl.ds(b * BLOCK, BLOCK), (b + 1) * BLOCK
                w = causal_weights(rows_of(qh, kv * per, per, rows), kh[kv, :n], b, per).astype(bf16)
                m = dot_nn(w, vh[kv, :n]).astype(bf16)
                for e in range(per):
                    mh[kv * per + e, rows] = m[e * BLOCK : (e + 1) * BLOCK]

    def leave_attention(slot):
        def join(rows):
            mixed[rows, :] = jnp.concatenate([mh[h, rows] for h in range(2 * heads)], axis=1)

        each_rows(tokens, ROWS, join)
        begin(4)
        for cp in keeps:
            cp.start()
        middle[...] = hid[...].astype(f32) + dot_nt(mixed[:, :hw], weight(slot, 0))
        middle[...] += dot_nt(mixed[:, hw:], weight(slot, 1))

        def rows_of_norm(rows):
            v = middle[rows, :]
            acc[rows, :] = v
            v = v * lax.rsqrt(jnp.mean(v * v, axis=1, keepdims=True) + EPSILON)
            n2[rows, :] = (v * gain[1:2, :]).astype(bf16)
            grad_n2[rows, :] = jnp.zeros_like(v)

        each_rows(tokens, ROWS, rows_of_norm)
        begin(2)

    def feed_forward(j, slot):
        @pl.when(j >= 2)
        def _():
            drain_tiles(j - 2)

        part = lax.rem(j, 2)

        @pl.loop(0, 2)
        def _(hh):
            act[0] = dot_nn(n2[...], weight(slot, hh)[:, :block])
            act[1] = dot_nn(n2[...], weight(slot, hh)[:, block : 2 * block])
            act[2] = dot_nn(ct[...], weight(slot, hh)[:, 2 * block :])

            def gated(rows):
                gate, up, grad = act[0, rows], act[1, rows], act[2, rows]
                sigma = jax.nn.sigmoid(gate)
                tiles[part, hh, 0, rows] = (gate * sigma * up).astype(bf16)
                tiles[part, hh, 1, rows] = (grad * up * sigma * (1.0 + gate * (1.0 - sigma))).astype(bf16)
                tiles[part, hh, 2, rows] = (grad * gate * sigma).astype(bf16)

            each_rows(tokens, ROWS // 2, gated)
            own, out = tile_copies(j, hh)

            @pl.when(hh == c)
            def _():
                for cp in own:
                    cp.start()

            @pl.when(hh != c)
            def _():
                for cp in out:
                    cp.start()

            acc[...] += dot_nt(tiles[part, hh, 0], weight(slot, hh)[:, 2 * block :])
            both = jnp.concatenate([tiles[part, hh, 1], tiles[part, hh, 2]], axis=1)
            grad_n2[...] += dot_nt(both, weight(slot, hh)[:, : 2 * block])

    count, lead = g.count, g.depth + 1

    @pl.loop(0, count + lead)
    def _(p):
        @pl.when(p == 0)
        def _():
            g_own.wait()
            gg_own.wait()
            begin(0)

        gg.advance(p)
        g.advance(p)
        u = p - lead

        @pl.when((u >= -1) & (u + 1 < count))
        def _():
            for hh in range(2):
                load(u + 1, hh, lax.rem(u + 1, 2)).start()

        @pl.when(u >= 0)
        def _():
            slot = lax.rem(u, 2)
            for hh in range(2):
                load(u, hh, slot).wait()

            @pl.when(u == 0)
            def _():
                normalize()
                project(slot, ((heads, qh, True),))

            @pl.when(u == 1)
            def _():
                project(slot, ((groups, kh, True), (groups, vh, False)))
                attend_half(0)

            @pl.when(u == 2)
            def _():
                attend_half(1)
                leave_attention(slot)

            @pl.when(u >= 3)
            def _():
                feed_forward(u - 3, slot)

    for hh in range(2):
        load(2, hh, 0).start()
    end(1)
    gain_sum[...] = jnp.zeros_like(gain_sum)

    def rows_back(rows):
        v = middle[rows, :]
        inverse = lax.rsqrt(jnp.mean(v * v, axis=1, keepdims=True) + EPSILON)
        unit, grad = v * inverse, grad_n2[rows, :]
        scaled = grad * gain[1:2, :]
        inner = jnp.mean(scaled * unit, axis=1, keepdims=True)
        total = ct[rows, :].astype(f32) + inverse * (scaled - unit * inner)
        grad_middle[rows, :] = total
        n1[rows, :] = total.astype(bf16)
        gain_sum[...] += jnp.sum(grad * unit, axis=0, keepdims=True)
        hidden_out[rows, :] = acc[rows, :].astype(bf16)

    each_rows(tokens, ROWS, rows_back)
    begin(3)
    for hh in range(2):
        load(2, hh, 0).wait()
        grad_mixed[:, hh * hw : (hh + 1) * hw] = dot_nn(n1[...], weight(0, hh))

    steps = count - 3
    for i in (0, 2, 3, 4):
        end(i)
    for cp in keeps:
        cp.wait()
    for j in range(max(steps - 2, 0), steps):
        drain_tiles(j)

    @pl.loop(0, steps)
    def _(j):
        for cp in tile_copies(j, 0)[1]:
            cp.wait_recv()

    g.finish()
    gg.finish()


def forward(line, shard, gains, hidden_in, cotangent, cosine, sine, block):
    tokens, d_model = hidden_in.shape
    rows, half = shard.shape
    width = 3 * block
    count = half // width
    steps = count - 3
    heads, groups = QUERY_HEADS // 2, KEY_VALUE_HEADS // 2
    bf16, f32 = jnp.bfloat16, jnp.float32
    struct = jax.ShapeDtypeStruct
    hbm, vmem = pl.BlockSpec(memory_space=pl.ANY), pl.BlockSpec(memory_space=pltpu.VMEM)
    dma = pltpu.SemaphoreType.DMA
    pair = struct((2, tokens, d_model), bf16)
    tile_pair = struct((2, tokens, steps * block), bf16)
    head_shape = lambda n: (n, tokens, HEAD_SIZE)
    slots = 2 * (line - 1) + 3
    outs = [
        struct((line, 2, 2, rows, 2 * half), bf16),
        struct((line, 2, 2) + gains.shape, bf16),
        struct(head_shape(2 * heads), bf16),
        struct(head_shape(2 * groups), bf16),
        struct(head_shape(2 * groups), bf16),
        struct((tokens, 2 * heads * HEAD_SIZE), bf16),
        pair,
        pair,
        pair,
        struct((2, tokens, heads * HEAD_SIZE), bf16),
        pair,
        tile_pair,
        tile_pair,
        tile_pair,
        struct((tokens, d_model), bf16),
        struct((tokens, d_model), f32),
        struct((tokens, 2 * heads * HEAD_SIZE), f32),
        struct((1, d_model), f32),
    ]
    V = pltpu.VMEM
    return pl.pallas_call(
        functools.partial(forward_kernel, line, width, block),
        out_shape=outs,
        in_specs=[vmem] * 6,
        out_specs=[hbm] * 14 + [vmem] * 4,
        scratch_shapes=[
            V((2, 2, line, 2, 2, rows, width), bf16),
            V((line, 2, 2) + gains.shape, bf16),
            V((8, d_model), f32),
            V((tokens, d_model), bf16),
            V((tokens, d_model), bf16),
            V((tokens, width), f32),
            V(head_shape(2 * heads), bf16),
            V(head_shape(2 * groups), bf16),
            V(head_shape(2 * groups), bf16),
            V(head_shape(2 * heads), bf16),
            V((tokens, 2 * heads * HEAD_SIZE), bf16),
            V((tokens, d_model), f32),
            V((tokens, d_model), f32),
            V((tokens, d_model), f32),
            V((3, tokens, block), f32),
            V((2, 2, 3, tokens, block), bf16),
            dma((count, 2, slots)),
            dma((count, 2, slots)),
            dma((1, 1, slots)),
            dma((1, 1, slots)),
            dma((2,)),
            dma((2, 2)),
            dma,
            dma((9,)),
            dma((5,)),
            dma((5,)),
            dma((steps, 3)),
            dma((steps, 3)),
            dma((steps, 3)),
        ],
        compiler_params=pltpu.CompilerParams(collective_id=0, has_side_effects=True, vmem_limit_bytes=64 * 2**20 - 2**17),
        name="gather_forward",
    )(shard, gains, hidden_in, cotangent, cosine, sine)


def against_kernel(grad, weight, out):
    part = dot_nt(grad[...], weight[...].reshape(out.shape[1], grad.shape[1]))

    @pl.when(pl.program_id(0) == 0)
    def _():
        out[...] = part

    @pl.when(pl.program_id(0) > 0)
    def _():
        out[...] += part


def against_columns(grad, full, width):
    tokens, columns = grad.shape
    line, rows = full.shape[0], full.shape[3]
    each, half = columns // 2 // width, full.shape[4] // 2 // width
    return pl.pallas_call(
        against_kernel,
        grid=(2 * each,),
        out_shape=jax.ShapeDtypeStruct((tokens, line * 4 * rows), jnp.float32),
        in_specs=[
            pl.BlockSpec((tokens, width), lambda i: (0, i)),
            pl.BlockSpec((line, 2, 2, rows, width), lambda i: (0, 0, 0, 0, (i // each) * half + i % each)),
        ],
        out_specs=pl.BlockSpec((tokens, line * 4 * rows), lambda i: (0, 0)),
        compiler_params=pltpu.CompilerParams(vmem_limit_bytes=40 * 2**20),
        name="against_columns",
    )(grad, full)


def norm_back(grad_normed, unit_rows, inverse_rms, gain):
    scaled = grad_normed * gain
    inner = jnp.mean(scaled * unit_rows, axis=1, keepdims=True)
    return (inverse_rms * (scaled - unit_rows * inner), jnp.sum(grad_normed * unit_rows, axis=0))


def cut(halves, width, mix):
    chunks, k = [], 0
    for w, half in enumerate(halves):
        pieces = -(-half // width)
        while half % (pieces * 128):
            pieces += 1
        for i in range(pieces):
            chunks.append((w, i * (half // pieces), half // pieces, mix[k % len(mix)]))
            k += 1
    return tuple(chunks)


GATHER_MIX = ("xyz", "zyx", "zxy", "yxz", "zyx", "zxy", "zyx", "zxy")
SCATTER_MIX = ("xyz", "yxz")


def layer(n_dp, n_tensor, hidden_in, query_weight, key_matrix, value_matrix, out_weight, gate_weight, up_weight, down_weight, attention_gain, feedforward_gain, cotangent):
    line = n_dp // 4
    rows = attention_gain.shape[0]
    width = rows * n_dp
    bf16, f32 = jnp.bfloat16, jnp.float32
    side = lax.axis_index("tensor")

    gains = jnp.zeros((8, 128), bf16).at[0, :rows].set(attention_gain).at[1, :rows].set(feedforward_gain)
    block = (query_weight.shape[1] // 3) & -128
    out_t, down_t = out_weight.T, down_weight.T
    pieces = [query_weight, key_matrix, value_matrix, out_t]
    for j in range(0, gate_weight.shape[1], block):
        pieces += [w[:, j : j + block] for w in (gate_weight, up_weight, down_t)]
    cosine, sine = rope_tables(SEQUENCE_LENGTH, HEAD_SIZE)
    (full, gains_full, q, k, v, mixed, n1, n2, ct, mixed_pair, gm, hidden, grad_gate_act, grad_up_act, hidden_out, grad_middle, grad_mixed, second_gain) = forward(
        line, jnp.concatenate(pieces, axis=1), gains, hidden_in, cotangent, cosine, sine, block
    )
    nq, nk = query_weight.shape[1], key_matrix.shape[1]
    gain_first = gains_full.reshape(n_dp, 8, 128)[:, 0, :rows].reshape(1, width).astype(f32)
    x = hidden_in.astype(f32)
    inverse_one = lax.rsqrt(jnp.mean(x * x, axis=1, keepdims=True) + EPSILON)
    unit_one = x * inverse_one
    grad_qkv_act = attend_back(q, k, v, mixed, grad_mixed, cosine, sine, n_tensor)
    grad_normed_one = against_columns(grad_qkv_act, full, 3 * block)
    first_part, first_gain = norm_back(grad_normed_one, unit_one, inverse_one, gain_first)
    grad_in = grad_middle + first_part

    swap = [(i, i ^ 1) for i in range(n_tensor)]
    other = lambda a: lax.ppermute(a, "tensor", swap)

    def of_half(a, which):
        size = a.shape[1] // n_tensor
        return lax.dynamic_slice_in_dim(a, which * size, size, axis=1)

    stack = lambda a: a.reshape(-1, a.shape[-1])
    qkv_pair = jnp.concatenate([of_half(grad_qkv_act, side), other(of_half(grad_qkv_act, 1 - side))], axis=0)
    weight_grad = lambda a, b: dot_tn(stack(a), b).astype(bf16)
    grads = [
        weight_grad(ct, stack(hidden)),
        weight_grad(n2, stack(grad_gate_act)),
        weight_grad(n2, stack(grad_up_act)),
        weight_grad(gm, stack(mixed_pair)),
        weight_grad(n1, qkv_pair),
    ]
    parts = jnp.stack([first_gain, second_gain[0]]).reshape(2, n_dp, rows).transpose(1, 0, 2)
    parts = jnp.pad(parts, ((0, 0), (0, 6), (0, 128 - rows))).astype(bf16)
    grads = [parts.reshape(line, 2, 2, 8, 128)] + [g.reshape(line, 2, 2, rows, g.shape[1]) for g in grads]
    g_gains, g_down, g_gate, g_up, g_out, g_qkv = scatter(line, cut([g.shape[-1] for g in grads], 512, SCATTER_MIX), grads, 1)
    return (
        hidden_out,
        grad_in,
        g_qkv[:, :nq],
        g_qkv[:, nq : nq + nk],
        g_qkv[:, nq + nk :],
        g_out.T,
        g_gate,
        g_up,
        g_down.T,
        g_gains[0, :rows],
        g_gains[1, :rows],
    )


def solution(mesh):
    split = P(("dp", "tensor"), None)
    row, column, gain = P("dp", "tensor"), P("tensor", "dp"), P("dp")
    return jax.shard_map(
        functools.partial(layer, mesh.shape["dp"], mesh.shape["tensor"]),
        mesh=mesh,
        in_specs=(split, row, row, row, column, row, row, column, gain, gain, split),
        out_specs=(split, split, row, row, row, column, row, row, column, gain, gain),
        check_vma=False,
    )
```

```python
import functools
import math

import jax
import jax.numpy as jnp
from jax import lax
from jax.experimental import pallas as pl
from jax.experimental.pallas import tpu as pltpu
from jax.sharding import PartitionSpec as P

QUERY_HEADS = 16
KEY_VALUE_HEADS = 8
HEAD_SIZE = 96
SEQUENCE_LENGTH = 512

EPSILON = 1e-05
THETA_BASE = 100000.0
MESH = pl.DeviceIdType.MESH


def place():
    d = lax.axis_index("dp")
    return lax.div(d, 4), lax.rem(lax.div(d, 2), 2), lax.rem(d, 2), lax.axis_index("tensor")


def dev(z, y, x, c):
    return (z * 4 + y * 2 + x, c)


def enter(line, pos):
    z, y, x, c = pos
    barrier = pltpu.get_barrier_semaphore()

    def greet(who):
        pl.semaphore_signal(barrier, inc=1, device_id=who, device_id_type=MESH)

    greet(dev(z, y, x, 1 - c))
    greet(dev(z, y, 1 - x, c))
    greet(dev(z, 1 - y, x, c))

    @pl.when(z > 0)
    def _():
        greet(dev(z - 1, y, x, c))

    @pl.when(z < line - 1)
    def _():
        greet(dev(z + 1, y, x, c))

    pl.semaphore_wait(barrier, 3 + (z > 0).astype(jnp.int32) + (z < line - 1).astype(jnp.int32))


def remote(src, dst, send, recv, who):
    return pltpu.make_async_remote_copy(src_ref=src, dst_ref=dst, send_sem=send, recv_sem=recv, device_id=who, device_id_type=MESH)


class Gather:
    def __init__(self, line, pos, shard, full, width, orders, paired, send, recv):
        self.line, self.pos, self.shard, self.full, self.width = line, pos, shard, full, width
        self.orders, self.paired, self.send, self.recv = orders, paired, send, recv
        self.count = shard.shape[-1] // width
        self.depth = line + 1 + paired

    def columns(self, t, sub):
        part = self.width // len(self.orders[0])
        return t * self.width + sub * part, part

    def region(self, t, sub, have, z=None):
        first, part = self.columns(t, sub)
        pz, py, px, c = self.pos
        if self.paired:
            first = first + c * self.shard.shape[-1]
        every = slice(None)
        zi = z if z is not None else (every if "z" in have else pz)
        cols = pl.ds(pl.multiple_of(first, 128), part)
        return self.full.at[zi, every if "y" in have else py, every if "x" in have else px, :, cols]

    def own(self, t, sub):
        first, part = self.columns(t, sub)
        return self.shard.at[:, pl.ds(pl.multiple_of(first, 128), part)]

    def copy(self, t, sub, slot, src, dst, who):
        return remote(src, dst, self.send.at[t, sub, slot], self.recv.at[t, sub, slot], who)

    def hop(self, t, sub, h, up, have, what):
        z, y, x, c = self.pos
        slot = (h - 1) * 2 + up
        if up:
            block, incoming, who = z - (h - 1), z - h, dev(z + 1, y, x, c)
            there, here = (z + 1 < self.line) & (z >= h - 1), z >= h
        else:
            block, incoming, who = z + (h - 1), z + h, dev(z - 1, y, x, c)
            there, here = (z > 0) & (z + h - 1 < self.line), z + h < self.line

        @pl.when(here if what == "recv" else there)
        def _():
            if what == "recv":
                r = self.region(t, sub, have, incoming)
                self.copy(t, sub, slot, r, r, dev(z, y, x, 1 - c)).wait_recv()
                return
            r = self.region(t, sub, have, block)
            cp = self.copy(t, sub, slot, self.own(t, sub) if h == 1 and not have else r, r, who)
            cp.start() if what == "start" else cp.wait_send()

    def act(self, t, sub, order, i, what):
        z, y, x, c = self.pos
        moves, have = [], ""
        for axis in order:
            moves += [(axis, h, have) for h in (range(1, self.line) if axis == "z" else (0,))]
            have += axis
        if self.paired:
            moves.append(("c", 0, have))
        axis, h, have = moves[i]
        if axis == "z":
            for up in (1, 0):
                self.hop(t, sub, h, up, have, what)
            return
        who = {"y": dev(z, 1 - y, x, c), "x": dev(z, y, 1 - x, c), "c": dev(z, y, x, 1 - c)}[axis]
        land = self.region(t, sub, have)
        cp = self.copy(t, sub, 2 * (self.line - 1) + "yxc".index(axis), land if have else self.own(t, sub), land, who)
        {"start": cp.start, "recv": cp.wait_recv, "sent": cp.wait_send}[what]()

    def each(self, t, fn):
        there = (t >= 0) & (t < self.count)
        for v, orders in enumerate(self.orders):
            turn_of = there if len(self.orders) == 1 else there & ((lax.rem(t + 4, 4) == 0) == (v == 1))

            @pl.when(turn_of)
            def _():
                for sub, order in enumerate(orders):
                    fn(sub, order)

    def step(self, t, s):
        def go(sub, order):
            if s > 0:
                self.act(t, sub, order, s - 1, "recv")
            if s < self.depth:
                self.act(t, sub, order, s, "start")

        self.each(t, go)

    def advance(self, p):
        for s in range(self.depth + 1):
            self.step(p - s, s)

    def finish(self):
        @pl.loop(0, self.count)
        def _(t):
            self.each(t, lambda sub, order: [self.act(t, sub, order, i, "sent") for i in range(self.depth)])


def own_copy(g, sem):
    z, y, x, c = g.pos
    first = c * g.shard.shape[-1] if g.paired else 0
    return pltpu.make_async_copy(g.shard, g.full.at[z, y, x, :, pl.ds(pl.multiple_of(first, 128), g.shard.shape[-1])], sem)


def rope_tables(length, width):
    half_width = width // 2
    inverse = THETA_BASE ** (-(jnp.arange(half_width, dtype=jnp.float32) * 2.0 / width))
    angles = jnp.arange(length, dtype=jnp.float32)[:, None] * inverse[None, :]
    cosine, sine = jnp.cos(angles), jnp.sin(angles)
    return jnp.concatenate([cosine, cosine], axis=1), jnp.concatenate([-sine, sine], axis=1)


def turn(x, cosine, sine):
    half = x.shape[-1] // 2
    return x * cosine + jnp.concatenate([x[:, half:], x[:, :half]], axis=1) * sine


def dot_nt(a, b):
    return lax.dot_general(a, b, (((1,), (1,)), ((), ())), preferred_element_type=jnp.float32)


def dot_tn(a, b):
    return lax.dot_general(a, b, (((0,), (0,)), ((), ())), preferred_element_type=jnp.float32)


def dot_nn(a, b):
    return jnp.dot(a, b, preferred_element_type=jnp.float32)


BLOCK = 128


def causal_weights(q, k, b, heads):
    scores = dot_nt(q, k) * (1.0 / math.sqrt(HEAD_SIZE))
    n = scores.shape[1]
    row = lax.broadcasted_iota(jnp.int32, scores.shape, 0) % BLOCK + b * BLOCK
    keep = row >= lax.broadcasted_iota(jnp.int32, scores.shape, 1)
    scores = jnp.where(keep, scores, -jnp.inf)
    log_total = jnp.log(jnp.sum(jnp.exp(scores), axis=1, keepdims=True))
    return jnp.exp(scores - log_total)


def rows_of(ref, first, heads, rows):
    return jnp.concatenate([ref[first + i, rows] for i in range(heads)], axis=0)


ROWS = 128


def each_rows(tokens, step, fn):
    @pl.loop(0, tokens // step)
    def _(r):
        fn(pl.ds(pl.multiple_of(r * step, step), step))


def forward_kernel(line, width, block, *refs):
    refs = list(refs)
    take = lambda n: [refs.pop(0) for _ in range(n)]
    query_in, key_in, value_in, gate_in, up_in, out_in, down_in, gain_a, gain_b, hid, ct, cosine, sine = take(13)
    full, gains_full, q_out, k_out, v_out, mixed_out, n1_pair, n2_pair, ct_pair, mixed_pair, gm_pair = take(11)
    tile_pairs = take(3)
    hidden_out, grad_middle, grad_mixed, gain_sum, gain = take(5)
    wbuf, gain_buf, n1, n2, flat, qh, kh, vh, mh, mixed, middle, acc, grad_n2, act, tiles, shard, gains, turned = take(18)
    send, recv, gsend, grecv, own_sem, load_sem, gain_sem, local_sem, pair_send, pair_recv, tile_local, tile_send, tile_recv, shard_sem = take(14)

    pos = place()
    z, y, x, c = pos
    tokens, d_model = hid.shape
    half = shard.shape[-1]
    heads, groups = qh.shape[0] // 2, kh.shape[0] // 2
    sibling = dev(z, y, x, 1 - c)
    bf16, f32 = jnp.bfloat16, jnp.float32

    g = Gather(line, pos, shard, full, width, (("zyx", "zxy"), ("xyz", "yxz")), 1, send, recv)
    gg = Gather(line, pos, gains, gains_full, gains.shape[-1], (("zyx",),), 0, gsend, grecv)
    g_own, gg_own = own_copy(g, own_sem.at[0]), own_copy(gg, own_sem.at[1])
    steps = (half // width) - 3
    fills, at = [], 0
    for src in (query_in, key_in, value_in):
        fills.append((src, at, src.shape[1]))
        at += src.shape[1]
    out_at, at = at, at + out_in.shape[0]
    for j in range(steps):
        for i, src in enumerate((gate_in, up_in)):
            fills.append((src.at[:, pl.ds(j * block, block)], at + j * width + i * block, block))
    fills = [pltpu.make_async_copy(src, shard.at[:, pl.ds(to, n)], shard_sem.at[i]) for i, (src, to, n) in enumerate(fills)]
    for cp in fills:
        cp.start()
    gains[...] = jnp.zeros_like(gains)
    top = lax.broadcasted_iota(jnp.int32, (gains.shape[0], gain_a.shape[1]), 0) == 0
    gains[:, : gain_a.shape[1]] = jnp.where(top, gain_a[...].astype(f32), gain_b[...].astype(f32)).astype(bf16)
    shard[:, out_at:at] = out_in[...].T
    for j in range(steps):
        shard[:, at + j * width + 2 * block : at + (j + 1) * width] = down_in[j * block : (j + 1) * block, :].T
    enter(line, pos)
    for cp in fills:
        cp.wait()
    g_own.start()
    gg_own.start()

    def load(t, hh, slot):
        cols = pl.ds(pl.multiple_of(hh * half + t * width, 128), width)
        return pltpu.make_async_copy(full.at[:, :, :, :, cols], wbuf.at[slot, hh], load_sem.at[slot, hh])

    def weight(slot, hh):
        return wbuf[slot, hh].reshape(d_model, width)

    def share(i, own_src, own_dst, other_src, other_dst):
        return pltpu.make_async_copy(own_src, own_dst, local_sem.at[i]), remote(other_src, other_dst, pair_send.at[i], pair_recv.at[i], sibling)

    ends = (pl.ds(0, tokens), pl.ds(tokens, tokens))
    lefts = ((ct, ct_pair), (n1, n1_pair), (n2, n2_pair), (n1, gm_pair))
    shares = [share(i, turned.at[i], pair.at[:, ends[0]], turned.at[i], pair.at[:, ends[1]]) for i, (_, pair) in enumerate(lefts)]
    hw = mixed.shape[1] // 2
    side = lambda ref, s, w: ref.at[:, pl.ds(pl.multiple_of(s * w, 128), w)]
    shares.append(share(4, side(mixed, c, hw), mixed_pair.at[0], side(mixed, 1 - c, hw), mixed_pair.at[1]))
    keeps = [pltpu.make_async_copy(src, dst, local_sem.at[5 + i]) for i, (src, dst) in enumerate(((qh, q_out), (kh, k_out), (vh, v_out), (mixed, mixed_out)))]

    def begin(i):
        if i < len(lefts):
            span = 256

            @pl.loop(0, d_model // span)
            def _(e):
                at = pl.ds(pl.multiple_of(e * span, span), span)
                turned[i, at, :] = lefts[i][0][:, at].T

        for cp in shares[i]:
            cp.start()

    def end(i):
        for cp in shares[i]:
            cp.wait()

    def tile_copies(j, hh):
        slot = lax.rem(j, 2)
        cols = pl.ds(pl.multiple_of(j * block, 128), block)
        own = [pltpu.make_async_copy(tiles.at[slot, hh, i], pair.at[0, :, cols], tile_local.at[j, i]) for i, pair in enumerate(tile_pairs)]
        out = [remote(tiles.at[slot, hh, i], pair.at[1, :, cols], tile_send.at[j, i], tile_recv.at[j, i], sibling) for i, pair in enumerate(tile_pairs)]
        return own, out

    def drain_tiles(j):
        for cp in tile_copies(j, 0)[0]:
            cp.wait()
        for cp in tile_copies(j, 0)[1]:
            cp.wait_send()

    def normalize():
        loaded = pltpu.make_async_copy(gains_full, gain_buf, gain_sem)
        loaded.start()
        loaded.wait()
        n = d_model // (gain_buf.shape[0] * 4)
        table = gain_buf[...].astype(f32)
        for i in range(2):
            gain[i : i + 1, :] = jnp.concatenate([table[a, b, e, i : i + 1, :n] for a in range(gain_buf.shape[0]) for b in range(2) for e in range(2)], axis=1)

        def rows_of_norm(rows):
            v = hid[rows, :].astype(f32)
            v = v * lax.rsqrt(jnp.mean(v * v, axis=1, keepdims=True) + EPSILON)
            n1[rows, :] = (v * gain[0:1, :]).astype(bf16)

        each_rows(tokens, ROWS, rows_of_norm)
        begin(1)

    def project(slot, outs):
        @pl.loop(0, 2)
        def _(hh):
            flat[...] = dot_nn(n1[...], weight(slot, hh))

            def to_heads(rows):
                cos, sin = cosine[rows, :], sine[rows, :]
                first = 0
                for n, target, turned in outs:
                    for h in range(n):
                        v = flat[rows, (first + h) * HEAD_SIZE : (first + h + 1) * HEAD_SIZE]
                        target[hh * n + h, rows] = (turn(v, cos, sin) if turned else v).astype(bf16)
                    first += n

            each_rows(tokens, ROWS, to_heads)

    def attend_half(hh):
        per = heads // groups
        blocks = tokens // BLOCK

        @pl.loop(0, groups)
        def _(i):
            kv = hh * groups + i
            for b in range(blocks):
                rows, n = pl.ds(b * BLOCK, BLOCK), (b + 1) * BLOCK
                w = causal_weights(rows_of(qh, kv * per, per, rows), kh[kv, :n], b, per).astype(bf16)
                m = dot_nn(w, vh[kv, :n]).astype(bf16)
                for e in range(per):
                    mh[kv * per + e, rows] = m[e * BLOCK : (e + 1) * BLOCK]

    def leave_attention(slot):
        def join(rows):
            mixed[rows, :] = jnp.concatenate([mh[h, rows] for h in range(2 * heads)], axis=1)

        each_rows(tokens, ROWS, join)
        begin(4)
        for cp in keeps:
            cp.start()
        middle[...] = hid[...].astype(f32) + dot_nt(mixed[:, :hw], weight(slot, 0))
        middle[...] += dot_nt(mixed[:, hw:], weight(slot, 1))

        def rows_of_norm(rows):
            v = middle[rows, :]
            acc[rows, :] = v
            v = v * lax.rsqrt(jnp.mean(v * v, axis=1, keepdims=True) + EPSILON)
            n2[rows, :] = (v * gain[1:2, :]).astype(bf16)
            grad_n2[rows, :] = jnp.zeros_like(v)

        each_rows(tokens, ROWS, rows_of_norm)
        begin(2)

    def feed_forward(j, slot):
        @pl.when(j >= 2)
        def _():
            drain_tiles(j - 2)

        part = lax.rem(j, 2)

        @pl.loop(0, 2)
        def _(hh):
            act[0] = dot_nn(n2[...], weight(slot, hh)[:, :block])
            act[1] = dot_nn(n2[...], weight(slot, hh)[:, block : 2 * block])
            act[2] = dot_nn(ct[...], weight(slot, hh)[:, 2 * block :])

            def gated(rows):
                gate, up, grad = act[0, rows], act[1, rows], act[2, rows]
                sigma = jax.nn.sigmoid(gate)
                tiles[part, hh, 0, rows] = (gate * sigma * up).astype(bf16)
                tiles[part, hh, 1, rows] = (grad * up * sigma * (1.0 + gate * (1.0 - sigma))).astype(bf16)
                tiles[part, hh, 2, rows] = (grad * gate * sigma).astype(bf16)

            each_rows(tokens, ROWS // 2, gated)
            own, out = tile_copies(j, hh)

            @pl.when(hh == c)
            def _():
                for cp in own:
                    cp.start()

            @pl.when(hh != c)
            def _():
                for cp in out:
                    cp.start()

            acc[...] += dot_nt(tiles[part, hh, 0], weight(slot, hh)[:, 2 * block :])
            both = jnp.concatenate([tiles[part, hh, 1], tiles[part, hh, 2]], axis=1)
            grad_n2[...] += dot_nt(both, weight(slot, hh)[:, : 2 * block])

    count, lead = g.count, g.depth + 1

    @pl.loop(0, count + lead)
    def _(p):
        @pl.when(p == 0)
        def _():
            g_own.wait()
            gg_own.wait()
            begin(0)

        gg.advance(p)
        g.advance(p)
        u = p - lead

        @pl.when((u >= -1) & (u + 1 < count))
        def _():
            for hh in range(2):
                load(u + 1, hh, lax.rem(u + 1, 2)).start()

        @pl.when(u >= 0)
        def _():
            slot = lax.rem(u, 2)
            for hh in range(2):
                load(u, hh, slot).wait()

            @pl.when(u == 0)
            def _():
                normalize()
                project(slot, ((heads, qh, True),))

            @pl.when(u == 1)
            def _():
                project(slot, ((groups, kh, True), (groups, vh, False)))
                attend_half(0)

            @pl.when(u == 2)
            def _():
                attend_half(1)
                leave_attention(slot)

            @pl.when(u >= 3)
            def _():
                feed_forward(u - 3, slot)

    for hh in range(2):
        load(2, hh, 0).start()
    gain_sum[...] = jnp.zeros_like(gain_sum)

    def rows_back(rows):
        v = middle[rows, :]
        inverse = lax.rsqrt(jnp.mean(v * v, axis=1, keepdims=True) + EPSILON)
        unit, grad = v * inverse, grad_n2[rows, :]
        scaled = grad * gain[1:2, :]
        inner = jnp.mean(scaled * unit, axis=1, keepdims=True)
        total = ct[rows, :].astype(f32) + inverse * (scaled - unit * inner)
        grad_middle[rows, :] = total
        n1[rows, :] = total.astype(bf16)
        gain_sum[...] += jnp.sum(grad * unit, axis=0, keepdims=True)
        hidden_out[rows, :] = acc[rows, :].astype(bf16)

    each_rows(tokens, ROWS, rows_back)
    begin(3)
    for hh in range(2):
        load(2, hh, 0).wait()
        grad_mixed[:, hh * hw : (hh + 1) * hw] = dot_nn(n1[...], weight(0, hh))

    for i in (0, 1, 2, 3, 4):
        end(i)
    for cp in keeps:
        cp.wait()
    for j in range(max(steps - 2, 0), steps):
        drain_tiles(j)

    @pl.loop(0, steps)
    def _(j):
        for cp in tile_copies(j, 0)[1]:
            cp.wait_recv()

    g.finish()
    gg.finish()


def forward(line, shards, gain_pair, hidden_in, cotangent, cosine, sine, block):
    tokens, d_model = hidden_in.shape
    rows = gain_pair[0].shape[1]
    half = sum(s.shape[1] for s in shards[:5]) + sum(s.shape[0] for s in shards[5:])
    gains = jax.ShapeDtypeStruct((8, 128), jnp.bfloat16)
    width = 3 * block
    count = half // width
    steps = count - 3
    heads, groups = QUERY_HEADS // 2, KEY_VALUE_HEADS // 2
    bf16, f32 = jnp.bfloat16, jnp.float32
    struct = jax.ShapeDtypeStruct
    hbm, vmem = pl.BlockSpec(memory_space=pl.ANY), pl.BlockSpec(memory_space=pltpu.VMEM)
    dma = pltpu.SemaphoreType.DMA
    pair = struct((d_model, 2 * tokens), bf16)
    tile_pair = struct((2, tokens, steps * block), bf16)
    head_shape = lambda n: (n, tokens, HEAD_SIZE)
    slots = 2 * (line - 1) + 3
    outs = [
        struct((line, 2, 2, rows, 2 * half), bf16),
        struct((line, 2, 2) + gains.shape, bf16),
        struct(head_shape(2 * heads), bf16),
        struct(head_shape(2 * groups), bf16),
        struct(head_shape(2 * groups), bf16),
        struct((tokens, 2 * heads * HEAD_SIZE), bf16),
        pair,
        pair,
        pair,
        struct((2, tokens, heads * HEAD_SIZE), bf16),
        pair,
        tile_pair,
        tile_pair,
        tile_pair,
        struct((tokens, d_model), bf16),
        struct((tokens, d_model), f32),
        struct((tokens, 2 * heads * HEAD_SIZE), f32),
        struct((1, d_model), f32),
        struct((8, d_model), f32),
    ]
    V = pltpu.VMEM
    return pl.pallas_call(
        functools.partial(forward_kernel, line, width, block),
        out_shape=outs,
        in_specs=[hbm] * 5 + [vmem] * 8,
        out_specs=[hbm] * 14 + [vmem] * 5,
        scratch_shapes=[
            V((2, 2, line, 2, 2, rows, width), bf16),
            V((line, 2, 2) + gains.shape, bf16),
            V((tokens, d_model), bf16),
            V((tokens, d_model), bf16),
            V((tokens, width), f32),
            V(head_shape(2 * heads), bf16),
            V(head_shape(2 * groups), bf16),
            V(head_shape(2 * groups), bf16),
            V(head_shape(2 * heads), bf16),
            V((tokens, 2 * heads * HEAD_SIZE), bf16),
            V((tokens, d_model), f32),
            V((tokens, d_model), f32),
            V((tokens, d_model), f32),
            V((3, tokens, block), f32),
            V((2, 2, 3, tokens, block), bf16),
            V((rows, half), bf16),
            V(gains.shape, bf16),
            V((4, d_model, tokens), bf16),
            dma((count, 2, slots)),
            dma((count, 2, slots)),
            dma((1, 1, slots)),
            dma((1, 1, slots)),
            dma((2,)),
            dma((2, 2)),
            dma,
            dma((9,)),
            dma((5,)),
            dma((5,)),
            dma((steps, 3)),
            dma((steps, 3)),
            dma((steps, 3)),
            dma((3 + 2 * steps,)),
        ],
        compiler_params=pltpu.CompilerParams(collective_id=0, has_side_effects=True, vmem_limit_bytes=64 * 2**20 - 2**17),
        name="gather_forward",
    )(*shards, *gain_pair, hidden_in, cotangent, cosine, sine)


class Scatter:
    def __init__(self, line, pos, count, own, first, second, up, down, send, recv, final):
        self.line, self.pos, self.count, self.final = line, pos, count, final
        self.own, self.first, self.second, self.up, self.down, self.send, self.recv = own, first, second, up, down, send, recv
        self.ring, self.own_ring = first.shape[0], own.shape[0]
        self.lags = [0, 2, 4] + [5 + j for j in range(line - 1)] + [4 + line, 5 + line]
        self.depth = self.lags[-1]

    def copy(self, t, slot, src, dst, who):
        r = lax.rem(t, self.ring)
        return remote(src, dst, self.send.at[r, slot], self.recv.at[r, slot], who)

    def merge(self, dst, a, b, loops):
        def go(lead, rest):
            if not rest:
                dst[lead] = a[lead] + b[lead]
            elif rest[0] > 2:
                @pl.loop(0, rest[0])
                def _(i):
                    go(lead + (i,), rest[1:])
            else:
                for i in range(rest[0]):
                    go(lead + (i,), rest[1:])

        go((), loops)

    def pair_moves(self, t, v):
        z, y, x, c = self.pos
        r, o = lax.rem(t, self.ring), lax.rem(t, self.own_ring)
        own, first, second = self.own.at[o], self.first.at[r], self.second.at[r]
        over_x, over_y = dev(z, y, 1 - x, c), dev(z, 1 - y, x, c)
        if v == 0:
            give, keep, who = own.at[:, :, 1 - x], own.at[:, :, x], (over_x, over_y)
        else:
            give, keep, who = own.at[:, 1 - y], own.at[:, y], (over_y, over_x)
        a, b = (1 - y, y) if v == 0 else (1 - x, x)
        one = self.copy(t, 0, give, first, who[0])
        two = self.copy(t, 1, first.at[:, a], second, who[1])
        return one, two, keep, first, second, first.at[:, b]

    def hop(self, t, j):
        z, y, x, c = self.pos
        r = lax.rem(t, self.ring)
        cur = self.second.at[r]
        for way, ref, target, edge in ((0, self.up.at[r, j], self.line - 1 - j, z == 0), (1, self.down.at[r, j], j, z == self.line - 1)):
            nxt = dev(z + 1, y, x, c) if way == 0 else dev(z - 1, y, x, c)
            passes = (target > z) if way == 0 else (target < z)

            @pl.when(passes & edge)
            def _():
                self.copy(t, 2 + 2 * j + way, cur.at[target], ref, nxt).start()

            @pl.when(passes & ~edge)
            def _():
                cp = self.copy(t, 2 + 2 * j + way, ref, ref, nxt)
                cp.wait_recv()
                ref[...] = ref[...] + cur[target]
                cp.start()

    def close(self, t):
        z, y, x, c = self.pos
        r = lax.rem(t, self.ring)
        ku, kd = self.line - 1 - z, z
        has_up, has_down = z > 0, z < self.line - 1
        for has, way, ref, k in ((has_up, 0, self.up, ku), (has_down, 1, self.down, kd)):

            @pl.when(has)
            def _():
                self.copy(t, 2 + 2 * k + way, ref.at[r, k], ref.at[r, k], dev(z, y, x, 1 - c)).wait_recv()

        f32 = jnp.float32
        total = self.second[r, z].astype(f32)
        last = self.line - 2
        below = self.up[r, jnp.minimum(ku, last)].astype(f32)
        above = self.down[r, jnp.minimum(kd, last)].astype(f32)
        total = total + jnp.where(has_up, below, 0.0) + jnp.where(has_down, above, 0.0)
        self.final(t, total)

    def drain(self, t):
        z, y, x, c = self.pos
        r = lax.rem(t, self.ring)
        self.pair_moves(t, 0)[1].wait_send()
        for j in range(self.line - 1):
            for way, ref, target in ((0, self.up, self.line - 1 - j), (1, self.down, j)):

                @pl.when((target > z) if way == 0 else (target < z))
                def _():
                    self.copy(t, 2 + 2 * j + way, ref.at[r, j], ref.at[r, j], dev(z, y, x, 1 - c)).wait_send()

    def when(self, t, fn):
        @pl.when((t >= 0) & (t < self.count))
        def _():
            fn()

    def both(self, t, fn):
        for v in range(2):
            @pl.when((t >= 0) & (t < self.count) & (lax.rem(t + 2, 2) == v))
            def _():
                fn(v)

    def begin(self, t):
        self.both(t, lambda v: self.pair_moves(t, v)[0].start())

    def release(self, t):
        self.when(t, lambda: self.pair_moves(t, 0)[0].wait_send())

    def advance(self, p):
        line = self.line

        def one(v, t):
            first_copy, second_copy, keep, first, second, _ = self.pair_moves(t, v)
            first_copy.wait_recv()
            self.merge(first, first, keep, (line, 2))
            second_copy.start()

        def two(v, t):
            _, second_copy, _, _, second, keep = self.pair_moves(t, v)
            second_copy.wait_recv()
            self.merge(second, second, keep, (line,))

        t = p - self.lags[1]
        self.both(t, lambda v, t=t: one(v, t))
        t = p - self.lags[2]
        self.both(t, lambda v, t=t: two(v, t))
        for j in range(line - 1):
            t = p - self.lags[3 + j]
            self.when(t, lambda t=t, j=j: self.hop(t, j))
        t = p - self.lags[-2]
        self.when(t, lambda t=t: self.close(t))
        t = p - self.lags[-1]
        self.when(t, lambda t=t: self.drain(t))


def greet_all(n, pos):
    z, y, x, c = pos
    d = z * 4 + y * 2 + x
    barrier = pltpu.get_barrier_semaphore()

    @pl.loop(1, n)
    def _(i):
        pl.semaphore_signal(barrier, inc=1, device_id=(lax.rem(d + i, n), c), device_id_type=MESH)

    pl.semaphore_signal(barrier, inc=1, device_id=(d, 1 - c), device_id_type=MESH)
    pl.semaphore_wait(barrier, n)


def backward_kernel(line, cols, starts, *refs):
    refs = list(refs)
    take = lambda n: [refs.pop(0) for _ in range(n)]
    q, k, v, mixed, grad_mixed, full, hid, grad_middle, gains, gain_two, cosine, sine = take(12)
    n1_pair, n2_pair, ct_pair, gm_pair, mixed_pair, hidden_pair, gate_pair, up_pair = take(8)
    qkv_pair, grad_query, grad_key, grad_value, grad_in, out_out, out_gate, out_up, out_down, out_gains = take(10)
    own, first, second, up, down, xt, ybuf, qh, kh, vh, mh, gh, gm, dots, dq, dk, dv, dqkv, wbuf, gmid, hbuf, out_qkv, gain_one, part, parts_in, pair_in = take(26)
    send, recv, xsem, ysem, half_sem, wsem, msem, qkv_local, qkv_send, qkv_recv, part_send, part_recv, out_sem, swap_sem = take(14)

    pos = place()
    z, y, x, c = pos
    d = z * 4 + y * 2 + x
    n = line * 4
    tokens, d_model = hid.shape
    count = starts[-1]
    heads, groups = qh.shape[0], kh.shape[0]
    share = heads // groups
    blocks = tokens // BLOCK
    width = wbuf.shape[-1]
    half_width = dqkv.shape[1] // 2
    scale = 1.0 / math.sqrt(HEAD_SIZE)
    bf16, f32 = jnp.bfloat16, jnp.float32
    sources = (hidden_pair, gate_pair, up_pair, mixed_pair, qkv_pair)
    lefts = ((0, ct_pair), (starts[1], n2_pair), (starts[3], gm_pair), (starts[4], n1_pair))

    def final(t, total):
        for i, (out, turned) in enumerate(((out_down, True), (out_gate, False), (out_up, False), (out_out, True), (out_qkv, False))):
            at = pl.ds(pl.multiple_of((t - starts[i]) * cols, 128), cols)

            @pl.when((t >= starts[i]) & (t < starts[i + 1]))
            def _():
                if turned:
                    out[at, :] = total.T
                else:
                    out[:, at] = total

    s = Scatter(line, pos, count, own, first, second, up, down, send, recv, final)

    def load_left(i):
        return pltpu.make_async_copy(lefts[i][1], xt.at[i % 2], xsem.at[i % 2])

    def load_right(t, act):
        slot = lax.rem(t, 2)
        for i, src in enumerate(sources):
            at = pl.ds(pl.multiple_of((t - starts[i]) * cols, 128), cols)

            @pl.when((t >= starts[i]) & (t < starts[i + 1]))
            def _():
                cp = pltpu.make_async_copy(src.at[:, :, at], ybuf.at[slot], ysem.at[slot])
                cp.start() if act == "start" else cp.wait()

    def half_loads(hh):
        take_heads = lambda ref, m: ref.at[pl.ds(hh * m, m)]
        lanes = pl.ds(pl.multiple_of(hh * mh.shape[1], 128), mh.shape[1])
        pairs = ((take_heads(q, heads), qh), (take_heads(k, groups), kh), (take_heads(v, groups), vh), (mixed.at[:, lanes], mh), (grad_mixed.at[:, lanes], gh))
        return [pltpu.make_async_copy(src, dst, half_sem.at[i]) for i, (src, dst) in enumerate(pairs)]

    def half_load(hh, act):
        for cp in half_loads(hh):
            cp.start() if act == "start" else cp.wait()

    each = half_width // width
    half_columns = full.shape[-1] // 2

    def weights(i):
        at = pl.ds(pl.multiple_of((i // each) * half_columns + (i % each) * width, 128), width)
        return pltpu.make_async_copy(full.at[:, :, :, :, at], wbuf.at[i % 2], wsem.at[i % 2])

    others = [pltpu.make_async_copy(grad_middle, gmid, msem.at[0]), pltpu.make_async_copy(hid, hbuf, msem.at[1])]

    own_half = lambda ref, which: ref.at[:, pl.ds(pl.multiple_of(which * half_width, 128), half_width)]

    def qkv_copies():
        return (
            pltpu.make_async_copy(own_half(dqkv, c), qkv_pair.at[0], qkv_local),
            remote(own_half(dqkv, 1 - c), qkv_pair.at[1], qkv_send, qkv_recv, (d, 1 - c)),
        )

    def prepare(hh):
        half_load(hh, "wait")

        def rows_of_dots(rows):
            for h in range(heads):
                lanes = slice(h * HEAD_SIZE, (h + 1) * HEAD_SIZE)
                g = gh[rows, lanes]
                dots[h, rows] = jnp.sum(g * mh[rows, lanes].astype(f32), axis=1, keepdims=True)
                gm[h, rows] = g.astype(bf16)

        each_rows(tokens, ROWS, rows_of_dots)
        dk[...] = jnp.zeros_like(dk)
        dv[...] = jnp.zeros_like(dv)

    def group_back(g, which):
        for b in which:
            rows, m = pl.ds(b * BLOCK, BLOCK), (b + 1) * BLOCK
            qb, gb, db = (rows_of(ref, g * share, share, rows) for ref in (qh, gm, dots))
            kb, vb = kh[g, :m], vh[g, :m]
            p = causal_weights(qb, kb, b, share)
            ds = (p * (dot_nt(gb, vb) - db)).astype(bf16)
            dv[g, :m] += dot_tn(p.astype(bf16), gb)
            dk[g, :m] += dot_tn(ds, qb)
            r = dot_nn(ds, kb) * scale
            for i in range(share):
                dq[g * share + i, rows] = r[i * BLOCK : (i + 1) * BLOCK]

    def join(hh):
        def rows_of_join(rows):
            cos, sin = cosine[rows, :], -sine[rows, :]
            parts = [turn(dq[h, rows], cos, sin) for h in range(heads)]
            parts += [turn(dk[g, rows] * scale, cos, sin) for g in range(groups)]
            parts += [dv[g, rows] for g in range(groups)]
            dqkv[rows, pl.ds(pl.multiple_of(hh * half_width, 128), half_width)] = jnp.concatenate([a.astype(bf16) for a in parts], axis=1)

        each_rows(tokens, ROWS, rows_of_join)

    def against(i):
        weights(i).wait()
        r = dot_nt(dqkv[:, i * width : (i + 1) * width], wbuf[i % 2].reshape(d_model, width))
        if i == 0:
            grad_in[...] = r
        else:
            grad_in[...] += r
        if i + 2 < 2 * each:
            weights(i + 2).start()

    def norm_one_back():
        for cp in others:
            cp.wait()
        gain_one[...] = jnp.zeros_like(gain_one)

        def rows_back(rows):
            a = hbuf[rows, :].astype(f32)
            inverse = lax.rsqrt(jnp.mean(a * a, axis=1, keepdims=True) + EPSILON)
            unit, grad = a * inverse, grad_in[rows, :]
            scaled = grad * gains[0:1, :]
            inner = jnp.mean(scaled * unit, axis=1, keepdims=True)
            grad_in[rows, :] = gmid[rows, :] + inverse * (scaled - unit * inner)
            gain_one[...] += jnp.sum(grad * unit, axis=0, keepdims=True)

        each_rows(tokens, ROWS, rows_back)
        size = d_model // n
        part[...] = jnp.zeros_like(part)
        for i in range(n):
            for row, ref in enumerate((gain_one, gain_two)):
                part[i, row : row + 1, :size] = ref[:, i * size : (i + 1) * size]

    def part_copy(i):
        to = lax.rem(d + i, n)
        return remote(part.at[to], parts_in.at[i], part_send.at[i], part_recv.at[i], (to, c))

    load_left(0).start()
    load_left(1).start()
    load_right(0, "start")
    half_load(0, "start")
    for cp in others:
        cp.start()
    for i in range(2):
        weights(i).start()
    greet_all(n, pos)

    stages = 2 * groups + 2
    turns = 2 * stages
    norm_at = turns + 2 * each

    @pl.loop(0, count + s.depth)
    def _(p):
        s.release(p - s.own_ring)
        for i, (at, _) in enumerate(lefts):

            @pl.when(p == at)
            def _():
                load_left(i).wait()
                if 1 <= i < len(lefts) - 1:
                    load_left(i + 1).start()

        @pl.when(p == starts[4] - 2)
        def _():
            for cp in qkv_copies():
                cp.wait()

        @pl.when(p < count)
        def _():
            load_right(p, "wait")

            @pl.when(p + 1 < count)
            def _():
                load_right(p + 1, "start")

            side = lax.rem(sum((p >= at).astype(jnp.int32) for at, _ in lefts[1:]), 2)
            right = ybuf[lax.rem(p, 2)].reshape(2 * tokens, cols)
            own[lax.rem(p, s.own_ring)] = dot_nn(xt[side], right).reshape(own.shape[1:]).astype(bf16)
            s.begin(p)

        s.advance(p)

        @pl.when(p < turns)
        def _():
            hh, r = lax.div(p, stages), lax.rem(p, stages)

            @pl.when(r == 0)
            def _():
                prepare(hh)

            for e, which in enumerate((range(blocks - 1), range(blocks - 1, blocks))):

                @pl.when((r > 0) & (r <= 2 * groups) & (lax.rem(r + 1, 2) == e))
                def _():
                    group_back(lax.div(r - 1, 2), which)

            @pl.when(r == stages - 1)
            def _():
                join(hh)

                @pl.when(hh == 0)
                def _():
                    half_load(1, "start")

                @pl.when(hh == 1)
                def _():
                    for cp in qkv_copies():
                        cp.start()

        for i in range(2 * each):

            @pl.when(p == turns + i)
            def _():
                against(i)

        @pl.when(p == norm_at)
        def _():
            norm_one_back()

        @pl.when(p == norm_at + 1)
        def _():
            @pl.loop(1, n)
            def _(i):
                part_copy(i).start()

    total = part[d]

    @pl.loop(1, n)
    def _(i):
        part_copy(i).wait()

    total = total + jnp.sum(parts_in[1:], axis=0)
    out_gains[...] = total
    swap = remote(out_gains, pair_in, swap_sem.at[0], swap_sem.at[1], (d, 1 - c))
    swap.start()
    first_column = 0
    for i, out in enumerate((grad_query, grad_key, grad_value)):
        cp = pltpu.make_async_copy(out_qkv.at[:, pl.ds(first_column, out.shape[1])], out, out_sem.at[i])
        cp.start()
        cp.wait()
        first_column += out.shape[1]
    swap.wait()
    out_gains[...] += pair_in[...]
    for t in range(count - s.own_ring + s.depth, count):
        s.release(t)


def backward(line, cols, arrays, halves):
    q, k, v, mixed, grad_mixed, full, hid = arrays[:7]
    tokens, d_model = hid.shape
    rows = full.shape[3]
    n = line * 4
    down_w, gate_w, up_w, out_w, q_w, k_w, v_w = halves
    qkv_w = q_w + k_w + v_w
    starts = [0]
    for w in (down_w, gate_w, up_w, out_w, qkv_w):
        starts.append(starts[-1] + w // cols)
    heads, groups = q.shape[0] // 2, k.shape[0] // 2
    width = q_w
    bf16, f32 = jnp.bfloat16, jnp.float32
    struct, V, dma = jax.ShapeDtypeStruct, pltpu.VMEM, pltpu.SemaphoreType.DMA
    hbm, vmem = pl.BlockSpec(memory_space=pl.ANY), pl.BlockSpec(memory_space=pltpu.VMEM)
    ring, own_ring = line + 12, 4
    head = lambda m: (m, tokens, HEAD_SIZE)
    sems = 2 + 2 * (line - 1)
    outs = [struct((2, tokens, qkv_w), bf16)]
    outs += [struct((rows, w), f32) for w in (q_w, k_w, v_w)]
    outs += [struct((tokens, d_model), f32), struct((out_w, rows), f32), struct((rows, gate_w), f32), struct((rows, up_w), f32), struct((down_w, rows), f32), struct((8, 128), f32)]
    return pl.pallas_call(
        functools.partial(backward_kernel, line, cols, tuple(starts)),
        out_shape=outs,
        in_specs=[hbm] * 8 + [vmem] * 4 + [hbm] * 8,
        out_specs=[hbm] * 4 + [vmem] * 6,
        scratch_shapes=[
            V((own_ring, line, 2, 2, rows, cols), bf16),
            V((ring, line, 2, rows, cols), bf16),
            V((ring, line, rows, cols), bf16),
            V((ring, line - 1, rows, cols), bf16),
            V((ring, line - 1, rows, cols), bf16),
            V((2, d_model, 2 * tokens), bf16),
            V((2, 2, tokens, cols), bf16),
            V(head(heads), bf16),
            V(head(groups), bf16),
            V(head(groups), bf16),
            V((tokens, heads * HEAD_SIZE), bf16),
            V((tokens, heads * HEAD_SIZE), f32),
            V(head(heads), bf16),
            V((heads, tokens, 1), f32),
            V(head(heads), f32),
            V(head(groups), f32),
            V(head(groups), f32),
            V((tokens, 2 * qkv_w), bf16),
            V((2, line, 2, 2, rows, width), bf16),
            V((tokens, d_model), f32),
            V((tokens, d_model), bf16),
            V((rows, qkv_w), f32),
            V((1, d_model), f32),
            V((n, 8, 128), f32),
            V((n, 8, 128), f32),
            V((8, 128), f32),
            dma((ring, sems)),
            dma((ring, sems)),
            dma((2,)),
            dma((2,)),
            dma((5,)),
            dma((2,)),
            dma((2,)),
            dma,
            dma,
            dma,
            dma((n,)),
            dma((n,)),
            dma((3,)),
            dma((2,)),
        ],
        compiler_params=pltpu.CompilerParams(collective_id=1, has_side_effects=True, vmem_limit_bytes=64 * 2**20 - 2**17),
        name="backward_scatter",
    )(*arrays)


def layer(n_dp, n_tensor, hidden_in, query_weight, key_matrix, value_matrix, out_weight, gate_weight, up_weight, down_weight, attention_gain, feedforward_gain, cotangent):
    line = n_dp // 4
    rows = attention_gain.shape[0]
    block = (query_weight.shape[1] // 3) & -128
    cosine, sine = rope_tables(SEQUENCE_LENGTH, HEAD_SIZE)
    (full, _, q, k, v, mixed, n1, n2, ct, mixed_pair, gm, hidden, gate, up, hidden_out, grad_middle, grad_mixed, gain_two, gain_rows) = forward(
        line,
        (query_weight, key_matrix, value_matrix, gate_weight, up_weight, out_weight, down_weight),
        (attention_gain.reshape(1, rows), feedforward_gain.reshape(1, rows)),
        hidden_in,
        cotangent,
        cosine,
        sine,
        block,
    )
    arrays = (q, k, v, mixed, grad_mixed, full, hidden_in, grad_middle, gain_rows, gain_two, cosine, sine, n1, n2, ct, gm, mixed_pair, hidden, gate, up)
    halves = (down_weight.shape[0], gate_weight.shape[1], up_weight.shape[1], out_weight.shape[0], query_weight.shape[1], key_matrix.shape[1], value_matrix.shape[1])
    _, g_query, g_key, g_value, grad_in, g_out, g_gate, g_up, g_down, g_gains = backward(line, 256 if line <= 4 else 128, arrays, halves)
    return hidden_out, grad_in, g_query, g_key, g_value, g_out, g_gate, g_up, g_down, g_gains[0, :rows], g_gains[1, :rows]


def solution(mesh):
    split = P(("dp", "tensor"), None)
    row, column, gain = P("dp", "tensor"), P("tensor", "dp"), P("dp")
    return jax.shard_map(
        functools.partial(layer, mesh.shape["dp"], mesh.shape["tensor"]),
        mesh=mesh,
        in_specs=(split, row, row, row, column, row, row, column, gain, gain, split),
        out_specs=(split, split, row, row, row, column, row, row, column, gain, gain),
        check_vma=False,
    )
```

```python
import functools
import math

import jax
import jax.numpy as jnp
from jax import lax
from jax.experimental import pallas as pl
from jax.experimental.pallas import tpu as pltpu
from jax.sharding import PartitionSpec as P

QUERY_HEADS = 16
KEY_VALUE_HEADS = 8
HEAD_SIZE = 96
SEQUENCE_LENGTH = 512

EPSILON = 1e-05
THETA_BASE = 100000.0
MESH = pl.DeviceIdType.MESH


def place():
    d = lax.axis_index("dp")
    return lax.div(d, 4), lax.rem(lax.div(d, 2), 2), lax.rem(d, 2), lax.axis_index("tensor")


def dev(z, y, x, c):
    return (z * 4 + y * 2 + x, c)


def enter(line, pos):
    z, y, x, c = pos
    barrier = pltpu.get_barrier_semaphore()

    def greet(who):
        pl.semaphore_signal(barrier, inc=1, device_id=who, device_id_type=MESH)

    greet(dev(z, y, x, 1 - c))
    greet(dev(z, y, 1 - x, c))
    greet(dev(z, 1 - y, x, c))

    @pl.when(z > 0)
    def _():
        greet(dev(z - 1, y, x, c))

    @pl.when(z < line - 1)
    def _():
        greet(dev(z + 1, y, x, c))

    pl.semaphore_wait(barrier, 3 + (z > 0).astype(jnp.int32) + (z < line - 1).astype(jnp.int32))


def remote(src, dst, send, recv, who):
    return pltpu.make_async_remote_copy(src_ref=src, dst_ref=dst, send_sem=send, recv_sem=recv, device_id=who, device_id_type=MESH)


class Gather:
    def __init__(self, line, pos, shard, full, width, orders, paired, send, recv):
        self.line, self.pos, self.shard, self.full, self.width = line, pos, shard, full, width
        self.orders, self.paired, self.send, self.recv = orders, paired, send, recv
        self.count = shard.shape[-1] // width
        self.depth = line + 1 + paired

    def columns(self, t, sub):
        part = self.width // len(self.orders[0])
        return t * self.width + sub * part, part

    def region(self, t, sub, have, z=None):
        first, part = self.columns(t, sub)
        pz, py, px, c = self.pos
        if self.paired:
            first = first + c * self.shard.shape[-1]
        every = slice(None)
        zi = z if z is not None else (every if "z" in have else pz)
        cols = pl.ds(pl.multiple_of(first, 128), part)
        return self.full.at[zi, every if "y" in have else py, every if "x" in have else px, :, cols]

    def own(self, t, sub):
        first, part = self.columns(t, sub)
        return self.shard.at[:, pl.ds(pl.multiple_of(first, 128), part)]

    def copy(self, t, sub, slot, src, dst, who):
        return remote(src, dst, self.send.at[t, sub, slot], self.recv.at[t, sub, slot], who)

    def hop(self, t, sub, h, up, have, what):
        z, y, x, c = self.pos
        slot = (h - 1) * 2 + up
        if up:
            block, incoming, who = z - (h - 1), z - h, dev(z + 1, y, x, c)
            there, here = (z + 1 < self.line) & (z >= h - 1), z >= h
        else:
            block, incoming, who = z + (h - 1), z + h, dev(z - 1, y, x, c)
            there, here = (z > 0) & (z + h - 1 < self.line), z + h < self.line

        @pl.when(here if what == "recv" else there)
        def _():
            if what == "recv":
                r = self.region(t, sub, have, incoming)
                self.copy(t, sub, slot, r, r, dev(z, y, x, 1 - c)).wait_recv()
                return
            r = self.region(t, sub, have, block)
            cp = self.copy(t, sub, slot, self.own(t, sub) if h == 1 and not have else r, r, who)
            cp.start() if what == "start" else cp.wait_send()

    def act(self, t, sub, order, i, what):
        z, y, x, c = self.pos
        moves, have = [], ""
        for axis in order:
            moves += [(axis, h, have) for h in (range(1, self.line) if axis == "z" else (0,))]
            have += axis
        if self.paired:
            moves.append(("c", 0, have))
        axis, h, have = moves[i]
        if axis == "z":
            for up in (1, 0):
                self.hop(t, sub, h, up, have, what)
            return
        who = {"y": dev(z, 1 - y, x, c), "x": dev(z, y, 1 - x, c), "c": dev(z, y, x, 1 - c)}[axis]
        land = self.region(t, sub, have)
        cp = self.copy(t, sub, 2 * (self.line - 1) + "yxc".index(axis), land if have else self.own(t, sub), land, who)
        {"start": cp.start, "recv": cp.wait_recv, "sent": cp.wait_send}[what]()

    def each(self, t, fn):
        there = (t >= 0) & (t < self.count)
        for v, orders in enumerate(self.orders):
            turn_of = there if len(self.orders) == 1 else there & ((lax.rem(t + 6, 6) == 0) == (v == 1))

            @pl.when(turn_of)
            def _():
                for sub, order in enumerate(orders):
                    fn(sub, order)

    def step(self, t, s):
        def go(sub, order):
            if s > 0:
                self.act(t, sub, order, s - 1, "recv")
            if s < self.depth:
                self.act(t, sub, order, s, "start")

        self.each(t, go)

    def advance(self, p):
        for s in range(self.depth + 1):
            self.step(p - s, s)

    def finish(self):
        @pl.loop(0, self.count)
        def _(t):
            self.each(t, lambda sub, order: [self.act(t, sub, order, i, "sent") for i in range(self.depth)])


def own_copy(g, sem):
    z, y, x, c = g.pos
    first = c * g.shard.shape[-1] if g.paired else 0
    return pltpu.make_async_copy(g.shard, g.full.at[z, y, x, :, pl.ds(pl.multiple_of(first, 128), g.shard.shape[-1])], sem)


def rope_tables(length, width):
    half_width = width // 2
    inverse = THETA_BASE ** (-(jnp.arange(half_width, dtype=jnp.float32) * 2.0 / width))
    angles = jnp.arange(length, dtype=jnp.float32)[:, None] * inverse[None, :]
    cosine, sine = jnp.cos(angles), jnp.sin(angles)
    return jnp.concatenate([cosine, cosine], axis=1), jnp.concatenate([-sine, sine], axis=1)


def turn(x, cosine, sine):
    half = x.shape[-1] // 2
    return x * cosine + jnp.concatenate([x[:, half:], x[:, :half]], axis=1) * sine


def dot_nt(a, b):
    return lax.dot_general(a, b, (((1,), (1,)), ((), ())), preferred_element_type=jnp.float32)


def dot_tn(a, b):
    return lax.dot_general(a, b, (((0,), (0,)), ((), ())), preferred_element_type=jnp.float32)


def dot_nn(a, b):
    return jnp.dot(a, b, preferred_element_type=jnp.float32)


BLOCK = 128


def causal_weights(q, k, b, heads):
    scores = dot_nt(q, k) * (1.0 / math.sqrt(HEAD_SIZE))
    n = scores.shape[1]
    row = lax.broadcasted_iota(jnp.int32, scores.shape, 0) % BLOCK + b * BLOCK
    keep = row >= lax.broadcasted_iota(jnp.int32, scores.shape, 1)
    scores = jnp.where(keep, scores, -jnp.inf)
    log_total = jnp.log(jnp.sum(jnp.exp(scores), axis=1, keepdims=True))
    return jnp.exp(scores - log_total)


def rows_of(ref, first, heads, rows):
    return jnp.concatenate([ref[first + i, rows] for i in range(heads)], axis=0)


ROWS = 128


def each_rows(tokens, step, fn):
    @pl.loop(0, tokens // step)
    def _(r):
        fn(pl.ds(pl.multiple_of(r * step, step), step))


def forward_kernel(line, width, block, *refs):
    refs = list(refs)
    take = lambda n: [refs.pop(0) for _ in range(n)]
    query_in, key_in, value_in, gate_in, up_in, out_in, down_in, gain_a, gain_b, hid, ct, cosine, sine = take(13)
    full, gains_full, q_out, k_out, v_out, mixed_out, n1_pair, n2_pair, ct_pair, mixed_pair, middle_out = take(11)
    tile_pairs = take(3)
    hidden_out, grad_n2, gain = take(3)
    wbuf, gain_buf, n1, n2, flat, qh, kh, vh, mh, mixed, middle, acc, act, tiles, shard, gains, turned = take(17)
    send, recv, gsend, grecv, own_sem, load_sem, gain_sem, local_sem, pair_send, pair_recv, tile_local, tile_send, tile_recv, shard_sem = take(14)

    pos = place()
    z, y, x, c = pos
    tokens, d_model = hid.shape
    half = shard.shape[-1]
    heads, groups = qh.shape[0] // 2, kh.shape[0] // 2
    sibling = dev(z, y, x, 1 - c)
    bf16, f32 = jnp.bfloat16, jnp.float32

    g = Gather(line, pos, shard, full, width, (("zyx", "zxy"), ("xyz", "yxz")), 1, send, recv)
    gg = Gather(line, pos, gains, gains_full, gains.shape[-1], (("zyx",),), 0, gsend, grecv)
    g_own, gg_own = own_copy(g, own_sem.at[0]), own_copy(gg, own_sem.at[1])
    steps = (half // width) - 3
    fills, at = [], 0
    for src in (query_in, key_in, value_in):
        fills.append((src, at, src.shape[1]))
        at += src.shape[1]
    fills.append((out_in, at, out_in.shape[1]))
    at += out_in.shape[1]
    for j in range(steps):
        for i, src in enumerate((gate_in, up_in, down_in)):
            fills.append((src.at[:, pl.ds(j * block, block)], at + j * width + i * block, block))
    fills = [pltpu.make_async_copy(src, shard.at[:, pl.ds(to, n)], shard_sem.at[i]) for i, (src, to, n) in enumerate(fills)]
    for cp in fills:
        cp.start()
    gains[...] = jnp.zeros_like(gains)
    top = lax.broadcasted_iota(jnp.int32, (gains.shape[0], gain_a.shape[1]), 0) == 0
    gains[:, : gain_a.shape[1]] = jnp.where(top, gain_a[...].astype(f32), gain_b[...].astype(f32)).astype(bf16)
    enter(line, pos)
    for cp in fills:
        cp.wait()
    g_own.start()
    gg_own.start()

    def load(t, hh, slot):
        cols = pl.ds(pl.multiple_of(hh * half + t * width, 128), width)
        return pltpu.make_async_copy(full.at[:, :, :, :, cols], wbuf.at[slot, hh], load_sem.at[slot, hh])

    def weight(slot, hh):
        return wbuf[slot, hh].reshape(d_model, width)

    def share(i, own_src, own_dst, other_src, other_dst):
        return pltpu.make_async_copy(own_src, own_dst, local_sem.at[i]), remote(other_src, other_dst, pair_send.at[i], pair_recv.at[i], sibling)

    ends = (pl.ds(0, tokens), pl.ds(tokens, tokens))
    lefts = ((ct, ct_pair), (n1, n1_pair), (n2, n2_pair))
    shares = [share(i, turned.at[i], pair.at[:, ends[0]], turned.at[i], pair.at[:, ends[1]]) for i, (_, pair) in enumerate(lefts)]
    hw = mixed.shape[1] // 2
    side = lambda ref, s, w: ref.at[:, pl.ds(pl.multiple_of(s * w, 128), w)]
    shares.append(share(3, side(mixed, c, hw), mixed_pair.at[0], side(mixed, 1 - c, hw), mixed_pair.at[1]))
    keeps = [pltpu.make_async_copy(src, dst, local_sem.at[4 + i]) for i, (src, dst) in enumerate(((qh, q_out), (kh, k_out), (vh, v_out), (mixed, mixed_out), (middle, middle_out)))]

    def begin(i):
        if i < len(lefts):
            span = 256

            @pl.loop(0, d_model // span)
            def _(e):
                at = pl.ds(pl.multiple_of(e * span, span), span)
                turned[i, at, :] = lefts[i][0][:, at].T

        for cp in shares[i]:
            cp.start()

    def end(i):
        for cp in shares[i]:
            cp.wait()

    def tile_copies(j, hh):
        slot = lax.rem(j, 2)
        cols = pl.ds(pl.multiple_of(j * block, 128), block)
        own = [pltpu.make_async_copy(tiles.at[slot, hh, i], pair.at[0, :, cols], tile_local.at[j, i]) for i, pair in enumerate(tile_pairs)]
        out = [remote(tiles.at[slot, hh, i], pair.at[1, :, cols], tile_send.at[j, i], tile_recv.at[j, i], sibling) for i, pair in enumerate(tile_pairs)]
        return own, out

    def drain_tiles(j):
        for cp in tile_copies(j, 0)[0]:
            cp.wait()
        for cp in tile_copies(j, 0)[1]:
            cp.wait_send()

    def normalize():
        loaded = pltpu.make_async_copy(gains_full, gain_buf, gain_sem)
        loaded.start()
        loaded.wait()
        n = d_model // (gain_buf.shape[0] * 4)
        table = gain_buf[...].astype(f32)
        for i in range(2):
            gain[i : i + 1, :] = jnp.concatenate([table[a, b, e, i : i + 1, :n] for a in range(gain_buf.shape[0]) for b in range(2) for e in range(2)], axis=1)

        def rows_of_norm(rows):
            v = hid[rows, :].astype(f32)
            v = v * lax.rsqrt(jnp.mean(v * v, axis=1, keepdims=True) + EPSILON)
            n1[rows, :] = (v * gain[0:1, :]).astype(bf16)

        each_rows(tokens, ROWS, rows_of_norm)
        begin(1)

    def project(slot, outs):
        @pl.loop(0, 2)
        def _(hh):
            flat[...] = dot_nn(n1[...], weight(slot, hh))

            def to_heads(rows):
                cos, sin = cosine[rows, :], sine[rows, :]
                first = 0
                for n, target, turned in outs:
                    for h in range(n):
                        v = flat[rows, (first + h) * HEAD_SIZE : (first + h + 1) * HEAD_SIZE]
                        target[hh * n + h, rows] = (turn(v, cos, sin) if turned else v).astype(bf16)
                    first += n

            each_rows(tokens, ROWS, to_heads)

    def attend_half(hh):
        per = heads // groups
        blocks = tokens // BLOCK

        @pl.loop(0, groups)
        def _(i):
            kv = hh * groups + i
            for b in range(blocks):
                rows, n = pl.ds(b * BLOCK, BLOCK), (b + 1) * BLOCK
                w = causal_weights(rows_of(qh, kv * per, per, rows), kh[kv, :n], b, per).astype(bf16)
                m = dot_nn(w, vh[kv, :n]).astype(bf16)
                for e in range(per):
                    mh[kv * per + e, rows] = m[e * BLOCK : (e + 1) * BLOCK]

    def leave_attention(slot):
        def join(rows):
            mixed[rows, :] = jnp.concatenate([mh[h, rows] for h in range(2 * heads)], axis=1)

        each_rows(tokens, ROWS, join)
        begin(3)
        for cp in keeps[:4]:
            cp.start()
        middle[...] = hid[...].astype(f32) + dot_nt(mixed[:, :hw], weight(slot, 0))
        middle[...] += dot_nt(mixed[:, hw:], weight(slot, 1))

        def rows_of_norm(rows):
            v = middle[rows, :]
            acc[rows, :] = v
            v = v * lax.rsqrt(jnp.mean(v * v, axis=1, keepdims=True) + EPSILON)
            n2[rows, :] = (v * gain[1:2, :]).astype(bf16)
            grad_n2[rows, :] = jnp.zeros_like(v)

        keeps[4].start()
        each_rows(tokens, ROWS, rows_of_norm)
        begin(2)

    def feed_forward(j, slot):
        @pl.when(j >= 2)
        def _():
            drain_tiles(j - 2)

        part = lax.rem(j, 2)

        @pl.loop(0, 2)
        def _(hh):
            act[0] = dot_nn(n2[...], weight(slot, hh)[:, :block])
            act[1] = dot_nn(n2[...], weight(slot, hh)[:, block : 2 * block])
            act[2] = dot_nn(ct[...], weight(slot, hh)[:, 2 * block :])

            def gated(rows):
                gate, up, grad = act[0, rows], act[1, rows], act[2, rows]
                sigma = jax.nn.sigmoid(gate)
                tiles[part, hh, 0, rows] = (gate * sigma * up).astype(bf16)
                tiles[part, hh, 1, rows] = (grad * up * sigma * (1.0 + gate * (1.0 - sigma))).astype(bf16)
                tiles[part, hh, 2, rows] = (grad * gate * sigma).astype(bf16)

            each_rows(tokens, ROWS // 2, gated)
            own, out = tile_copies(j, hh)

            @pl.when(hh == c)
            def _():
                for cp in own:
                    cp.start()

            @pl.when(hh != c)
            def _():
                for cp in out:
                    cp.start()

            acc[...] += dot_nt(tiles[part, hh, 0], weight(slot, hh)[:, 2 * block :])
            both = jnp.concatenate([tiles[part, hh, 1], tiles[part, hh, 2]], axis=1)
            grad_n2[...] += dot_nt(both, weight(slot, hh)[:, : 2 * block])

    count, lead = g.count, g.depth + 1

    @pl.loop(0, count + lead)
    def _(p):
        @pl.when(p == 0)
        def _():
            g_own.wait()
            gg_own.wait()
            begin(0)

        gg.advance(p)
        g.advance(p)
        u = p - lead

        @pl.when((u >= -1) & (u + 1 < count))
        def _():
            for hh in range(2):
                load(u + 1, hh, lax.rem(u + 1, 2)).start()

        @pl.when(u >= 0)
        def _():
            slot = lax.rem(u, 2)
            for hh in range(2):
                load(u, hh, slot).wait()

            @pl.when(u == 0)
            def _():
                normalize()
                project(slot, ((heads, qh, True),))

            @pl.when(u == 1)
            def _():
                project(slot, ((groups, kh, True), (groups, vh, False)))
                attend_half(0)

            @pl.when(u == 2)
            def _():
                attend_half(1)
                leave_attention(slot)

            @pl.when(u >= 3)
            def _():
                feed_forward(u - 3, slot)

    def rows_out(rows):
        hidden_out[rows, :] = acc[rows, :].astype(bf16)

    each_rows(tokens, ROWS, rows_out)
    for i in range(len(shares)):
        end(i)
    for cp in keeps:
        cp.wait()
    for j in range(max(steps - 2, 0), steps):
        drain_tiles(j)

    @pl.loop(0, steps)
    def _(j):
        for cp in tile_copies(j, 0)[1]:
            cp.wait_recv()

    g.finish()
    gg.finish()


def forward(line, shards, gain_pair, hidden_in, cotangent, cosine, sine, block):
    tokens, d_model = hidden_in.shape
    rows = gain_pair[0].shape[1]
    half = sum(s.shape[1] for s in shards)
    gains = jax.ShapeDtypeStruct((8, 128), jnp.bfloat16)
    width = 3 * block
    count = half // width
    steps = count - 3
    heads, groups = QUERY_HEADS // 2, KEY_VALUE_HEADS // 2
    bf16, f32 = jnp.bfloat16, jnp.float32
    struct = jax.ShapeDtypeStruct
    hbm, vmem = pl.BlockSpec(memory_space=pl.ANY), pl.BlockSpec(memory_space=pltpu.VMEM)
    dma = pltpu.SemaphoreType.DMA
    pair = struct((d_model, 2 * tokens), bf16)
    tile_pair = struct((2, tokens, steps * block), bf16)
    head_shape = lambda n: (n, tokens, HEAD_SIZE)
    slots = 2 * (line - 1) + 3
    outs = [
        struct((line, 2, 2, rows, 2 * half), bf16),
        struct((line, 2, 2) + gains.shape, bf16),
        struct(head_shape(2 * heads), bf16),
        struct(head_shape(2 * groups), bf16),
        struct(head_shape(2 * groups), bf16),
        struct((tokens, 2 * heads * HEAD_SIZE), bf16),
        pair,
        pair,
        pair,
        struct((2, tokens, heads * HEAD_SIZE), bf16),
        struct((tokens, d_model), f32),
        tile_pair,
        tile_pair,
        tile_pair,
        struct((tokens, d_model), bf16),
        struct((tokens, d_model), f32),
        struct((8, d_model), f32),
    ]
    V = pltpu.VMEM
    return pl.pallas_call(
        functools.partial(forward_kernel, line, width, block),
        out_shape=outs,
        in_specs=[hbm] * 7 + [vmem] * 6,
        out_specs=[hbm] * 14 + [vmem] * 3,
        scratch_shapes=[
            V((2, 2, line, 2, 2, rows, width), bf16),
            V((line, 2, 2) + gains.shape, bf16),
            V((tokens, d_model), bf16),
            V((tokens, d_model), bf16),
            V((tokens, width), f32),
            V(head_shape(2 * heads), bf16),
            V(head_shape(2 * groups), bf16),
            V(head_shape(2 * groups), bf16),
            V(head_shape(2 * heads), bf16),
            V((tokens, 2 * heads * HEAD_SIZE), bf16),
            V((tokens, d_model), f32),
            V((tokens, d_model), f32),
            V((3, tokens, block), f32),
            V((2, 2, 3, tokens, block), bf16),
            V((rows, half), bf16),
            V(gains.shape, bf16),
            V((3, d_model, tokens), bf16),
            dma((count, 2, slots)),
            dma((count, 2, slots)),
            dma((1, 1, slots)),
            dma((1, 1, slots)),
            dma((2,)),
            dma((2, 2)),
            dma,
            dma((9,)),
            dma((4,)),
            dma((4,)),
            dma((steps, 3)),
            dma((steps, 3)),
            dma((steps, 3)),
            dma((4 + 3 * steps,)),
        ],
        compiler_params=pltpu.CompilerParams(collective_id=0, has_side_effects=True, vmem_limit_bytes=64 * 2**20 - 2**17),
        name="gather_forward",
    )(*shards, *gain_pair, hidden_in, cotangent, cosine, sine)


class Scatter:
    def __init__(self, line, pos, count, own, first, second, up, down, send, recv, final):
        self.line, self.pos, self.count, self.final = line, pos, count, final
        self.own, self.first, self.second, self.up, self.down, self.send, self.recv = own, first, second, up, down, send, recv
        self.ring, self.own_ring = first.shape[0], own.shape[0]
        self.lags = [0, 2, 4] + [5 + j for j in range(line - 1)] + [4 + line, 5 + line]
        self.depth = self.lags[-1]

    def copy(self, t, slot, src, dst, who):
        r = lax.rem(t, self.ring)
        return remote(src, dst, self.send.at[r, slot], self.recv.at[r, slot], who)

    def merge(self, dst, a, b, loops):
        def go(lead, rest):
            if not rest:
                dst[lead] = a[lead] + b[lead]
            elif rest[0] > 2:
                @pl.loop(0, rest[0])
                def _(i):
                    go(lead + (i,), rest[1:])
            else:
                for i in range(rest[0]):
                    go(lead + (i,), rest[1:])

        go((), loops)

    def pair_moves(self, t, v):
        z, y, x, c = self.pos
        r, o = lax.rem(t, self.ring), lax.rem(t, self.own_ring)
        own, first, second = self.own.at[o], self.first.at[r], self.second.at[r]
        over_x, over_y = dev(z, y, 1 - x, c), dev(z, 1 - y, x, c)
        if v == 0:
            give, keep, who = own.at[:, :, 1 - x], own.at[:, :, x], (over_x, over_y)
        else:
            give, keep, who = own.at[:, 1 - y], own.at[:, y], (over_y, over_x)
        a, b = (1 - y, y) if v == 0 else (1 - x, x)
        one = self.copy(t, 0, give, first, who[0])
        two = self.copy(t, 1, first.at[:, a], second, who[1])
        return one, two, keep, first, second, first.at[:, b]

    def hop(self, p, j, way):
        z, y, x, c = self.pos
        last = self.line - 1
        travelled = z if way == 0 else last - z
        t = p - self.lags[3] - j - travelled
        target = last - j if way == 0 else j
        passes = (target > z) if way == 0 else (target < z)

        def go():
            r = lax.rem(t, self.ring)
            cur, ref = self.second.at[r], (self.up if way == 0 else self.down).at[r, j]
            nxt = dev(z + 1, y, x, c) if way == 0 else dev(z - 1, y, x, c)

            @pl.when(travelled == 0)
            def _():
                self.copy(t, 2 + 2 * j + way, cur.at[target], ref, nxt).start()

            @pl.when(travelled > 0)
            def _():
                cp = self.copy(t, 2 + 2 * j + way, ref, ref, nxt)
                cp.wait_recv()
                ref[...] = ref[...] + cur[target]
                cp.start()

        @pl.when(passes & (t >= 0) & (t < self.count))
        def _():
            go()

    def close(self, t):
        z, y, x, c = self.pos
        r = lax.rem(t, self.ring)
        ku, kd = self.line - 1 - z, z
        has_up, has_down = z > 0, z < self.line - 1
        for has, way, ref, k in ((has_up, 0, self.up, ku), (has_down, 1, self.down, kd)):

            @pl.when(has)
            def _():
                self.copy(t, 2 + 2 * k + way, ref.at[r, k], ref.at[r, k], dev(z, y, x, 1 - c)).wait_recv()

        f32 = jnp.float32
        total = self.second[r, z].astype(f32)
        last = self.line - 2
        below = self.up[r, jnp.minimum(ku, last)].astype(f32)
        above = self.down[r, jnp.minimum(kd, last)].astype(f32)
        total = total + jnp.where(has_up, below, 0.0) + jnp.where(has_down, above, 0.0)
        self.final(t, total)

    def drain(self, t):
        z, y, x, c = self.pos
        r = lax.rem(t, self.ring)
        self.pair_moves(t, 0)[1].wait_send()
        for j in range(self.line - 1):
            for way, ref, target in ((0, self.up, self.line - 1 - j), (1, self.down, j)):

                @pl.when((target > z) if way == 0 else (target < z))
                def _():
                    self.copy(t, 2 + 2 * j + way, ref.at[r, j], ref.at[r, j], dev(z, y, x, 1 - c)).wait_send()

    def when(self, t, fn):
        @pl.when((t >= 0) & (t < self.count))
        def _():
            fn()

    def both(self, t, fn):
        for v in range(2):
            @pl.when((t >= 0) & (t < self.count) & (lax.rem(t + 2, 2) == v))
            def _():
                fn(v)

    def begin(self, t):
        self.both(t, lambda v: self.pair_moves(t, v)[0].start())

    def release(self, t):
        self.when(t, lambda: self.pair_moves(t, 0)[0].wait_send())

    def advance(self, p):
        line = self.line

        def one(v, t):
            first_copy, second_copy, keep, first, second, _ = self.pair_moves(t, v)
            first_copy.wait_recv()
            self.merge(first, first, keep, (line, 2))
            second_copy.start()

        def two(v, t):
            _, second_copy, _, _, second, keep = self.pair_moves(t, v)
            second_copy.wait_recv()
            self.merge(second, second, keep, (line,))

        t = p - self.lags[1]
        self.both(t, lambda v, t=t: one(v, t))
        t = p - self.lags[2]
        self.both(t, lambda v, t=t: two(v, t))
        for j in range(line - 1):
            for way in range(2):
                self.hop(p, j, way)
        t = p - self.lags[-2]
        self.when(t, lambda t=t: self.close(t))
        t = p - self.lags[-1]
        self.when(t, lambda t=t: self.drain(t))


def greet_all(n, pos):
    z, y, x, c = pos
    d = z * 4 + y * 2 + x
    barrier = pltpu.get_barrier_semaphore()

    @pl.loop(1, n)
    def _(i):
        pl.semaphore_signal(barrier, inc=1, device_id=(lax.rem(d + i, n), c), device_id_type=MESH)

    pl.semaphore_signal(barrier, inc=1, device_id=(d, 1 - c), device_id_type=MESH)
    pl.semaphore_wait(barrier, n)


def backward_kernel(line, cols, starts, *refs):
    refs = list(refs)
    take = lambda n: [refs.pop(0) for _ in range(n)]
    q, k, v, mixed, full, hid, ct, middle, grad_n2, gains, cosine, sine = take(12)
    n1_pair, n2_pair, ct_pair, mixed_pair, hidden_pair, gate_pair, up_pair = take(7)
    qkv_pair, grad_query, grad_key, grad_value, grad_in, out_out, out_gate, out_up, out_down, out_gains, gm_pair = take(11)
    own, first, second, up, down, xt, ybuf, qh, kh, vh, mh, gh, gm, dots, dq, dk, dv, dqkv, wbuf, gmid, hbuf, out_qkv, gain_one, part, parts_in, pair_in, gain_two, gmb, turned = take(29)
    send, recv, xsem, ysem, half_sem, wsem, msem, qkv_local, qkv_send, qkv_recv, part_send, part_recv, out_sem, swap_sem, gm_sem = take(15)

    pos = place()
    z, y, x, c = pos
    d = z * 4 + y * 2 + x
    n = line * 4
    tokens, d_model = hid.shape
    count = starts[-1]
    heads, groups = qh.shape[0], kh.shape[0]
    share = heads // groups
    blocks = tokens // BLOCK
    width = wbuf.shape[-1]
    half_width = dqkv.shape[1] // 2
    scale = 1.0 / math.sqrt(HEAD_SIZE)
    bf16, f32 = jnp.bfloat16, jnp.float32
    sources = (hidden_pair, gate_pair, up_pair, mixed_pair, qkv_pair)
    lefts = ((0, ct_pair), (starts[1], n2_pair), (starts[3], gm_pair), (starts[4], n1_pair))

    def final(t, total):
        for i, out in enumerate((out_down, out_gate, out_up, out_out, out_qkv)):
            at = pl.ds(pl.multiple_of((t - starts[i]) * cols, 128), cols)

            @pl.when((t >= starts[i]) & (t < starts[i + 1]))
            def _():
                out[:, at] = total

    s = Scatter(line, pos, count, own, first, second, up, down, send, recv, final)

    def load_left(i):
        return pltpu.make_async_copy(lefts[i][1], xt.at[i % 2], xsem.at[i % 2])

    def load_right(t, act):
        slot = lax.rem(t, 2)
        for i, src in enumerate(sources):
            at = pl.ds(pl.multiple_of((t - starts[i]) * cols, 128), cols)

            @pl.when((t >= starts[i]) & (t < starts[i + 1]))
            def _():
                cp = pltpu.make_async_copy(src.at[:, :, at], ybuf.at[slot], ysem.at[slot])
                cp.start() if act == "start" else cp.wait()

    def half_loads(hh):
        take_heads = lambda ref, m: ref.at[pl.ds(hh * m, m)]
        lanes = pl.ds(pl.multiple_of(hh * mh.shape[1], 128), mh.shape[1])
        pairs = ((take_heads(q, heads), qh), (take_heads(k, groups), kh), (take_heads(v, groups), vh), (mixed.at[:, lanes], mh))
        return [pltpu.make_async_copy(src, dst, half_sem.at[i]) for i, (src, dst) in enumerate(pairs)]

    def half_load(hh, act):
        for cp in half_loads(hh):
            cp.start() if act == "start" else cp.wait()

    each = half_width // width
    half_columns = full.shape[-1] // 2

    def weights(i):
        at = (i * half_columns + each * width) if i < 2 else ((i - 2) // each * half_columns + (i - 2) % each * width)
        return pltpu.make_async_copy(full.at[:, :, :, :, pl.ds(at, width)], wbuf.at[i % 2], wsem.at[i % 2])

    def weight(i):
        return wbuf[i % 2].reshape(d_model, width)

    middle_in = pltpu.make_async_copy(middle, grad_in, msem.at[0])
    grad_n2_in = pltpu.make_async_copy(grad_n2, gmid, msem.at[1])
    ct_in, hid_in = (pltpu.make_async_copy(src, hbuf, msem.at[2]) for src in (ct, hid))

    own_half = lambda ref, which: ref.at[:, pl.ds(pl.multiple_of(which * half_width, 128), half_width)]

    def qkv_copies():
        return (
            pltpu.make_async_copy(own_half(dqkv, c), qkv_pair.at[0], qkv_local),
            remote(own_half(dqkv, 1 - c), qkv_pair.at[1], qkv_send, qkv_recv, (d, 1 - c)),
        )

    def gm_copies():
        return (
            pltpu.make_async_copy(turned, gm_pair.at[:, pl.ds(0, tokens)], gm_sem.at[0]),
            remote(turned, gm_pair.at[:, pl.ds(tokens, tokens)], gm_sem.at[1], gm_sem.at[2], (d, 1 - c)),
        )

    def norm_two_back():
        for cp in (middle_in, grad_n2_in, ct_in):
            cp.wait()
        gain_two[...] = jnp.zeros_like(gain_two)

        def rows_back(rows):
            a, grad = grad_in[rows, :], gmid[rows, :]
            inverse = lax.rsqrt(jnp.mean(a * a, axis=1, keepdims=True) + EPSILON)
            unit = a * inverse
            scaled = grad * gains[1:2, :]
            inner = jnp.mean(scaled * unit, axis=1, keepdims=True)
            total = hbuf[rows, :].astype(f32) + inverse * (scaled - unit * inner)
            gmid[rows, :] = total
            gmb[rows, :] = total.astype(bf16)
            gain_two[...] += jnp.sum(grad * unit, axis=0, keepdims=True)

        each_rows(tokens, ROWS, rows_back)
        hid_in.start()
        span = 256

        @pl.loop(0, d_model // span)
        def _(e):
            at = pl.ds(pl.multiple_of(e * span, span), span)
            turned[at, :] = gmb[:, at].T

        for cp in gm_copies():
            cp.start()

    def through_out(i):
        weights(i).wait()
        gh[...] = dot_nn(gmb[...], weight(i))
        weights(i + 2).start()

    def prepare(hh):
        half_load(hh, "wait")

        def rows_of_dots(rows):
            for h in range(heads):
                lanes = slice(h * HEAD_SIZE, (h + 1) * HEAD_SIZE)
                g = gh[rows, lanes]
                dots[h, rows] = jnp.sum(g * mh[rows, lanes].astype(f32), axis=1, keepdims=True)
                gm[h, rows] = g.astype(bf16)

        each_rows(tokens, ROWS, rows_of_dots)
        dk[...] = jnp.zeros_like(dk)
        dv[...] = jnp.zeros_like(dv)

    def group_back(g, which):
        for b in which:
            rows, m = pl.ds(b * BLOCK, BLOCK), (b + 1) * BLOCK
            qb, gb, db = (rows_of(ref, g * share, share, rows) for ref in (qh, gm, dots))
            kb, vb = kh[g, :m], vh[g, :m]
            p = causal_weights(qb, kb, b, share)
            ds = (p * (dot_nt(gb, vb) - db)).astype(bf16)
            dv[g, :m] += dot_tn(p.astype(bf16), gb)
            dk[g, :m] += dot_tn(ds, qb)
            r = dot_nn(ds, kb) * scale
            for i in range(share):
                dq[g * share + i, rows] = r[i * BLOCK : (i + 1) * BLOCK]

    def join(hh):
        def rows_of_join(rows):
            cos, sin = cosine[rows, :], -sine[rows, :]
            parts = [turn(dq[h, rows], cos, sin) for h in range(heads)]
            parts += [turn(dk[g, rows] * scale, cos, sin) for g in range(groups)]
            parts += [dv[g, rows] for g in range(groups)]
            dqkv[rows, pl.ds(pl.multiple_of(hh * half_width, 128), half_width)] = jnp.concatenate([a.astype(bf16) for a in parts], axis=1)

        each_rows(tokens, ROWS, rows_of_join)

    def against(i):
        weights(i + 2).wait()
        r = dot_nt(dqkv[:, i * width : (i + 1) * width], weight(i))
        if i == 0:
            grad_in[...] = r
        else:
            grad_in[...] += r
        if i + 2 < 2 * each:
            weights(i + 4).start()

    def norm_one_back():
        hid_in.wait()
        gain_one[...] = jnp.zeros_like(gain_one)

        def rows_back(rows):
            a = hbuf[rows, :].astype(f32)
            inverse = lax.rsqrt(jnp.mean(a * a, axis=1, keepdims=True) + EPSILON)
            unit, grad = a * inverse, grad_in[rows, :]
            scaled = grad * gains[0:1, :]
            inner = jnp.mean(scaled * unit, axis=1, keepdims=True)
            grad_in[rows, :] = gmid[rows, :] + inverse * (scaled - unit * inner)
            gain_one[...] += jnp.sum(grad * unit, axis=0, keepdims=True)

        each_rows(tokens, ROWS, rows_back)
        size = d_model // n
        part[...] = jnp.zeros_like(part)
        for i in range(n):
            for row, ref in enumerate((gain_one, gain_two)):
                part[i, row : row + 1, :size] = ref[:, i * size : (i + 1) * size]

    def part_copy(i):
        to = lax.rem(d + i, n)
        return remote(part.at[to], parts_in.at[i], part_send.at[i], part_recv.at[i], (to, c))

    load_left(0).start()
    load_left(1).start()
    load_right(0, "start")
    half_load(0, "start")
    for cp in (middle_in, grad_n2_in, ct_in):
        cp.start()
    for i in range(2):
        weights(i).start()
    greet_all(n, pos)

    stages = 2 * groups + 3
    turns = 1 + 2 * stages
    norm_at = turns + 2 * each

    @pl.loop(0, count + s.depth)
    def _(p):
        s.release(p - s.own_ring)
        for i, (at, _) in enumerate(lefts):

            @pl.when(p == at)
            def _():
                load_left(i).wait()
                if 1 <= i < len(lefts) - 1:
                    load_left(i + 1).start()

        @pl.when(p == starts[1] - 1)
        def _():
            for cp in gm_copies():
                cp.wait()

        @pl.when(p == starts[4] - 2)
        def _():
            for cp in qkv_copies():
                cp.wait()

        @pl.when(p < count)
        def _():
            load_right(p, "wait")

            @pl.when(p + 1 < count)
            def _():
                load_right(p + 1, "start")

            side = lax.rem(sum((p >= at).astype(jnp.int32) for at, _ in lefts[1:]), 2)
            right = ybuf[lax.rem(p, 2)].reshape(2 * tokens, cols)
            own[lax.rem(p, s.own_ring)] = dot_nn(xt[side], right).reshape(own.shape[1:]).astype(bf16)
            s.begin(p)

        s.advance(p)

        @pl.when(p == 0)
        def _():
            norm_two_back()

        for i in range(2):

            @pl.when(p == 1 + i * stages)
            def _():
                through_out(i)

        @pl.when((p > 0) & (p < turns))
        def _():
            hh, r = lax.div(p - 1, stages), lax.rem(p - 1, stages) - 1

            @pl.when(r == 0)
            def _():
                prepare(hh)

            for e, which in enumerate((range(blocks - 1), range(blocks - 1, blocks))):

                @pl.when((r > 0) & (r <= 2 * groups) & (lax.rem(r + 1, 2) == e))
                def _():
                    group_back(lax.div(r - 1, 2), which)

            @pl.when(r == stages - 2)
            def _():
                join(hh)

                @pl.when(hh == 0)
                def _():
                    half_load(1, "start")

                @pl.when(hh == 1)
                def _():
                    for cp in qkv_copies():
                        cp.start()

        for i in range(2 * each):

            @pl.when(p == turns + i)
            def _():
                against(i)

        @pl.when(p == norm_at)
        def _():
            norm_one_back()

        @pl.when(p == norm_at + 1)
        def _():
            @pl.loop(1, n)
            def _(i):
                part_copy(i).start()

    total = part[d]

    @pl.loop(1, n)
    def _(i):
        part_copy(i).wait()

    total = total + jnp.sum(parts_in[1:], axis=0)
    out_gains[...] = total
    swap = remote(out_gains, pair_in, swap_sem.at[0], swap_sem.at[1], (d, 1 - c))
    swap.start()
    first_column = 0
    for i, out in enumerate((grad_query, grad_key, grad_value)):
        cp = pltpu.make_async_copy(out_qkv.at[:, pl.ds(first_column, out.shape[1])], out, out_sem.at[i])
        cp.start()
        cp.wait()
        first_column += out.shape[1]
    swap.wait()
    out_gains[...] += pair_in[...]
    for t in range(count - s.own_ring + s.depth, count):
        s.release(t)


def backward(line, cols, arrays, halves):
    q, k, v, mixed, full, hid = arrays[:6]
    tokens, d_model = hid.shape
    rows = full.shape[3]
    n = line * 4
    down_w, gate_w, up_w, out_w, q_w, k_w, v_w = halves
    qkv_w = q_w + k_w + v_w
    starts = [0]
    for w in (down_w, gate_w, up_w, out_w, qkv_w):
        starts.append(starts[-1] + w // cols)
    heads, groups = q.shape[0] // 2, k.shape[0] // 2
    width = q_w
    bf16, f32 = jnp.bfloat16, jnp.float32
    struct, V, dma = jax.ShapeDtypeStruct, pltpu.VMEM, pltpu.SemaphoreType.DMA
    hbm, vmem = pl.BlockSpec(memory_space=pl.ANY), pl.BlockSpec(memory_space=pltpu.VMEM)
    ring, own_ring = line + 12, 4
    head = lambda m: (m, tokens, HEAD_SIZE)
    sems = 2 + 2 * (line - 1)
    outs = [struct((2, tokens, qkv_w), bf16)]
    outs += [struct((rows, w), f32) for w in (q_w, k_w, v_w)]
    outs += [struct((tokens, d_model), f32), struct((rows, out_w), f32), struct((rows, gate_w), f32), struct((rows, up_w), f32), struct((rows, down_w), f32), struct((8, 128), f32)]
    outs += [struct((d_model, 2 * tokens), bf16)]
    return pl.pallas_call(
        functools.partial(backward_kernel, line, cols, tuple(starts)),
        out_shape=outs,
        in_specs=[hbm] * 9 + [vmem] * 3 + [hbm] * 7,
        out_specs=[hbm] * 4 + [vmem] * 6 + [hbm],
        scratch_shapes=[
            V((own_ring, line, 2, 2, rows, cols), bf16),
            V((ring, line, 2, rows, cols), bf16),
            V((ring, line, rows, cols), bf16),
            V((ring, line - 1, rows, cols), bf16),
            V((ring, line - 1, rows, cols), bf16),
            V((2, d_model, 2 * tokens), bf16),
            V((2, 2, tokens, cols), bf16),
            V(head(heads), bf16),
            V(head(groups), bf16),
            V(head(groups), bf16),
            V((tokens, heads * HEAD_SIZE), bf16),
            V((tokens, heads * HEAD_SIZE), f32),
            V(head(heads), bf16),
            V((heads, tokens, 1), f32),
            V(head(heads), f32),
            V(head(groups), f32),
            V(head(groups), f32),
            V((tokens, 2 * qkv_w), bf16),
            V((2, line, 2, 2, rows, width), bf16),
            V((tokens, d_model), f32),
            V((tokens, d_model), bf16),
            V((rows, qkv_w), f32),
            V((1, d_model), f32),
            V((n, 8, 128), f32),
            V((n, 8, 128), f32),
            V((8, 128), f32),
            V((1, d_model), f32),
            V((tokens, d_model), bf16),
            V((d_model, tokens), bf16),
            dma((ring, sems)),
            dma((ring, sems)),
            dma((2,)),
            dma((2,)),
            dma((4,)),
            dma((2,)),
            dma((3,)),
            dma,
            dma,
            dma,
            dma((n,)),
            dma((n,)),
            dma((3,)),
            dma((2,)),
            dma((3,)),
        ],
        compiler_params=pltpu.CompilerParams(collective_id=1, has_side_effects=True, vmem_limit_bytes=64 * 2**20 - 2**17),
        name="backward_scatter",
    )(*arrays)


def finish_kernel(n, *refs):
    srcs, outs, bufs, (loads, stores) = refs[:n], refs[n : 2 * n], refs[2 * n : 3 * n], refs[3 * n :]
    for i in range(n):
        pltpu.make_async_copy(srcs[i], bufs[i], loads.at[i]).start()
    for i in range(n):
        pltpu.make_async_copy(srcs[i], bufs[i], loads.at[i]).wait()
        pltpu.make_async_copy(bufs[i], outs[i], stores.at[i]).start()
    for i in range(n):
        pltpu.make_async_copy(bufs[i], outs[i], stores.at[i]).wait()


def finish(arrays):
    n = len(arrays)
    hbm = pl.BlockSpec(memory_space=pl.ANY)
    return pl.pallas_call(
        functools.partial(finish_kernel, n),
        out_shape=[jax.ShapeDtypeStruct(a.shape, a.dtype) for a in arrays],
        in_specs=[hbm] * n,
        out_specs=[hbm] * n,
        scratch_shapes=[pltpu.VMEM(a.shape, a.dtype) for a in arrays] + [pltpu.SemaphoreType.DMA((n,)), pltpu.SemaphoreType.DMA((n,))],
        compiler_params=pltpu.CompilerParams(vmem_limit_bytes=48 * 2**20),
        name="finish",
    )(*arrays)


def layer(n_dp, n_tensor, hidden_in, query_weight, key_matrix, value_matrix, out_weight, gate_weight, up_weight, down_weight, attention_gain, feedforward_gain, cotangent):
    line = n_dp // 4
    rows = attention_gain.shape[0]
    block = (query_weight.shape[1] // 3) & -128
    cosine, sine = rope_tables(SEQUENCE_LENGTH, HEAD_SIZE)
    (full, _, q, k, v, mixed, n1, n2, ct, mixed_pair, middle, hidden, gate, up, hidden_out, grad_n2, gain_rows) = forward(
        line,
        (query_weight, key_matrix, value_matrix, gate_weight, up_weight, out_weight.T, down_weight.T),
        (attention_gain.reshape(1, rows), feedforward_gain.reshape(1, rows)),
        hidden_in,
        cotangent,
        cosine,
        sine,
        block,
    )
    arrays = (q, k, v, mixed, full, hidden_in, cotangent, middle, grad_n2, gain_rows, cosine, sine, n1, n2, ct, mixed_pair, hidden, gate, up)
    halves = (down_weight.shape[0], gate_weight.shape[1], up_weight.shape[1], out_weight.shape[0], query_weight.shape[1], key_matrix.shape[1], value_matrix.shape[1])
    results = backward(line, 256 if line <= 4 else 128, arrays, halves)
    g_query, g_key, g_value, grad_in, g_out, g_gate, g_up, g_down, hidden_out = finish(list(results[1:9]) + [hidden_out])
    g_gains = results[9]
    return hidden_out, grad_in, g_query, g_key, g_value, g_out.T, g_gate, g_up, g_down.T, g_gains[0, :rows], g_gains[1, :rows]


def solution(mesh):
    split = P(("dp", "tensor"), None)
    row, column, gain = P("dp", "tensor"), P("tensor", "dp"), P("dp")
    return jax.shard_map(
        functools.partial(layer, mesh.shape["dp"], mesh.shape["tensor"]),
        mesh=mesh,
        in_specs=(split, row, row, row, column, row, row, column, gain, gain, split),
        out_specs=(split, split, row, row, row, column, row, row, column, gain, gain),
        check_vma=False,
    )
```

```python
import functools
import math

import jax
import jax.numpy as jnp
from jax import lax
from jax.experimental import pallas as pl
from jax.experimental.pallas import tpu as pltpu
from jax.sharding import PartitionSpec as P

QUERY_HEADS = 16
KEY_VALUE_HEADS = 8
HEAD_SIZE = 96
SEQUENCE_LENGTH = 512

EPSILON = 1e-05
THETA_BASE = 100000.0
MESH = pl.DeviceIdType.MESH


def place():
    d = lax.axis_index("dp")
    return lax.div(d, 4), lax.rem(lax.div(d, 2), 2), lax.rem(d, 2), lax.axis_index("tensor")


def dev(z, y, x, c):
    return (z * 4 + y * 2 + x, c)


def enter(line, pos):
    z, y, x, c = pos
    barrier = pltpu.get_barrier_semaphore()

    def greet(who):
        pl.semaphore_signal(barrier, inc=1, device_id=who, device_id_type=MESH)

    greet(dev(z, y, x, 1 - c))
    greet(dev(z, y, 1 - x, c))
    greet(dev(z, 1 - y, x, c))

    @pl.when(z > 0)
    def _():
        greet(dev(z - 1, y, x, c))

    @pl.when(z < line - 1)
    def _():
        greet(dev(z + 1, y, x, c))

    pl.semaphore_wait(barrier, 3 + (z > 0).astype(jnp.int32) + (z < line - 1).astype(jnp.int32))


def remote(src, dst, send, recv, who):
    return pltpu.make_async_remote_copy(src_ref=src, dst_ref=dst, send_sem=send, recv_sem=recv, device_id=who, device_id_type=MESH)


class Gather:
    def __init__(self, line, pos, shard, full, width, orders, paired, send, recv):
        self.line, self.pos, self.shard, self.full, self.width = line, pos, shard, full, width
        self.orders, self.paired, self.send, self.recv = orders, paired, send, recv
        self.count = shard.shape[-1] // width
        self.depth = line + 1 + paired

    def columns(self, t, sub):
        return t * self.width + sub[1], sub[2]

    def region(self, t, sub, have, z=None):
        first, part = self.columns(t, sub)
        pz, py, px, c = self.pos
        if self.paired:
            first = first + c * self.shard.shape[-1]
        every = slice(None)
        zi = z if z is not None else (every if "z" in have else pz)
        cols = pl.ds(pl.multiple_of(first, 128), part)
        return self.full.at[zi, every if "y" in have else py, every if "x" in have else px, :, cols]

    def own(self, t, sub):
        first, part = self.columns(t, sub)
        return self.shard.at[:, pl.ds(pl.multiple_of(first, 128), part)]

    def copy(self, t, sub, slot, src, dst, who):
        return remote(src, dst, self.send.at[t, sub[0], slot], self.recv.at[t, sub[0], slot], who)

    def hop(self, t, sub, h, up, have, what):
        z, y, x, c = self.pos
        slot = (h - 1) * 2 + up
        if up:
            block, incoming, who = z - (h - 1), z - h, dev(z + 1, y, x, c)
            there, here = (z + 1 < self.line) & (z >= h - 1), z >= h
        else:
            block, incoming, who = z + (h - 1), z + h, dev(z - 1, y, x, c)
            there, here = (z > 0) & (z + h - 1 < self.line), z + h < self.line

        @pl.when(here if what == "recv" else there)
        def _():
            if what == "recv":
                r = self.region(t, sub, have, incoming)
                self.copy(t, sub, slot, r, r, dev(z, y, x, 1 - c)).wait_recv()
                return
            r = self.region(t, sub, have, block)
            cp = self.copy(t, sub, slot, self.own(t, sub) if h == 1 and not have else r, r, who)
            cp.start() if what == "start" else cp.wait_send()

    def act(self, t, sub, order, i, what):
        z, y, x, c = self.pos
        moves, have = [], ""
        for axis in order:
            moves += [(axis, h, have) for h in (range(1, self.line) if axis == "z" else (0,))]
            have += axis
        if self.paired:
            moves.append(("c", 0, have))
        axis, h, have = moves[i]
        if axis == "z":
            for up in (1, 0):
                self.hop(t, sub, h, up, have, what)
            return
        who = {"y": dev(z, 1 - y, x, c), "x": dev(z, y, 1 - x, c), "c": dev(z, y, x, 1 - c)}[axis]
        land = self.region(t, sub, have)
        cp = self.copy(t, sub, 2 * (self.line - 1) + "yxc".index(axis), land if have else self.own(t, sub), land, who)
        {"start": cp.start, "recv": cp.wait_recv, "sent": cp.wait_send}[what]()

    def each(self, t, fn):
        there = (t >= 0) & (t < self.count)
        for v, orders in enumerate(self.orders):
            turn_of = there if len(self.orders) == 1 else there & ((lax.rem(t + 3, 3) == 0) == (v == 1))

            @pl.when(turn_of)
            def _():
                for sub, (order, first, columns) in enumerate(orders):
                    fn((sub, first, columns), order)

    def step(self, t, s):
        def go(sub, order):
            if s > 0:
                self.act(t, sub, order, s - 1, "recv")
            if s < self.depth:
                self.act(t, sub, order, s, "start")

        self.each(t, go)

    def advance(self, p):
        for s in range(self.depth + 1):
            self.step(p - s, s)

    def finish(self):
        @pl.loop(0, self.count)
        def _(t):
            self.each(t, lambda sub, order: [self.act(t, sub, order, i, "sent") for i in range(self.depth)])


def own_copy(g, sem):
    z, y, x, c = g.pos
    first = c * g.shard.shape[-1] if g.paired else 0
    return pltpu.make_async_copy(g.shard, g.full.at[z, y, x, :, pl.ds(pl.multiple_of(first, 128), g.shard.shape[-1])], sem)


def rope_tables(length, width):
    half_width = width // 2
    inverse = THETA_BASE ** (-(jnp.arange(half_width, dtype=jnp.float32) * 2.0 / width))
    angles = jnp.arange(length, dtype=jnp.float32)[:, None] * inverse[None, :]
    cosine, sine = jnp.cos(angles), jnp.sin(angles)
    return jnp.concatenate([cosine, cosine], axis=1), jnp.concatenate([-sine, sine], axis=1)


def turn(x, cosine, sine):
    half = x.shape[-1] // 2
    return x * cosine + jnp.concatenate([x[:, half:], x[:, :half]], axis=1) * sine


def dot_nt(a, b):
    return lax.dot_general(a, b, (((1,), (1,)), ((), ())), preferred_element_type=jnp.float32)


def dot_tn(a, b):
    return lax.dot_general(a, b, (((0,), (0,)), ((), ())), preferred_element_type=jnp.float32)


def dot_nn(a, b):
    return jnp.dot(a, b, preferred_element_type=jnp.float32)


BLOCK = 128


def causal_weights(q, k, b, heads):
    scores = dot_nt(q, k) * (1.0 / math.sqrt(HEAD_SIZE))
    n = scores.shape[1]
    row = lax.broadcasted_iota(jnp.int32, scores.shape, 0) % BLOCK + b * BLOCK
    keep = row >= lax.broadcasted_iota(jnp.int32, scores.shape, 1)
    scores = jnp.where(keep, scores, -jnp.inf)
    log_total = jnp.log(jnp.sum(jnp.exp(scores), axis=1, keepdims=True))
    return jnp.exp(scores - log_total)


def rows_of(ref, first, heads, rows):
    return jnp.concatenate([ref[first + i, rows] for i in range(heads)], axis=0)


ROWS = 128


def each_rows(tokens, step, fn):
    @pl.loop(0, tokens // step)
    def _(r):
        fn(pl.ds(pl.multiple_of(r * step, step), step))


def forward_kernel(line, width, block, *refs):
    refs = list(refs)
    take = lambda n: [refs.pop(0) for _ in range(n)]
    query_in, key_in, value_in, gate_in, up_in, out_in, down_in, gain_a, gain_b, hid, ct, cosine, sine = take(13)
    full, gains_full, q_out, k_out, v_out, mixed_out, n1_pair, n2_pair, ct_pair, mixed_pair, middle_out = take(11)
    tile_pairs = take(3)
    hidden_out, grad_n2, gain = take(3)
    wbuf, gain_buf, n1, n2, flat, qh, kh, vh, mh, mixed, middle, acc, act, tiles, shard, gains, turned = take(17)
    send, recv, gsend, grecv, own_sem, load_sem, gain_sem, local_sem, pair_send, pair_recv, tile_local, tile_send, tile_recv, shard_sem = take(14)

    pos = place()
    z, y, x, c = pos
    tokens, d_model = hid.shape
    half = shard.shape[-1]
    heads, groups = qh.shape[0] // 2, kh.shape[0] // 2
    sibling = dev(z, y, x, 1 - c)
    bf16, f32 = jnp.bfloat16, jnp.float32

    third, half_w = width // 3, width // 2
    mixes = (
        (("zyx", 0, third), ("zxy", third, third), ("xyz", 2 * third, third // 2), ("yxz", 2 * third + third // 2, third // 2)),
        (("zyx", 0, half_w), ("zxy", half_w, half_w)),
    )
    g = Gather(line, pos, shard, full, width, mixes, 1, send, recv)
    gg = Gather(line, pos, gains, gains_full, gains.shape[-1], ((("zyx", 0, gains.shape[-1]),),), 0, gsend, grecv)
    g_own, gg_own = own_copy(g, own_sem.at[0]), own_copy(gg, own_sem.at[1])
    steps = (half // width) - 3
    fills, at = [], 0
    for src in (query_in, key_in, value_in):
        fills.append((src, at, src.shape[1]))
        at += src.shape[1]
    fills.append((out_in, at, out_in.shape[1]))
    at += out_in.shape[1]
    for j in range(steps):
        for i, src in enumerate((gate_in, up_in, down_in)):
            fills.append((src.at[:, pl.ds(j * block, block)], at + j * width + i * block, block))
    fills = [pltpu.make_async_copy(src, shard.at[:, pl.ds(to, n)], shard_sem.at[i]) for i, (src, to, n) in enumerate(fills)]
    for cp in fills:
        cp.start()
    gains[...] = jnp.zeros_like(gains)
    top = lax.broadcasted_iota(jnp.int32, (gains.shape[0], gain_a.shape[1]), 0) == 0
    gains[:, : gain_a.shape[1]] = jnp.where(top, gain_a[...].astype(f32), gain_b[...].astype(f32)).astype(bf16)
    enter(line, pos)
    for cp in fills:
        cp.wait()
    g_own.start()
    gg_own.start()

    def load(t, hh, slot):
        cols = pl.ds(pl.multiple_of(hh * half + t * width, 128), width)
        return pltpu.make_async_copy(full.at[:, :, :, :, cols], wbuf.at[slot, hh], load_sem.at[slot, hh])

    def weight(slot, hh):
        return wbuf[slot, hh].reshape(d_model, width)

    def share(i, own_src, own_dst, other_src, other_dst):
        return pltpu.make_async_copy(own_src, own_dst, local_sem.at[i]), remote(other_src, other_dst, pair_send.at[i], pair_recv.at[i], sibling)

    ends = (pl.ds(0, tokens), pl.ds(tokens, tokens))
    lefts = ((ct, ct_pair), (n1, n1_pair), (n2, n2_pair))
    shares = [share(i, turned.at[i], pair.at[:, ends[0]], turned.at[i], pair.at[:, ends[1]]) for i, (_, pair) in enumerate(lefts)]
    hw = mixed.shape[1] // 2
    side = lambda ref, s, w: ref.at[:, pl.ds(pl.multiple_of(s * w, 128), w)]
    shares.append(share(3, side(mixed, c, hw), mixed_pair.at[0], side(mixed, 1 - c, hw), mixed_pair.at[1]))
    keeps = [pltpu.make_async_copy(src, dst, local_sem.at[4 + i]) for i, (src, dst) in enumerate(((qh, q_out), (kh, k_out), (vh, v_out), (mixed, mixed_out), (middle, middle_out)))]

    def begin(i):
        if i < len(lefts):
            span = 256

            @pl.loop(0, d_model // span)
            def _(e):
                at = pl.ds(pl.multiple_of(e * span, span), span)
                turned[i, at, :] = lefts[i][0][:, at].T

        for cp in shares[i]:
            cp.start()

    def end(i):
        for cp in shares[i]:
            cp.wait()

    def tile_copies(j, hh):
        slot = lax.rem(j, 2)
        cols = pl.ds(pl.multiple_of(j * block, 128), block)
        own = [pltpu.make_async_copy(tiles.at[slot, hh, i], pair.at[0, :, cols], tile_local.at[j, i]) for i, pair in enumerate(tile_pairs)]
        out = [remote(tiles.at[slot, hh, i], pair.at[1, :, cols], tile_send.at[j, i], tile_recv.at[j, i], sibling) for i, pair in enumerate(tile_pairs)]
        return own, out

    def drain_tiles(j):
        for cp in tile_copies(j, 0)[0]:
            cp.wait()
        for cp in tile_copies(j, 0)[1]:
            cp.wait_send()

    def normalize():
        loaded = pltpu.make_async_copy(gains_full, gain_buf, gain_sem)
        loaded.start()
        loaded.wait()
        n = d_model // (gain_buf.shape[0] * 4)
        table = gain_buf[...].astype(f32)
        for i in range(2):
            gain[i : i + 1, :] = jnp.concatenate([table[a, b, e, i : i + 1, :n] for a in range(gain_buf.shape[0]) for b in range(2) for e in range(2)], axis=1)

        def rows_of_norm(rows):
            v = hid[rows, :].astype(f32)
            v = v * lax.rsqrt(jnp.mean(v * v, axis=1, keepdims=True) + EPSILON)
            n1[rows, :] = (v * gain[0:1, :]).astype(bf16)

        each_rows(tokens, ROWS, rows_of_norm)
        begin(1)

    def project(slot, outs):
        @pl.loop(0, 2)
        def _(hh):
            flat[...] = dot_nn(n1[...], weight(slot, hh))

            def to_heads(rows):
                cos, sin = cosine[rows, :], sine[rows, :]
                first = 0
                for n, target, turned in outs:
                    for h in range(n):
                        v = flat[rows, (first + h) * HEAD_SIZE : (first + h + 1) * HEAD_SIZE]
                        target[hh * n + h, rows] = (turn(v, cos, sin) if turned else v).astype(bf16)
                    first += n

            each_rows(tokens, ROWS, to_heads)

    def attend_half(hh):
        per = heads // groups
        blocks = tokens // BLOCK

        @pl.loop(0, groups)
        def _(i):
            kv = hh * groups + i
            for b in range(blocks):
                rows, n = pl.ds(b * BLOCK, BLOCK), (b + 1) * BLOCK
                w = causal_weights(rows_of(qh, kv * per, per, rows), kh[kv, :n], b, per).astype(bf16)
                m = dot_nn(w, vh[kv, :n]).astype(bf16)
                for e in range(per):
                    mh[kv * per + e, rows] = m[e * BLOCK : (e + 1) * BLOCK]

    def leave_attention(slot):
        def join(rows):
            mixed[rows, :] = jnp.concatenate([mh[h, rows] for h in range(2 * heads)], axis=1)

        each_rows(tokens, ROWS, join)
        begin(3)
        for cp in keeps[:4]:
            cp.start()
        middle[...] = hid[...].astype(f32) + dot_nt(mixed[:, :hw], weight(slot, 0))
        middle[...] += dot_nt(mixed[:, hw:], weight(slot, 1))

        def rows_of_norm(rows):
            v = middle[rows, :]
            acc[rows, :] = v
            v = v * lax.rsqrt(jnp.mean(v * v, axis=1, keepdims=True) + EPSILON)
            n2[rows, :] = (v * gain[1:2, :]).astype(bf16)
            grad_n2[rows, :] = jnp.zeros_like(v)

        keeps[4].start()
        each_rows(tokens, ROWS, rows_of_norm)
        begin(2)

    def feed_forward(j, slot):
        @pl.when(j >= 2)
        def _():
            drain_tiles(j - 2)

        part = lax.rem(j, 2)

        @pl.loop(0, 2)
        def _(hh):
            act[0] = dot_nn(n2[...], weight(slot, hh)[:, :block])
            act[1] = dot_nn(n2[...], weight(slot, hh)[:, block : 2 * block])
            act[2] = dot_nn(ct[...], weight(slot, hh)[:, 2 * block :])

            def gated(rows):
                gate, up, grad = act[0, rows], act[1, rows], act[2, rows]
                sigma = jax.nn.sigmoid(gate)
                tiles[part, hh, 0, rows] = (gate * sigma * up).astype(bf16)
                tiles[part, hh, 1, rows] = (grad * up * sigma * (1.0 + gate * (1.0 - sigma))).astype(bf16)
                tiles[part, hh, 2, rows] = (grad * gate * sigma).astype(bf16)

            each_rows(tokens, ROWS // 2, gated)
            own, out = tile_copies(j, hh)

            @pl.when(hh == c)
            def _():
                for cp in own:
                    cp.start()

            @pl.when(hh != c)
            def _():
                for cp in out:
                    cp.start()

            acc[...] += dot_nt(tiles[part, hh, 0], weight(slot, hh)[:, 2 * block :])
            both = jnp.concatenate([tiles[part, hh, 1], tiles[part, hh, 2]], axis=1)
            grad_n2[...] += dot_nt(both, weight(slot, hh)[:, : 2 * block])

    count, lead = g.count, g.depth + 1

    @pl.loop(0, count + lead)
    def _(p):
        @pl.when(p == 0)
        def _():
            g_own.wait()
            gg_own.wait()
            begin(0)

        gg.advance(p)
        g.advance(p)
        u = p - lead

        @pl.when((u >= -1) & (u + 1 < count))
        def _():
            for hh in range(2):
                load(u + 1, hh, lax.rem(u + 1, 2)).start()

        @pl.when(u >= 0)
        def _():
            slot = lax.rem(u, 2)
            for hh in range(2):
                load(u, hh, slot).wait()

            @pl.when(u == 0)
            def _():
                normalize()
                project(slot, ((heads, qh, True),))

            @pl.when(u == 1)
            def _():
                project(slot, ((groups, kh, True), (groups, vh, False)))
                attend_half(0)

            @pl.when(u == 2)
            def _():
                attend_half(1)
                leave_attention(slot)

            @pl.when(u >= 3)
            def _():
                feed_forward(u - 3, slot)

    def rows_out(rows):
        hidden_out[rows, :] = acc[rows, :].astype(bf16)

    each_rows(tokens, ROWS, rows_out)
    for i in range(len(shares)):
        end(i)
    for cp in keeps:
        cp.wait()
    for j in range(max(steps - 2, 0), steps):
        drain_tiles(j)

    @pl.loop(0, steps)
    def _(j):
        for cp in tile_copies(j, 0)[1]:
            cp.wait_recv()

    g.finish()
    gg.finish()


def forward(line, shards, gain_pair, hidden_in, cotangent, cosine, sine, block):
    tokens, d_model = hidden_in.shape
    rows = gain_pair[0].shape[1]
    half = sum(s.shape[1] for s in shards)
    gains = jax.ShapeDtypeStruct((8, 128), jnp.bfloat16)
    width = 3 * block
    count = half // width
    steps = count - 3
    heads, groups = QUERY_HEADS // 2, KEY_VALUE_HEADS // 2
    bf16, f32 = jnp.bfloat16, jnp.float32
    struct = jax.ShapeDtypeStruct
    hbm, vmem = pl.BlockSpec(memory_space=pl.ANY), pl.BlockSpec(memory_space=pltpu.VMEM)
    dma = pltpu.SemaphoreType.DMA
    pair = struct((d_model, 2 * tokens), bf16)
    tile_pair = struct((2, tokens, steps * block), bf16)
    head_shape = lambda n: (n, tokens, HEAD_SIZE)
    slots = 2 * (line - 1) + 3
    outs = [
        struct((line, 2, 2, rows, 2 * half), bf16),
        struct((line, 2, 2) + gains.shape, bf16),
        struct(head_shape(2 * heads), bf16),
        struct(head_shape(2 * groups), bf16),
        struct(head_shape(2 * groups), bf16),
        struct((tokens, 2 * heads * HEAD_SIZE), bf16),
        pair,
        pair,
        pair,
        struct((2, tokens, heads * HEAD_SIZE), bf16),
        struct((tokens, d_model), f32),
        tile_pair,
        tile_pair,
        tile_pair,
        struct((tokens, d_model), bf16),
        struct((tokens, d_model), f32),
        struct((8, d_model), f32),
    ]
    V = pltpu.VMEM
    return pl.pallas_call(
        functools.partial(forward_kernel, line, width, block),
        out_shape=outs,
        in_specs=[hbm] * 7 + [vmem] * 6,
        out_specs=[hbm] * 14 + [vmem] * 3,
        scratch_shapes=[
            V((2, 2, line, 2, 2, rows, width), bf16),
            V((line, 2, 2) + gains.shape, bf16),
            V((tokens, d_model), bf16),
            V((tokens, d_model), bf16),
            V((tokens, width), f32),
            V(head_shape(2 * heads), bf16),
            V(head_shape(2 * groups), bf16),
            V(head_shape(2 * groups), bf16),
            V(head_shape(2 * heads), bf16),
            V((tokens, 2 * heads * HEAD_SIZE), bf16),
            V((tokens, d_model), f32),
            V((tokens, d_model), f32),
            V((3, tokens, block), f32),
            V((2, 2, 3, tokens, block), bf16),
            V((rows, half), bf16),
            V(gains.shape, bf16),
            V((3, d_model, tokens), bf16),
            dma((count, 4, slots)),
            dma((count, 4, slots)),
            dma((1, 1, slots)),
            dma((1, 1, slots)),
            dma((2,)),
            dma((2, 2)),
            dma,
            dma((9,)),
            dma((4,)),
            dma((4,)),
            dma((steps, 3)),
            dma((steps, 3)),
            dma((steps, 3)),
            dma((4 + 3 * steps,)),
        ],
        compiler_params=pltpu.CompilerParams(collective_id=0, has_side_effects=True, vmem_limit_bytes=64 * 2**20 - 2**17),
        name="gather_forward",
    )(*shards, *gain_pair, hidden_in, cotangent, cosine, sine)


class Scatter:
    def __init__(self, line, pos, count, own, first, second, up, down, send, recv, final):
        self.line, self.pos, self.count, self.final = line, pos, count, final
        self.own, self.first, self.second, self.up, self.down, self.send, self.recv = own, first, second, up, down, send, recv
        self.ring, self.own_ring = first.shape[0], own.shape[0]
        self.lags = [0, 2, 4] + [5 + j for j in range(line - 1)] + [4 + line, 5 + line]
        self.depth = self.lags[-1]

    def copy(self, t, slot, src, dst, who):
        r = lax.rem(t, self.ring)
        return remote(src, dst, self.send.at[r, slot], self.recv.at[r, slot], who)

    def merge(self, dst, a, b, loops):
        def go(lead, rest):
            if not rest:
                dst[lead] = a[lead] + b[lead]
            elif rest[0] > 2:
                @pl.loop(0, rest[0])
                def _(i):
                    go(lead + (i,), rest[1:])
            else:
                for i in range(rest[0]):
                    go(lead + (i,), rest[1:])

        go((), loops)

    def pair_moves(self, t, v):
        z, y, x, c = self.pos
        r, o = lax.rem(t, self.ring), lax.rem(t, self.own_ring)
        own, first, second = self.own.at[o], self.first.at[r], self.second.at[r]
        over_x, over_y = dev(z, y, 1 - x, c), dev(z, 1 - y, x, c)
        if v == 0:
            give, keep, who = own.at[:, :, 1 - x], own.at[:, :, x], (over_x, over_y)
        else:
            give, keep, who = own.at[:, 1 - y], own.at[:, y], (over_y, over_x)
        a, b = (1 - y, y) if v == 0 else (1 - x, x)
        one = self.copy(t, 0, give, first, who[0])
        two = self.copy(t, 1, first.at[:, a], second, who[1])
        return one, two, keep, first, second, first.at[:, b]

    def hop(self, p, j, way):
        z, y, x, c = self.pos
        last = self.line - 1
        travelled = z if way == 0 else last - z
        t = p - self.lags[3] - j - travelled
        target = last - j if way == 0 else j
        passes = (target > z) if way == 0 else (target < z)

        def go():
            r = lax.rem(t, self.ring)
            cur, ref = self.second.at[r], (self.up if way == 0 else self.down).at[r, j]
            nxt = dev(z + 1, y, x, c) if way == 0 else dev(z - 1, y, x, c)

            @pl.when(travelled == 0)
            def _():
                self.copy(t, 2 + 2 * j + way, cur.at[target], ref, nxt).start()

            @pl.when(travelled > 0)
            def _():
                cp = self.copy(t, 2 + 2 * j + way, ref, ref, nxt)
                cp.wait_recv()
                ref[...] = ref[...] + cur[target]
                cp.start()

        @pl.when(passes & (t >= 0) & (t < self.count))
        def _():
            go()

    def close(self, t):
        z, y, x, c = self.pos
        r = lax.rem(t, self.ring)
        ku, kd = self.line - 1 - z, z
        has_up, has_down = z > 0, z < self.line - 1
        for has, way, ref, k in ((has_up, 0, self.up, ku), (has_down, 1, self.down, kd)):

            @pl.when(has)
            def _():
                self.copy(t, 2 + 2 * k + way, ref.at[r, k], ref.at[r, k], dev(z, y, x, 1 - c)).wait_recv()

        f32 = jnp.float32
        total = self.second[r, z].astype(f32)
        last = self.line - 2
        below = self.up[r, jnp.minimum(ku, last)].astype(f32)
        above = self.down[r, jnp.minimum(kd, last)].astype(f32)
        total = total + jnp.where(has_up, below, 0.0) + jnp.where(has_down, above, 0.0)
        self.final(t, total)

    def drain(self, t):
        z, y, x, c = self.pos
        r = lax.rem(t, self.ring)
        self.pair_moves(t, 0)[1].wait_send()
        for j in range(self.line - 1):
            for way, ref, target in ((0, self.up, self.line - 1 - j), (1, self.down, j)):

                @pl.when((target > z) if way == 0 else (target < z))
                def _():
                    self.copy(t, 2 + 2 * j + way, ref.at[r, j], ref.at[r, j], dev(z, y, x, 1 - c)).wait_send()

    def when(self, t, fn):
        @pl.when((t >= 0) & (t < self.count))
        def _():
            fn()

    def both(self, t, fn):
        for v in range(2):
            @pl.when((t >= 0) & (t < self.count) & (lax.rem(t + 2, 2) == v))
            def _():
                fn(v)

    def begin(self, t):
        self.both(t, lambda v: self.pair_moves(t, v)[0].start())

    def release(self, t):
        self.when(t, lambda: self.pair_moves(t, 0)[0].wait_send())

    def advance(self, p):
        line = self.line

        def one(v, t):
            first_copy, second_copy, keep, first, second, _ = self.pair_moves(t, v)
            first_copy.wait_recv()
            self.merge(first, first, keep, (line, 2))
            second_copy.start()

        def two(v, t):
            _, second_copy, _, _, second, keep = self.pair_moves(t, v)
            second_copy.wait_recv()
            self.merge(second, second, keep, (line,))

        t = p - self.lags[1]
        self.both(t, lambda v, t=t: one(v, t))
        t = p - self.lags[2]
        self.both(t, lambda v, t=t: two(v, t))
        for j in range(line - 1):
            for way in range(2):
                self.hop(p, j, way)
        t = p - self.lags[-2]
        self.when(t, lambda t=t: self.close(t))
        t = p - self.lags[-1]
        self.when(t, lambda t=t: self.drain(t))


def greet_all(n, pos):
    z, y, x, c = pos
    d = z * 4 + y * 2 + x
    barrier = pltpu.get_barrier_semaphore()

    @pl.loop(1, n)
    def _(i):
        pl.semaphore_signal(barrier, inc=1, device_id=(lax.rem(d + i, n), c), device_id_type=MESH)

    pl.semaphore_signal(barrier, inc=1, device_id=(d, 1 - c), device_id_type=MESH)
    pl.semaphore_wait(barrier, n)


def backward_kernel(line, cols, starts, *refs):
    refs = list(refs)
    take = lambda n: [refs.pop(0) for _ in range(n)]
    q, k, v, mixed, full, hid, ct, middle, grad_n2, gains, cosine, sine = take(12)
    n1_pair, n2_pair, ct_pair, mixed_pair, hidden_pair, gate_pair, up_pair = take(7)
    qkv_pair, grad_query, grad_key, grad_value, grad_in, out_out, out_gate, out_up, out_down, out_gains, gm_pair = take(11)
    own, first, second, up, down, xt, ybuf, qh, kh, vh, mh, gh, gm, dots, dq, dk, dv, dqkv, wbuf, gmid, hbuf, out_qkv, gain_one, part, parts_in, pair_in, gain_two, gmb, turned = take(29)
    send, recv, xsem, ysem, half_sem, wsem, msem, qkv_local, qkv_send, qkv_recv, part_send, part_recv, out_sem, swap_sem, gm_sem = take(15)

    pos = place()
    z, y, x, c = pos
    d = z * 4 + y * 2 + x
    n = line * 4
    tokens, d_model = hid.shape
    count = starts[-1]
    heads, groups = qh.shape[0], kh.shape[0]
    share = heads // groups
    blocks = tokens // BLOCK
    width = wbuf.shape[-1]
    half_width = dqkv.shape[1] // 2
    scale = 1.0 / math.sqrt(HEAD_SIZE)
    bf16, f32 = jnp.bfloat16, jnp.float32
    sources = (hidden_pair, gate_pair, up_pair, mixed_pair, qkv_pair)
    lefts = ((0, ct_pair), (starts[1], n2_pair), (starts[3], gm_pair), (starts[4], n1_pair))

    def final(t, total):
        for i, out in enumerate((out_down, out_gate, out_up, out_out, out_qkv)):
            at = pl.ds(pl.multiple_of((t - starts[i]) * cols, 128), cols)

            @pl.when((t >= starts[i]) & (t < starts[i + 1]))
            def _():
                out[:, at] = total

    s = Scatter(line, pos, count, own, first, second, up, down, send, recv, final)

    def load_left(i):
        return pltpu.make_async_copy(lefts[i][1], xt.at[i % 2], xsem.at[i % 2])

    def load_right(t, act):
        slot = lax.rem(t, 2)
        for i, src in enumerate(sources):
            at = pl.ds(pl.multiple_of((t - starts[i]) * cols, 128), cols)

            @pl.when((t >= starts[i]) & (t < starts[i + 1]))
            def _():
                cp = pltpu.make_async_copy(src.at[:, :, at], ybuf.at[slot], ysem.at[slot])
                cp.start() if act == "start" else cp.wait()

    def half_loads(hh):
        take_heads = lambda ref, m: ref.at[pl.ds(hh * m, m)]
        lanes = pl.ds(pl.multiple_of(hh * mh.shape[1], 128), mh.shape[1])
        pairs = ((take_heads(q, heads), qh), (take_heads(k, groups), kh), (take_heads(v, groups), vh), (mixed.at[:, lanes], mh))
        return [pltpu.make_async_copy(src, dst, half_sem.at[i]) for i, (src, dst) in enumerate(pairs)]

    def half_load(hh, act):
        for cp in half_loads(hh):
            cp.start() if act == "start" else cp.wait()

    each = half_width // width
    half_columns = full.shape[-1] // 2

    def weights(i):
        at = (i * half_columns + each * width) if i < 2 else ((i - 2) // each * half_columns + (i - 2) % each * width)
        return pltpu.make_async_copy(full.at[:, :, :, :, pl.ds(at, width)], wbuf.at[i % 2], wsem.at[i % 2])

    def weight(i):
        return wbuf[i % 2].reshape(d_model, width)

    middle_in = pltpu.make_async_copy(middle, grad_in, msem.at[0])
    grad_n2_in = pltpu.make_async_copy(grad_n2, gmid, msem.at[1])
    ct_in, hid_in = (pltpu.make_async_copy(src, hbuf, msem.at[2]) for src in (ct, hid))

    own_half = lambda ref, which: ref.at[:, pl.ds(pl.multiple_of(which * half_width, 128), half_width)]

    def qkv_copies():
        return (
            pltpu.make_async_copy(own_half(dqkv, c), qkv_pair.at[0], qkv_local),
            remote(own_half(dqkv, 1 - c), qkv_pair.at[1], qkv_send, qkv_recv, (d, 1 - c)),
        )

    def gm_copies():
        return (
            pltpu.make_async_copy(turned, gm_pair.at[:, pl.ds(0, tokens)], gm_sem.at[0]),
            remote(turned, gm_pair.at[:, pl.ds(tokens, tokens)], gm_sem.at[1], gm_sem.at[2], (d, 1 - c)),
        )

    def norm_two_back():
        for cp in (middle_in, grad_n2_in, ct_in):
            cp.wait()
        gain_two[...] = jnp.zeros_like(gain_two)

        def rows_back(rows):
            a, grad = grad_in[rows, :], gmid[rows, :]
            inverse = lax.rsqrt(jnp.mean(a * a, axis=1, keepdims=True) + EPSILON)
            unit = a * inverse
            scaled = grad * gains[1:2, :]
            inner = jnp.mean(scaled * unit, axis=1, keepdims=True)
            total = hbuf[rows, :].astype(f32) + inverse * (scaled - unit * inner)
            gmid[rows, :] = total
            gmb[rows, :] = total.astype(bf16)
            gain_two[...] += jnp.sum(grad * unit, axis=0, keepdims=True)

        each_rows(tokens, ROWS, rows_back)
        hid_in.start()
        span = 256

        @pl.loop(0, d_model // span)
        def _(e):
            at = pl.ds(pl.multiple_of(e * span, span), span)
            turned[at, :] = gmb[:, at].T

        for cp in gm_copies():
            cp.start()

    def through_out(i):
        weights(i).wait()
        gh[...] = dot_nn(gmb[...], weight(i))
        weights(i + 2).start()

    def prepare(hh):
        half_load(hh, "wait")

        def rows_of_dots(rows):
            for h in range(heads):
                lanes = slice(h * HEAD_SIZE, (h + 1) * HEAD_SIZE)
                g = gh[rows, lanes]
                dots[h, rows] = jnp.sum(g * mh[rows, lanes].astype(f32), axis=1, keepdims=True)
                gm[h, rows] = g.astype(bf16)

        each_rows(tokens, ROWS, rows_of_dots)
        dk[...] = jnp.zeros_like(dk)
        dv[...] = jnp.zeros_like(dv)

    def group_back(g, which):
        for b in which:
            rows, m = pl.ds(b * BLOCK, BLOCK), (b + 1) * BLOCK
            qb, gb, db = (rows_of(ref, g * share, share, rows) for ref in (qh, gm, dots))
            kb, vb = kh[g, :m], vh[g, :m]
            p = causal_weights(qb, kb, b, share)
            ds = (p * (dot_nt(gb, vb) - db)).astype(bf16)
            dv[g, :m] += dot_tn(p.astype(bf16), gb)
            dk[g, :m] += dot_tn(ds, qb)
            r = dot_nn(ds, kb) * scale
            for i in range(share):
                dq[g * share + i, rows] = r[i * BLOCK : (i + 1) * BLOCK]

    def join(hh):
        def rows_of_join(rows):
            cos, sin = cosine[rows, :], -sine[rows, :]
            parts = [turn(dq[h, rows], cos, sin) for h in range(heads)]
            parts += [turn(dk[g, rows] * scale, cos, sin) for g in range(groups)]
            parts += [dv[g, rows] for g in range(groups)]
            dqkv[rows, pl.ds(pl.multiple_of(hh * half_width, 128), half_width)] = jnp.concatenate([a.astype(bf16) for a in parts], axis=1)

        each_rows(tokens, ROWS, rows_of_join)

    def against(i):
        weights(i + 2).wait()
        r = dot_nt(dqkv[:, i * width : (i + 1) * width], weight(i))
        if i == 0:
            grad_in[...] = r
        else:
            grad_in[...] += r
        if i + 2 < 2 * each:
            weights(i + 4).start()

    def norm_one_back():
        hid_in.wait()
        gain_one[...] = jnp.zeros_like(gain_one)

        def rows_back(rows):
            a = hbuf[rows, :].astype(f32)
            inverse = lax.rsqrt(jnp.mean(a * a, axis=1, keepdims=True) + EPSILON)
            unit, grad = a * inverse, grad_in[rows, :]
            scaled = grad * gains[0:1, :]
            inner = jnp.mean(scaled * unit, axis=1, keepdims=True)
            grad_in[rows, :] = gmid[rows, :] + inverse * (scaled - unit * inner)
            gain_one[...] += jnp.sum(grad * unit, axis=0, keepdims=True)

        each_rows(tokens, ROWS, rows_back)
        size = d_model // n
        part[...] = jnp.zeros_like(part)
        for i in range(n):
            for row, ref in enumerate((gain_one, gain_two)):
                part[i, row : row + 1, :size] = ref[:, i * size : (i + 1) * size]

    def part_copy(i):
        to = lax.rem(d + i, n)
        return remote(part.at[to], parts_in.at[i], part_send.at[i], part_recv.at[i], (to, c))

    load_left(0).start()
    load_left(1).start()
    load_right(0, "start")
    half_load(0, "start")
    for cp in (middle_in, grad_n2_in, ct_in):
        cp.start()
    for i in range(2):
        weights(i).start()
    greet_all(n, pos)

    stages = 2 * groups + 3
    turns = 1 + 2 * stages
    norm_at = turns + 2 * each

    @pl.loop(0, count + s.depth)
    def _(p):
        s.release(p - s.own_ring)
        for i, (at, _) in enumerate(lefts):

            @pl.when(p == at)
            def _():
                load_left(i).wait()
                if 1 <= i < len(lefts) - 1:
                    load_left(i + 1).start()

        @pl.when(p == starts[1] - 1)
        def _():
            for cp in gm_copies():
                cp.wait()

        @pl.when(p == starts[4] - 2)
        def _():
            for cp in qkv_copies():
                cp.wait()

        @pl.when(p < count)
        def _():
            load_right(p, "wait")

            @pl.when(p + 1 < count)
            def _():
                load_right(p + 1, "start")

            side = lax.rem(sum((p >= at).astype(jnp.int32) for at, _ in lefts[1:]), 2)
            right = ybuf[lax.rem(p, 2)].reshape(2 * tokens, cols)
            own[lax.rem(p, s.own_ring)] = dot_nn(xt[side], right).reshape(own.shape[1:]).astype(bf16)
            s.begin(p)

        s.advance(p)

        @pl.when(p == 0)
        def _():
            norm_two_back()

        for i in range(2):

            @pl.when(p == 1 + i * stages)
            def _():
                through_out(i)

        @pl.when((p > 0) & (p < turns))
        def _():
            hh, r = lax.div(p - 1, stages), lax.rem(p - 1, stages) - 1

            @pl.when(r == 0)
            def _():
                prepare(hh)

            for e, which in enumerate((range(blocks - 1), range(blocks - 1, blocks))):

                @pl.when((r > 0) & (r <= 2 * groups) & (lax.rem(r + 1, 2) == e))
                def _():
                    group_back(lax.div(r - 1, 2), which)

            @pl.when(r == stages - 2)
            def _():
                join(hh)

                @pl.when(hh == 0)
                def _():
                    half_load(1, "start")

                @pl.when(hh == 1)
                def _():
                    for cp in qkv_copies():
                        cp.start()

        for i in range(2 * each):

            @pl.when(p == turns + i)
            def _():
                against(i)

        @pl.when(p == norm_at)
        def _():
            norm_one_back()

        @pl.when(p == norm_at + 1)
        def _():
            @pl.loop(1, n)
            def _(i):
                part_copy(i).start()

    total = part[d]

    @pl.loop(1, n)
    def _(i):
        part_copy(i).wait()

    total = total + jnp.sum(parts_in[1:], axis=0)
    out_gains[...] = total
    swap = remote(out_gains, pair_in, swap_sem.at[0], swap_sem.at[1], (d, 1 - c))
    swap.start()
    first_column = 0
    for i, out in enumerate((grad_query, grad_key, grad_value)):
        cp = pltpu.make_async_copy(out_qkv.at[:, pl.ds(first_column, out.shape[1])], out, out_sem.at[i])
        cp.start()
        cp.wait()
        first_column += out.shape[1]
    swap.wait()
    out_gains[...] += pair_in[...]
    for t in range(count - s.own_ring + s.depth, count):
        s.release(t)


def backward(line, cols, arrays, halves):
    q, k, v, mixed, full, hid = arrays[:6]
    tokens, d_model = hid.shape
    rows = full.shape[3]
    n = line * 4
    down_w, gate_w, up_w, out_w, q_w, k_w, v_w = halves
    qkv_w = q_w + k_w + v_w
    starts = [0]
    for w in (down_w, gate_w, up_w, out_w, qkv_w):
        starts.append(starts[-1] + w // cols)
    heads, groups = q.shape[0] // 2, k.shape[0] // 2
    width = q_w
    bf16, f32 = jnp.bfloat16, jnp.float32
    struct, V, dma = jax.ShapeDtypeStruct, pltpu.VMEM, pltpu.SemaphoreType.DMA
    hbm, vmem = pl.BlockSpec(memory_space=pl.ANY), pl.BlockSpec(memory_space=pltpu.VMEM)
    ring, own_ring = line + 12, 4
    head = lambda m: (m, tokens, HEAD_SIZE)
    sems = 2 + 2 * (line - 1)
    outs = [struct((2, tokens, qkv_w), bf16)]
    outs += [struct((rows, w), f32) for w in (q_w, k_w, v_w)]
    outs += [struct((tokens, d_model), f32), struct((rows, out_w), f32), struct((rows, gate_w), f32), struct((rows, up_w), f32), struct((rows, down_w), f32), struct((8, 128), f32)]
    outs += [struct((d_model, 2 * tokens), bf16)]
    return pl.pallas_call(
        functools.partial(backward_kernel, line, cols, tuple(starts)),
        out_shape=outs,
        in_specs=[hbm] * 9 + [vmem] * 3 + [hbm] * 7,
        out_specs=[hbm] * 4 + [vmem] * 6 + [hbm],
        scratch_shapes=[
            V((own_ring, line, 2, 2, rows, cols), bf16),
            V((ring, line, 2, rows, cols), bf16),
            V((ring, line, rows, cols), bf16),
            V((ring, line - 1, rows, cols), bf16),
            V((ring, line - 1, rows, cols), bf16),
            V((2, d_model, 2 * tokens), bf16),
            V((2, 2, tokens, cols), bf16),
            V(head(heads), bf16),
            V(head(groups), bf16),
            V(head(groups), bf16),
            V((tokens, heads * HEAD_SIZE), bf16),
            V((tokens, heads * HEAD_SIZE), f32),
            V(head(heads), bf16),
            V((heads, tokens, 1), f32),
            V(head(heads), f32),
            V(head(groups), f32),
            V(head(groups), f32),
            V((tokens, 2 * qkv_w), bf16),
            V((2, line, 2, 2, rows, width), bf16),
            V((tokens, d_model), f32),
            V((tokens, d_model), bf16),
            V((rows, qkv_w), f32),
            V((1, d_model), f32),
            V((n, 8, 128), f32),
            V((n, 8, 128), f32),
            V((8, 128), f32),
            V((1, d_model), f32),
            V((tokens, d_model), bf16),
            V((d_model, tokens), bf16),
            dma((ring, sems)),
            dma((ring, sems)),
            dma((2,)),
            dma((2,)),
            dma((4,)),
            dma((2,)),
            dma((3,)),
            dma,
            dma,
            dma,
            dma((n,)),
            dma((n,)),
            dma((3,)),
            dma((2,)),
            dma((3,)),
        ],
        compiler_params=pltpu.CompilerParams(collective_id=1, has_side_effects=True, vmem_limit_bytes=64 * 2**20 - 2**17),
        name="backward_scatter",
    )(*arrays)


def finish_kernel(n, *refs):
    srcs, outs, bufs, (loads, stores) = refs[:n], refs[n : 2 * n], refs[2 * n : 3 * n], refs[3 * n :]
    for i in range(n):
        pltpu.make_async_copy(srcs[i], bufs[i], loads.at[i]).start()
    for i in range(n):
        pltpu.make_async_copy(srcs[i], bufs[i], loads.at[i]).wait()
        pltpu.make_async_copy(bufs[i], outs[i], stores.at[i]).start()
    for i in range(n):
        pltpu.make_async_copy(bufs[i], outs[i], stores.at[i]).wait()


def finish(arrays):
    n = len(arrays)
    hbm = pl.BlockSpec(memory_space=pl.ANY)
    return pl.pallas_call(
        functools.partial(finish_kernel, n),
        out_shape=[jax.ShapeDtypeStruct(a.shape, a.dtype) for a in arrays],
        in_specs=[hbm] * n,
        out_specs=[hbm] * n,
        scratch_shapes=[pltpu.VMEM(a.shape, a.dtype) for a in arrays] + [pltpu.SemaphoreType.DMA((n,)), pltpu.SemaphoreType.DMA((n,))],
        compiler_params=pltpu.CompilerParams(vmem_limit_bytes=64 * 2**20 - 2**17),
        name="finish",
    )(*arrays)


def layer(n_dp, n_tensor, hidden_in, query_weight, key_matrix, value_matrix, out_weight, gate_weight, up_weight, down_weight, attention_gain, feedforward_gain, cotangent):
    line = n_dp // 4
    rows = attention_gain.shape[0]
    block = (query_weight.shape[1] // 3) & -128
    cosine, sine = rope_tables(SEQUENCE_LENGTH, HEAD_SIZE)
    (full, _, q, k, v, mixed, n1, n2, ct, mixed_pair, middle, hidden, gate, up, hidden_out, grad_n2, gain_rows) = forward(
        line,
        (query_weight, key_matrix, value_matrix, gate_weight, up_weight, out_weight.T, down_weight.T),
        (attention_gain.reshape(1, rows), feedforward_gain.reshape(1, rows)),
        hidden_in,
        cotangent,
        cosine,
        sine,
        block,
    )
    arrays = (q, k, v, mixed, full, hidden_in, cotangent, middle, grad_n2, gain_rows, cosine, sine, n1, n2, ct, mixed_pair, hidden, gate, up)
    halves = (down_weight.shape[0], gate_weight.shape[1], up_weight.shape[1], out_weight.shape[0], query_weight.shape[1], key_matrix.shape[1], value_matrix.shape[1])
    results = backward(line, 256 if line <= 4 else 128, arrays, halves)
    g_query, g_key, g_value, grad_in, g_out, g_gate, g_up, g_down, hidden_out = finish(list(results[1:9]) + [hidden_out])
    g_gains = results[9]
    return hidden_out, grad_in, g_query, g_key, g_value, g_out.T, g_gate, g_up, g_down.T, g_gains[0, :rows], g_gains[1, :rows]


def solution(mesh):
    split = P(("dp", "tensor"), None)
    row, column, gain = P("dp", "tensor"), P("tensor", "dp"), P("dp")
    return jax.shard_map(
        functools.partial(layer, mesh.shape["dp"], mesh.shape["tensor"]),
        mesh=mesh,
        in_specs=(split, row, row, row, column, row, row, column, gain, gain, split),
        out_specs=(split, split, row, row, row, column, row, row, column, gain, gain),
        check_vma=False,
    )
```

```python
import functools
import math

import jax
import jax.numpy as jnp
from jax import lax
from jax.experimental import pallas as pl
from jax.experimental.pallas import tpu as pltpu
from jax.sharding import PartitionSpec as P

QUERY_HEADS = 16
KEY_VALUE_HEADS = 8
HEAD_SIZE = 96
SEQUENCE_LENGTH = 512

EPSILON = 1e-05
THETA_BASE = 100000.0
MESH = pl.DeviceIdType.MESH


def place():
    d = lax.axis_index("dp")
    return lax.div(d, 4), lax.rem(lax.div(d, 2), 2), lax.rem(d, 2), lax.axis_index("tensor")


def dev(z, y, x, c):
    return (z * 4 + y * 2 + x, c)


def enter(line, pos):
    z, y, x, c = pos
    barrier = pltpu.get_barrier_semaphore()

    def greet(who):
        pl.semaphore_signal(barrier, inc=1, device_id=who, device_id_type=MESH)

    greet(dev(z, y, x, 1 - c))
    greet(dev(z, y, 1 - x, c))
    greet(dev(z, 1 - y, x, c))

    @pl.when(z > 0)
    def _():
        greet(dev(z - 1, y, x, c))

    @pl.when(z < line - 1)
    def _():
        greet(dev(z + 1, y, x, c))

    pl.semaphore_wait(barrier, 3 + (z > 0).astype(jnp.int32) + (z < line - 1).astype(jnp.int32))


def remote(src, dst, send, recv, who):
    return pltpu.make_async_remote_copy(src_ref=src, dst_ref=dst, send_sem=send, recv_sem=recv, device_id=who, device_id_type=MESH)


class Gather:
    def __init__(self, line, pos, shard, full, width, orders, paired, send, recv):
        self.line, self.pos, self.shard, self.full, self.width = line, pos, shard, full, width
        self.orders, self.paired, self.send, self.recv = orders, paired, send, recv
        self.count = shard.shape[-1] // width
        self.depth = line + 1 + paired

    def columns(self, t, sub):
        return t * self.width + sub[1], sub[2]

    def region(self, t, sub, have, z=None):
        first, part = self.columns(t, sub)
        pz, py, px, c = self.pos
        if self.paired:
            first = first + c * self.shard.shape[-1]
        every = slice(None)
        zi = z if z is not None else (every if "z" in have else pz)
        cols = pl.ds(pl.multiple_of(first, 128), part)
        return self.full.at[zi, every if "y" in have else py, every if "x" in have else px, :, cols]

    def own(self, t, sub):
        first, part = self.columns(t, sub)
        return self.shard.at[:, pl.ds(pl.multiple_of(first, 128), part)]

    def copy(self, t, sub, slot, src, dst, who):
        return remote(src, dst, self.send.at[t, sub[0], slot], self.recv.at[t, sub[0], slot], who)

    def hop(self, t, sub, h, up, have, what):
        z, y, x, c = self.pos
        slot = (h - 1) * 2 + up
        if up:
            block, incoming, who = z - (h - 1), z - h, dev(z + 1, y, x, c)
            there, here = (z + 1 < self.line) & (z >= h - 1), z >= h
        else:
            block, incoming, who = z + (h - 1), z + h, dev(z - 1, y, x, c)
            there, here = (z > 0) & (z + h - 1 < self.line), z + h < self.line

        @pl.when(here if what == "recv" else there)
        def _():
            if what == "recv":
                r = self.region(t, sub, have, incoming)
                self.copy(t, sub, slot, r, r, dev(z, y, x, 1 - c)).wait_recv()
                return
            r = self.region(t, sub, have, block)
            cp = self.copy(t, sub, slot, self.own(t, sub) if h == 1 and not have else r, r, who)
            cp.start() if what == "start" else cp.wait_send()

    def act(self, t, sub, order, i, what):
        z, y, x, c = self.pos
        moves, have = [], ""
        for axis in order:
            moves += [(axis, h, have) for h in (range(1, self.line) if axis == "z" else (0,))]
            have += axis
        if self.paired:
            moves.append(("c", 0, have))
        axis, h, have = moves[i]
        if axis == "z":
            for up in (1, 0):
                self.hop(t, sub, h, up, have, what)
            return
        who = {"y": dev(z, 1 - y, x, c), "x": dev(z, y, 1 - x, c), "c": dev(z, y, x, 1 - c)}[axis]
        land = self.region(t, sub, have)
        cp = self.copy(t, sub, 2 * (self.line - 1) + "yxc".index(axis), land if have else self.own(t, sub), land, who)
        {"start": cp.start, "recv": cp.wait_recv, "sent": cp.wait_send}[what]()

    def each(self, t, fn):
        there = (t >= 0) & (t < self.count)
        for v, orders in enumerate(self.orders):
            turn_of = there if len(self.orders) == 1 else there & ((lax.rem(t + 3, 3) == 0) == (v == 1))

            @pl.when(turn_of)
            def _():
                for sub, (order, first, columns) in enumerate(orders):
                    fn((sub, first, columns), order)

    def step(self, t, s):
        def go(sub, order):
            if s > 0:
                self.act(t, sub, order, s - 1, "recv")
            if s < self.depth:
                self.act(t, sub, order, s, "start")

        self.each(t, go)

    def advance(self, p):
        for s in range(self.depth + 1):
            self.step(p - s, s)

    def finish(self):
        @pl.loop(0, self.count)
        def _(t):
            self.each(t, lambda sub, order: [self.act(t, sub, order, i, "sent") for i in range(self.depth)])


def own_copy(g, sem):
    z, y, x, c = g.pos
    first = c * g.shard.shape[-1] if g.paired else 0
    return pltpu.make_async_copy(g.shard, g.full.at[z, y, x, :, pl.ds(pl.multiple_of(first, 128), g.shard.shape[-1])], sem)


def rope_tables(length, width):
    half_width = width // 2
    inverse = THETA_BASE ** (-(jnp.arange(half_width, dtype=jnp.float32) * 2.0 / width))
    angles = jnp.arange(length, dtype=jnp.float32)[:, None] * inverse[None, :]
    cosine, sine = jnp.cos(angles), jnp.sin(angles)
    return jnp.concatenate([cosine, cosine], axis=1), jnp.concatenate([-sine, sine], axis=1)


def turn(x, cosine, sine):
    half = x.shape[-1] // 2
    return x * cosine + jnp.concatenate([x[:, half:], x[:, :half]], axis=1) * sine


def dot_nt(a, b):
    return lax.dot_general(a, b, (((1,), (1,)), ((), ())), preferred_element_type=jnp.float32)


def dot_tn(a, b):
    return lax.dot_general(a, b, (((0,), (0,)), ((), ())), preferred_element_type=jnp.float32)


def dot_nn(a, b):
    return jnp.dot(a, b, preferred_element_type=jnp.float32)


BLOCK = 128


def causal_weights(q, k, b, heads):
    scores = dot_nt(q, k) * (1.0 / math.sqrt(HEAD_SIZE))
    n = scores.shape[1]
    row = lax.broadcasted_iota(jnp.int32, scores.shape, 0) % BLOCK + b * BLOCK
    keep = row >= lax.broadcasted_iota(jnp.int32, scores.shape, 1)
    scores = jnp.where(keep, scores, -jnp.inf)
    log_total = jnp.log(jnp.sum(jnp.exp(scores), axis=1, keepdims=True))
    return jnp.exp(scores - log_total)


def rows_of(ref, first, heads, rows):
    return jnp.concatenate([ref[first + i, rows] for i in range(heads)], axis=0)


ROWS = 128


def each_rows(tokens, step, fn):
    @pl.loop(0, tokens // step)
    def _(r):
        fn(pl.ds(pl.multiple_of(r * step, step), step))


def forward_kernel(line, width, block, *refs):
    refs = list(refs)
    take = lambda n: [refs.pop(0) for _ in range(n)]
    query_in, key_in, value_in, gate_in, up_in, out_in, down_in, gain_a, gain_b, hid, ct, cosine, sine = take(13)
    full, gains_full, q_out, k_out, v_out, mixed_out, n1_pair, n2_pair, ct_pair, mixed_pair, middle_out = take(11)
    tile_pairs = take(3)
    hidden_out, grad_n2, gain = take(3)
    wbuf, gain_buf, n1, n2, flat, qh, kh, vh, mh, mixed, middle, acc, act, tiles, shard, gains, turned = take(17)
    send, recv, gsend, grecv, own_sem, load_sem, gain_sem, local_sem, pair_send, pair_recv, tile_local, tile_send, tile_recv, shard_sem = take(14)

    pos = place()
    z, y, x, c = pos
    tokens, d_model = hid.shape
    half = shard.shape[-1]
    heads, groups = qh.shape[0] // 2, kh.shape[0] // 2
    sibling = dev(z, y, x, 1 - c)
    bf16, f32 = jnp.bfloat16, jnp.float32

    third, half_w = width // 3, width // 2
    mixes = (
        (("zyx", 0, third), ("zxy", third, third), ("xyz", 2 * third, third // 2), ("yxz", 2 * third + third // 2, third // 2)),
        (("zyx", 0, half_w), ("zxy", half_w, half_w)),
    )
    g = Gather(line, pos, shard, full, width, mixes, 1, send, recv)
    gg = Gather(line, pos, gains, gains_full, gains.shape[-1], ((("zyx", 0, gains.shape[-1]),),), 0, gsend, grecv)
    g_own, gg_own = own_copy(g, own_sem.at[0]), own_copy(gg, own_sem.at[1])
    steps = (half // width) - 3
    fills, at = [], 0
    for src in (query_in, key_in, value_in):
        fills.append((src, at, src.shape[1]))
        at += src.shape[1]
    fills.append((out_in, at, out_in.shape[1]))
    at += out_in.shape[1]
    for j in range(steps):
        for i, src in enumerate((gate_in, up_in, down_in)):
            fills.append((src.at[:, pl.ds(j * block, block)], at + j * width + i * block, block))
    fills = [pltpu.make_async_copy(src, shard.at[:, pl.ds(to, n)], shard_sem.at[i]) for i, (src, to, n) in enumerate(fills)]
    for cp in fills:
        cp.start()
    gains[...] = jnp.zeros_like(gains)
    top = lax.broadcasted_iota(jnp.int32, (gains.shape[0], gain_a.shape[1]), 0) == 0
    gains[:, : gain_a.shape[1]] = jnp.where(top, gain_a[...].astype(f32), gain_b[...].astype(f32)).astype(bf16)
    enter(line, pos)
    for cp in fills:
        cp.wait()
    g_own.start()
    gg_own.start()

    def load(t, hh, slot):
        cols = pl.ds(pl.multiple_of(hh * half + t * width, 128), width)
        return pltpu.make_async_copy(full.at[:, :, :, :, cols], wbuf.at[slot, hh], load_sem.at[slot, hh])

    def weight(slot, hh):
        return wbuf[slot, hh].reshape(d_model, width)

    def share(i, own_src, own_dst, other_src, other_dst):
        return pltpu.make_async_copy(own_src, own_dst, local_sem.at[i]), remote(other_src, other_dst, pair_send.at[i], pair_recv.at[i], sibling)

    ends = (pl.ds(0, tokens), pl.ds(tokens, tokens))
    lefts = ((ct, ct_pair), (n1, n1_pair), (n2, n2_pair))
    shares = [share(i, turned.at[i], pair.at[:, ends[0]], turned.at[i], pair.at[:, ends[1]]) for i, (_, pair) in enumerate(lefts)]
    hw = mixed.shape[1] // 2
    side = lambda ref, s, w: ref.at[:, pl.ds(pl.multiple_of(s * w, 128), w)]
    shares.append(share(3, side(mixed, c, hw), mixed_pair.at[0], side(mixed, 1 - c, hw), mixed_pair.at[1]))
    keeps = [pltpu.make_async_copy(src, dst, local_sem.at[4 + i]) for i, (src, dst) in enumerate(((qh, q_out), (kh, k_out), (vh, v_out), (mixed, mixed_out), (middle, middle_out)))]

    def begin(i):
        if i < len(lefts):
            span = 256

            @pl.loop(0, d_model // span)
            def _(e):
                at = pl.ds(pl.multiple_of(e * span, span), span)
                turned[i, at, :] = lefts[i][0][:, at].T

        for cp in shares[i]:
            cp.start()

    def end(i):
        for cp in shares[i]:
            cp.wait()

    def tile_copies(j, hh):
        slot = lax.rem(j, 2)
        cols = pl.ds(pl.multiple_of(j * block, 128), block)
        own = [pltpu.make_async_copy(tiles.at[slot, hh, i], pair.at[0, :, cols], tile_local.at[j, i]) for i, pair in enumerate(tile_pairs)]
        out = [remote(tiles.at[slot, hh, i], pair.at[1, :, cols], tile_send.at[j, i], tile_recv.at[j, i], sibling) for i, pair in enumerate(tile_pairs)]
        return own, out

    def drain_tiles(j):
        for cp in tile_copies(j, 0)[0]:
            cp.wait()
        for cp in tile_copies(j, 0)[1]:
            cp.wait_send()

    def normalize():
        loaded = pltpu.make_async_copy(gains_full, gain_buf, gain_sem)
        loaded.start()
        loaded.wait()
        n = d_model // (gain_buf.shape[0] * 4)
        table = gain_buf[...].astype(f32)
        for i in range(2):
            gain[i : i + 1, :] = jnp.concatenate([table[a, b, e, i : i + 1, :n] for a in range(gain_buf.shape[0]) for b in range(2) for e in range(2)], axis=1)

        def rows_of_norm(rows):
            v = hid[rows, :].astype(f32)
            v = v * lax.rsqrt(jnp.mean(v * v, axis=1, keepdims=True) + EPSILON)
            n1[rows, :] = (v * gain[0:1, :]).astype(bf16)

        each_rows(tokens, ROWS, rows_of_norm)
        begin(1)

    def project(slot, outs):
        @pl.loop(0, 2)
        def _(hh):
            flat[...] = dot_nn(n1[...], weight(slot, hh))

            def to_heads(rows):
                cos, sin = cosine[rows, :], sine[rows, :]
                first = 0
                for n, target, turned in outs:
                    for h in range(n):
                        v = flat[rows, (first + h) * HEAD_SIZE : (first + h + 1) * HEAD_SIZE]
                        target[hh * n + h, rows] = (turn(v, cos, sin) if turned else v).astype(bf16)
                    first += n

            each_rows(tokens, ROWS, to_heads)

    def attend_half(hh):
        per = heads // groups
        blocks = tokens // BLOCK

        @pl.loop(0, groups)
        def _(i):
            kv = hh * groups + i
            for b in range(blocks):
                rows, n = pl.ds(b * BLOCK, BLOCK), (b + 1) * BLOCK
                w = causal_weights(rows_of(qh, kv * per, per, rows), kh[kv, :n], b, per).astype(bf16)
                m = dot_nn(w, vh[kv, :n]).astype(bf16)
                for e in range(per):
                    mh[kv * per + e, rows] = m[e * BLOCK : (e + 1) * BLOCK]

    def leave_attention(slot):
        def join(rows):
            mixed[rows, :] = jnp.concatenate([mh[h, rows] for h in range(2 * heads)], axis=1)

        each_rows(tokens, ROWS, join)
        begin(3)
        for cp in keeps[:4]:
            cp.start()
        middle[...] = hid[...].astype(f32) + dot_nt(mixed[:, :hw], weight(slot, 0))
        middle[...] += dot_nt(mixed[:, hw:], weight(slot, 1))

        def rows_of_norm(rows):
            v = middle[rows, :]
            acc[rows, :] = v
            v = v * lax.rsqrt(jnp.mean(v * v, axis=1, keepdims=True) + EPSILON)
            n2[rows, :] = (v * gain[1:2, :]).astype(bf16)
            grad_n2[rows, :] = jnp.zeros_like(v)

        keeps[4].start()
        each_rows(tokens, ROWS, rows_of_norm)
        begin(2)

    def feed_forward(j, slot):
        @pl.when(j >= 2)
        def _():
            drain_tiles(j - 2)

        part = lax.rem(j, 2)

        @pl.loop(0, 2)
        def _(hh):
            act[0] = dot_nn(n2[...], weight(slot, hh)[:, :block])
            act[1] = dot_nn(n2[...], weight(slot, hh)[:, block : 2 * block])
            act[2] = dot_nn(ct[...], weight(slot, hh)[:, 2 * block :])

            def gated(rows):
                gate, up, grad = act[0, rows], act[1, rows], act[2, rows]
                sigma = jax.nn.sigmoid(gate)
                tiles[part, hh, 0, rows] = (gate * sigma * up).astype(bf16)
                tiles[part, hh, 1, rows] = (grad * up * sigma * (1.0 + gate * (1.0 - sigma))).astype(bf16)
                tiles[part, hh, 2, rows] = (grad * gate * sigma).astype(bf16)

            each_rows(tokens, ROWS // 2, gated)
            own, out = tile_copies(j, hh)

            @pl.when(hh == c)
            def _():
                for cp in own:
                    cp.start()

            @pl.when(hh != c)
            def _():
                for cp in out:
                    cp.start()

            acc[...] += dot_nt(tiles[part, hh, 0], weight(slot, hh)[:, 2 * block :])
            both = jnp.concatenate([tiles[part, hh, 1], tiles[part, hh, 2]], axis=1)
            grad_n2[...] += dot_nt(both, weight(slot, hh)[:, : 2 * block])

    count, lead = g.count, g.depth + 1

    @pl.loop(0, count + lead)
    def _(p):
        @pl.when(p == 0)
        def _():
            g_own.wait()
            gg_own.wait()
            begin(0)

        gg.advance(p)
        g.advance(p)
        u = p - lead

        @pl.when((u >= -1) & (u + 1 < count))
        def _():
            for hh in range(2):
                load(u + 1, hh, lax.rem(u + 1, 2)).start()

        @pl.when(u >= 0)
        def _():
            slot = lax.rem(u, 2)
            for hh in range(2):
                load(u, hh, slot).wait()

            @pl.when(u == 0)
            def _():
                normalize()
                project(slot, ((heads, qh, True),))

            @pl.when(u == 1)
            def _():
                project(slot, ((groups, kh, True), (groups, vh, False)))
                attend_half(0)

            @pl.when(u == 2)
            def _():
                attend_half(1)
                leave_attention(slot)

            @pl.when(u >= 3)
            def _():
                feed_forward(u - 3, slot)

    def rows_out(rows):
        hidden_out[rows, :] = acc[rows, :].astype(bf16)

    each_rows(tokens, ROWS, rows_out)
    for i in range(len(shares)):
        end(i)
    for cp in keeps:
        cp.wait()
    for j in range(max(steps - 2, 0), steps):
        drain_tiles(j)

    @pl.loop(0, steps)
    def _(j):
        for cp in tile_copies(j, 0)[1]:
            cp.wait_recv()

    g.finish()
    gg.finish()


def forward(line, shards, gain_pair, hidden_in, cotangent, cosine, sine, block):
    tokens, d_model = hidden_in.shape
    rows = gain_pair[0].shape[1]
    half = sum(s.shape[1] for s in shards)
    gains = jax.ShapeDtypeStruct((8, 128), jnp.bfloat16)
    width = 3 * block
    count = half // width
    steps = count - 3
    heads, groups = QUERY_HEADS // 2, KEY_VALUE_HEADS // 2
    bf16, f32 = jnp.bfloat16, jnp.float32
    struct = jax.ShapeDtypeStruct
    hbm, vmem = pl.BlockSpec(memory_space=pl.ANY), pl.BlockSpec(memory_space=pltpu.VMEM)
    dma = pltpu.SemaphoreType.DMA
    pair = struct((d_model, 2 * tokens), bf16)
    tile_pair = struct((2, tokens, steps * block), bf16)
    head_shape = lambda n: (n, tokens, HEAD_SIZE)
    slots = 2 * (line - 1) + 3
    outs = [
        struct((line, 2, 2, rows, 2 * half), bf16),
        struct((line, 2, 2) + gains.shape, bf16),
        struct(head_shape(2 * heads), bf16),
        struct(head_shape(2 * groups), bf16),
        struct(head_shape(2 * groups), bf16),
        struct((tokens, 2 * heads * HEAD_SIZE), bf16),
        pair,
        pair,
        pair,
        struct((2, tokens, heads * HEAD_SIZE), bf16),
        struct((tokens, d_model), f32),
        tile_pair,
        tile_pair,
        tile_pair,
        struct((tokens, d_model), bf16),
        struct((tokens, d_model), f32),
        struct((8, d_model), f32),
    ]
    V = pltpu.VMEM
    return pl.pallas_call(
        functools.partial(forward_kernel, line, width, block),
        out_shape=outs,
        in_specs=[hbm] * 7 + [vmem] * 6,
        out_specs=[hbm] * 14 + [vmem] * 3,
        scratch_shapes=[
            V((2, 2, line, 2, 2, rows, width), bf16),
            V((line, 2, 2) + gains.shape, bf16),
            V((tokens, d_model), bf16),
            V((tokens, d_model), bf16),
            V((tokens, width), f32),
            V(head_shape(2 * heads), bf16),
            V(head_shape(2 * groups), bf16),
            V(head_shape(2 * groups), bf16),
            V(head_shape(2 * heads), bf16),
            V((tokens, 2 * heads * HEAD_SIZE), bf16),
            V((tokens, d_model), f32),
            V((tokens, d_model), f32),
            V((3, tokens, block), f32),
            V((2, 2, 3, tokens, block), bf16),
            V((rows, half), bf16),
            V(gains.shape, bf16),
            V((3, d_model, tokens), bf16),
            dma((count, 4, slots)),
            dma((count, 4, slots)),
            dma((1, 1, slots)),
            dma((1, 1, slots)),
            dma((2,)),
            dma((2, 2)),
            dma,
            dma((9,)),
            dma((4,)),
            dma((4,)),
            dma((steps, 3)),
            dma((steps, 3)),
            dma((steps, 3)),
            dma((4 + 3 * steps,)),
        ],
        compiler_params=pltpu.CompilerParams(collective_id=0, has_side_effects=True, vmem_limit_bytes=64 * 2**20 - 2**17),
        name="gather_forward",
    )(*shards, *gain_pair, hidden_in, cotangent, cosine, sine)


class Scatter:
    def __init__(self, line, pos, count, plain, early, final):
        self.line, self.pos, self.count, self.final = line, pos, count, final
        self.own, self.first, self.second, self.up, self.down, self.send, self.recv = plain
        self.early = early
        self.lags = [0, 2, 4, 5, 4 + line, 5 + line]
        self.depth = self.lags[-1]

    def is_early(self, t):
        return lax.rem(t + 5, 5) == 4

    def plain_number(self, t):
        return t - lax.div(t, 5)

    def parts(self, t, early):
        if early:
            i, (own, first, second, up, down, send, recv) = lax.div(t, 5), self.early
        else:
            i, own, first, second, up, down, send, recv = self.plain_number(t), self.own, self.first, self.second, self.up, self.down, self.send, self.recv
        o, r = lax.rem(i, own.shape[0]), lax.rem(i, first.shape[0])
        return own.at[o], first.at[r], second.at[r], up.at[r], down.at[r], send.at[r], recv.at[r]

    def place_of(self, t, early):
        return self.parts(t, early)[0]

    def merge(self, dst, a, b, loops):
        def go(lead, rest):
            if not rest:
                dst[lead] = a[lead] + b[lead]
            elif rest[0] > 2:
                @pl.loop(0, rest[0])
                def _(i):
                    go(lead + (i,), rest[1:])
            else:
                for i in range(rest[0]):
                    go(lead + (i,), rest[1:])

        go((), loops)

    def pair_moves(self, t, v):
        z, y, x, c = self.pos
        early = v >= 2
        own, first, second, _, _, send, recv = self.parts(t, early)
        over_x, over_y = dev(z, y, 1 - x, c), dev(z, 1 - y, x, c)
        lead = (z,) if early else (slice(None),)
        if v % 2 == 0:
            give, keep, who = own.at[lead + (slice(None), 1 - x)], own.at[lead + (slice(None), x)], (over_x, over_y)
        else:
            give, keep, who = own.at[lead + (1 - y,)], own.at[lead + (y,)], (over_y, over_x)
        a, b = (1 - y, y) if v % 2 == 0 else (1 - x, x)
        lead = () if early else (slice(None),)
        one = remote(give, first, send.at[0], recv.at[0], who[0])
        two = remote(first.at[lead + (a,)], second, send.at[1], recv.at[1], who[1])
        return one, two, keep, first, second, first.at[lead + (b,)]

    def hop(self, p, j, way, early):
        z, y, x, c = self.pos
        last = self.line - 1
        travelled = z if way == 0 else last - z
        t = p - (0 if early else self.lags[3]) - j - travelled
        target = last - j if way == 0 else j
        passes = (target > z) if way == 0 else (target < z)

        def go():
            own, _, second, up, down, send, recv = self.parts(t, early)
            cur, ref = own if early else second, (up if way == 0 else down).at[j]
            nxt = dev(z + 1, y, x, c) if way == 0 else dev(z - 1, y, x, c)
            slot = 2 + 2 * j + way

            @pl.when(travelled == 0)
            def _():
                remote(cur.at[target], ref, send.at[slot], recv.at[slot], nxt).start()

            @pl.when(travelled > 0)
            def _():
                cp = remote(ref, ref, send.at[slot], recv.at[slot], nxt)
                cp.wait_recv()
                self.merge(ref, ref, cur.at[target], (2, 2) if early else ())
                cp.start()

        @pl.when(passes & (t >= 0) & (t < self.count) & (self.is_early(t) == early))
        def _():
            go()

    def arrive(self, t, early):
        z, y, x, c = self.pos
        _, _, _, up, down, send, recv = self.parts(t, early)
        last = self.line - 1
        ends = []
        for way, ref, has, k in ((0, up, z > 0, last - z), (1, down, z < last, z)):

            @pl.when(has)
            def _():
                slot = 2 + 2 * k + way
                remote(ref.at[k], ref.at[k], send.at[slot], recv.at[slot], dev(z, y, x, 1 - c)).wait_recv()

            ends.append((has, ref.at[jnp.minimum(k, last - 1)]))
        return ends

    def close(self, t):
        f32 = jnp.float32
        total = self.parts(t, False)[2][self.pos[0]].astype(f32)
        for has, ref in self.arrive(t, False):
            total = total + jnp.where(has, ref[...].astype(f32), 0.0)
        self.final(t, total)

    def close_early(self, t, v):
        z = self.pos[0]
        mine = self.place_of(t, True).at[z]
        ends = self.arrive(t, True)
        for i in range(2):
            for k in range(2):
                total = mine[i, k].astype(jnp.float32)
                for has, ref in ends:
                    total = total + jnp.where(has, ref[i, k].astype(jnp.float32), 0.0)
                mine[i, k] = total.astype(mine.dtype)
        self.pair_moves(t, v)[0].start()

    def drain(self, t, early):
        z, y, x, c = self.pos
        _, _, _, up, down, send, recv = self.parts(t, early)
        if early:
            self.pair_moves(t, 2)[0].wait_send()
        self.pair_moves(t, 2 * early)[1].wait_send()
        for j in range(self.line - 1):
            for way, ref, target in ((0, up, self.line - 1 - j), (1, down, j)):

                @pl.when((target > z) if way == 0 else (target < z))
                def _():
                    slot = 2 + 2 * j + way
                    remote(ref.at[j], ref.at[j], send.at[slot], recv.at[slot], dev(z, y, x, 1 - c)).wait_send()

    def plain(self, t, fn):
        @pl.when((t >= 0) & (t < self.count) & ~self.is_early(t))
        def _():
            fn()

    def sorts(self, t, fn, early):
        number = lax.div(t, 5) if early else self.plain_number(t)
        for v in range(2):
            @pl.when((t >= 0) & (t < self.count) & (self.is_early(t) == early) & (lax.rem(number + 2, 2) == v))
            def _():
                fn(v + 2 * early)

    def begin(self, t):
        self.sorts(t, lambda v: self.pair_moves(t, v)[0].start(), False)

    def release(self, p):
        t = p - self.own.shape[0] * 5 // 4
        self.plain(t, lambda: self.pair_moves(t, 0)[0].wait_send())

    def advance(self, p):
        line = self.line

        def one(t, v):
            first_copy, second_copy, keep, first, second, _ = self.pair_moves(t, v)
            first_copy.wait_recv()
            self.merge(first, first, keep, (2,) if v >= 2 else (line, 2))
            second_copy.start()

        def two(t, v):
            _, second_copy, _, _, second, keep = self.pair_moves(t, v)
            second_copy.wait_recv()
            if v >= 2:
                self.final(t, keep[...].astype(jnp.float32) + second[...].astype(jnp.float32))
            else:
                self.merge(second, second, keep, (line,))

        for j in range(line - 1):
            for way in range(2):
                self.hop(p, j, way, True)
        for step, lag, early in ((one, self.lags[1], False), (two, self.lags[2], False), (self.close_early, line, True), (one, line + 2, True), (two, line + 4, True)):
            t = p - lag
            self.sorts(t, lambda v, t=t, step=step: step(t, v), early)
        for j in range(line - 1):
            for way in range(2):
                self.hop(p, j, way, False)
        t = p - self.lags[-2]
        self.plain(t, lambda t=t: self.close(t))
        t = p - self.lags[-1]
        self.plain(t, lambda t=t: self.drain(t, False))

        @pl.when((t >= 0) & (t < self.count) & self.is_early(t))
        def _():
            self.drain(t, True)


def greet_all(n, pos):
    z, y, x, c = pos
    d = z * 4 + y * 2 + x
    barrier = pltpu.get_barrier_semaphore()

    @pl.loop(1, n)
    def _(i):
        pl.semaphore_signal(barrier, inc=1, device_id=(lax.rem(d + i, n), c), device_id_type=MESH)

    pl.semaphore_signal(barrier, inc=1, device_id=(d, 1 - c), device_id_type=MESH)
    pl.semaphore_wait(barrier, n)


def backward_kernel(line, cols, starts, *refs):
    refs = list(refs)
    take = lambda n: [refs.pop(0) for _ in range(n)]
    q, k, v, mixed, full, hid, ct, middle, grad_n2, gains, cosine, sine = take(12)
    n1_pair, n2_pair, ct_pair, mixed_pair, hidden_pair, gate_pair, up_pair = take(7)
    qkv_pair, grad_query, grad_key, grad_value, grad_in, out_out, out_gate, out_up, out_down, out_gains, gm_pair = take(11)
    own, first, second, up, down, xt, ybuf, qh, kh, vh, mh, gh, gm, dots, dq, dk, dv, dqkv, wbuf, gmid, hbuf, out_qkv, gain_one, part, parts_in, pair_in, gain_two, gmb, turned, own_e, first_e, second_e, up_e, down_e = take(34)
    send, recv, xsem, ysem, half_sem, wsem, msem, qkv_local, qkv_send, qkv_recv, part_send, part_recv, out_sem, swap_sem, gm_sem, send_e, recv_e = take(17)

    pos = place()
    z, y, x, c = pos
    d = z * 4 + y * 2 + x
    n = line * 4
    tokens, d_model = hid.shape
    count = starts[-1]
    heads, groups = qh.shape[0], kh.shape[0]
    share = heads // groups
    blocks = tokens // BLOCK
    width = wbuf.shape[-1]
    half_width = dqkv.shape[1] // 2
    scale = 1.0 / math.sqrt(HEAD_SIZE)
    bf16, f32 = jnp.bfloat16, jnp.float32
    sources = (hidden_pair, gate_pair, up_pair, mixed_pair, qkv_pair)
    lefts = ((0, ct_pair), (starts[1], n2_pair), (starts[3], gm_pair), (starts[4], n1_pair))

    def final(t, total):
        for i, out in enumerate((out_down, out_gate, out_up, out_out, out_qkv)):
            at = pl.ds(pl.multiple_of((t - starts[i]) * cols, 128), cols)

            @pl.when((t >= starts[i]) & (t < starts[i + 1]))
            def _():
                out[:, at] = total

    s = Scatter(line, pos, count, (own, first, second, up, down, send, recv), (own_e, first_e, second_e, up_e, down_e, send_e, recv_e), final)

    def load_left(i):
        return pltpu.make_async_copy(lefts[i][1], xt.at[i % 2], xsem.at[i % 2])

    def load_right(t, act):
        slot = lax.rem(t, 2)
        for i, src in enumerate(sources):
            at = pl.ds(pl.multiple_of((t - starts[i]) * cols, 128), cols)

            @pl.when((t >= starts[i]) & (t < starts[i + 1]))
            def _():
                cp = pltpu.make_async_copy(src.at[:, :, at], ybuf.at[slot], ysem.at[slot])
                cp.start() if act == "start" else cp.wait()

    def half_loads(hh):
        take_heads = lambda ref, m: ref.at[pl.ds(hh * m, m)]
        lanes = pl.ds(pl.multiple_of(hh * mh.shape[1], 128), mh.shape[1])
        pairs = ((take_heads(q, heads), qh), (take_heads(k, groups), kh), (take_heads(v, groups), vh), (mixed.at[:, lanes], mh))
        return [pltpu.make_async_copy(src, dst, half_sem.at[i]) for i, (src, dst) in enumerate(pairs)]

    def half_load(hh, act):
        for cp in half_loads(hh):
            cp.start() if act == "start" else cp.wait()

    each = half_width // width
    half_columns = full.shape[-1] // 2

    def weights(i):
        at = (i * half_columns + each * width) if i < 2 else ((i - 2) // each * half_columns + (i - 2) % each * width)
        return pltpu.make_async_copy(full.at[:, :, :, :, pl.ds(at, width)], wbuf.at[i % 2], wsem.at[i % 2])

    def weight(i):
        return wbuf[i % 2].reshape(d_model, width)

    middle_in = pltpu.make_async_copy(middle, grad_in, msem.at[0])
    grad_n2_in = pltpu.make_async_copy(grad_n2, gmid, msem.at[1])
    ct_in, hid_in = (pltpu.make_async_copy(src, hbuf, msem.at[2]) for src in (ct, hid))

    own_half = lambda ref, which: ref.at[:, pl.ds(pl.multiple_of(which * half_width, 128), half_width)]

    def qkv_copies():
        return (
            pltpu.make_async_copy(own_half(dqkv, c), qkv_pair.at[0], qkv_local),
            remote(own_half(dqkv, 1 - c), qkv_pair.at[1], qkv_send, qkv_recv, (d, 1 - c)),
        )

    def gm_copies():
        return (
            pltpu.make_async_copy(turned, gm_pair.at[:, pl.ds(0, tokens)], gm_sem.at[0]),
            remote(turned, gm_pair.at[:, pl.ds(tokens, tokens)], gm_sem.at[1], gm_sem.at[2], (d, 1 - c)),
        )

    def norm_two_back():
        for cp in (middle_in, grad_n2_in, ct_in):
            cp.wait()
        gain_two[...] = jnp.zeros_like(gain_two)

        def rows_back(rows):
            a, grad = grad_in[rows, :], gmid[rows, :]
            inverse = lax.rsqrt(jnp.mean(a * a, axis=1, keepdims=True) + EPSILON)
            unit = a * inverse
            scaled = grad * gains[1:2, :]
            inner = jnp.mean(scaled * unit, axis=1, keepdims=True)
            total = hbuf[rows, :].astype(f32) + inverse * (scaled - unit * inner)
            gmid[rows, :] = total
            gmb[rows, :] = total.astype(bf16)
            gain_two[...] += jnp.sum(grad * unit, axis=0, keepdims=True)

        each_rows(tokens, ROWS, rows_back)
        hid_in.start()
        span = 256

        @pl.loop(0, d_model // span)
        def _(e):
            at = pl.ds(pl.multiple_of(e * span, span), span)
            turned[at, :] = gmb[:, at].T

        for cp in gm_copies():
            cp.start()

    def through_out(i):
        weights(i).wait()
        gh[...] = dot_nn(gmb[...], weight(i))
        weights(i + 2).start()

    def prepare(hh):
        half_load(hh, "wait")

        def rows_of_dots(rows):
            for h in range(heads):
                lanes = slice(h * HEAD_SIZE, (h + 1) * HEAD_SIZE)
                g = gh[rows, lanes]
                dots[h, rows] = jnp.sum(g * mh[rows, lanes].astype(f32), axis=1, keepdims=True)
                gm[h, rows] = g.astype(bf16)

        each_rows(tokens, ROWS, rows_of_dots)
        dk[...] = jnp.zeros_like(dk)
        dv[...] = jnp.zeros_like(dv)

    def group_back(g, which):
        for b in which:
            rows, m = pl.ds(b * BLOCK, BLOCK), (b + 1) * BLOCK
            qb, gb, db = (rows_of(ref, g * share, share, rows) for ref in (qh, gm, dots))
            kb, vb = kh[g, :m], vh[g, :m]
            p = causal_weights(qb, kb, b, share)
            ds = (p * (dot_nt(gb, vb) - db)).astype(bf16)
            dv[g, :m] += dot_tn(p.astype(bf16), gb)
            dk[g, :m] += dot_tn(ds, qb)
            r = dot_nn(ds, kb) * scale
            for i in range(share):
                dq[g * share + i, rows] = r[i * BLOCK : (i + 1) * BLOCK]

    def join(hh):
        def rows_of_join(rows):
            cos, sin = cosine[rows, :], -sine[rows, :]
            parts = [turn(dq[h, rows], cos, sin) for h in range(heads)]
            parts += [turn(dk[g, rows] * scale, cos, sin) for g in range(groups)]
            parts += [dv[g, rows] for g in range(groups)]
            dqkv[rows, pl.ds(pl.multiple_of(hh * half_width, 128), half_width)] = jnp.concatenate([a.astype(bf16) for a in parts], axis=1)

        each_rows(tokens, ROWS, rows_of_join)

    def against(i):
        weights(i + 2).wait()
        r = dot_nt(dqkv[:, i * width : (i + 1) * width], weight(i))
        if i == 0:
            grad_in[...] = r
        else:
            grad_in[...] += r
        if i + 2 < 2 * each:
            weights(i + 4).start()

    def norm_one_back():
        hid_in.wait()
        gain_one[...] = jnp.zeros_like(gain_one)

        def rows_back(rows):
            a = hbuf[rows, :].astype(f32)
            inverse = lax.rsqrt(jnp.mean(a * a, axis=1, keepdims=True) + EPSILON)
            unit, grad = a * inverse, grad_in[rows, :]
            scaled = grad * gains[0:1, :]
            inner = jnp.mean(scaled * unit, axis=1, keepdims=True)
            grad_in[rows, :] = gmid[rows, :] + inverse * (scaled - unit * inner)
            gain_one[...] += jnp.sum(grad * unit, axis=0, keepdims=True)

        each_rows(tokens, ROWS, rows_back)
        size = d_model // n
        part[...] = jnp.zeros_like(part)
        for i in range(n):
            for row, ref in enumerate((gain_one, gain_two)):
                part[i, row : row + 1, :size] = ref[:, i * size : (i + 1) * size]

    def part_copy(i):
        to = lax.rem(d + i, n)
        return remote(part.at[to], parts_in.at[i], part_send.at[i], part_recv.at[i], (to, c))

    load_left(0).start()
    load_left(1).start()
    load_right(0, "start")
    half_load(0, "start")
    for cp in (middle_in, grad_n2_in, ct_in):
        cp.start()
    for i in range(2):
        weights(i).start()
    greet_all(n, pos)

    stages = 2 * groups + 3
    turns = 1 + 2 * stages
    norm_at = turns + 2 * each

    @pl.loop(0, count + s.depth)
    def _(p):
        s.release(p)
        for i, (at, _) in enumerate(lefts):

            @pl.when(p == at)
            def _():
                load_left(i).wait()
                if 1 <= i < len(lefts) - 1:
                    load_left(i + 1).start()

        @pl.when(p == starts[1] - 1)
        def _():
            for cp in gm_copies():
                cp.wait()

        @pl.when(p == starts[4] - 2)
        def _():
            for cp in qkv_copies():
                cp.wait()

        @pl.when(p < count)
        def _():
            load_right(p, "wait")

            @pl.when(p + 1 < count)
            def _():
                load_right(p + 1, "start")

            side = lax.rem(sum((p >= at).astype(jnp.int32) for at, _ in lefts[1:]), 2)
            right = ybuf[lax.rem(p, 2)].reshape(2 * tokens, cols)
            for early in (False, True):

                @pl.when(s.is_early(p) == early)
                def _():
                    s.place_of(p, early)[...] = dot_nn(xt[side], right).reshape(own.shape[1:]).astype(bf16)

            s.begin(p)

        s.advance(p)

        @pl.when(p == 0)
        def _():
            norm_two_back()

        for i in range(2):

            @pl.when(p == 1 + i * stages)
            def _():
                through_out(i)

        @pl.when((p > 0) & (p < turns))
        def _():
            hh, r = lax.div(p - 1, stages), lax.rem(p - 1, stages) - 1

            @pl.when(r == 0)
            def _():
                prepare(hh)

            for e, which in enumerate((range(blocks - 1), range(blocks - 1, blocks))):

                @pl.when((r > 0) & (r <= 2 * groups) & (lax.rem(r + 1, 2) == e))
                def _():
                    group_back(lax.div(r - 1, 2), which)

            @pl.when(r == stages - 2)
            def _():
                join(hh)

                @pl.when(hh == 0)
                def _():
                    half_load(1, "start")

                @pl.when(hh == 1)
                def _():
                    for cp in qkv_copies():
                        cp.start()

        for i in range(2 * each):

            @pl.when(p == turns + i)
            def _():
                against(i)

        @pl.when(p == norm_at)
        def _():
            norm_one_back()

        @pl.when(p == norm_at + 1)
        def _():
            @pl.loop(1, n)
            def _(i):
                part_copy(i).start()

    total = part[d]

    @pl.loop(1, n)
    def _(i):
        part_copy(i).wait()

    total = total + jnp.sum(parts_in[1:], axis=0)
    out_gains[...] = total
    swap = remote(out_gains, pair_in, swap_sem.at[0], swap_sem.at[1], (d, 1 - c))
    swap.start()
    first_column = 0
    for i, out in enumerate((grad_query, grad_key, grad_value)):
        cp = pltpu.make_async_copy(out_qkv.at[:, pl.ds(first_column, out.shape[1])], out, out_sem.at[i])
        cp.start()
        cp.wait()
        first_column += out.shape[1]
    swap.wait()
    out_gains[...] += pair_in[...]


def backward(line, cols, arrays, halves):
    q, k, v, mixed, full, hid = arrays[:6]
    tokens, d_model = hid.shape
    rows = full.shape[3]
    n = line * 4
    down_w, gate_w, up_w, out_w, q_w, k_w, v_w = halves
    qkv_w = q_w + k_w + v_w
    starts = [0]
    for w in (down_w, gate_w, up_w, out_w, qkv_w):
        starts.append(starts[-1] + w // cols)
    heads, groups = q.shape[0] // 2, k.shape[0] // 2
    width = q_w
    bf16, f32 = jnp.bfloat16, jnp.float32
    struct, V, dma = jax.ShapeDtypeStruct, pltpu.VMEM, pltpu.SemaphoreType.DMA
    hbm, vmem = pl.BlockSpec(memory_space=pl.ANY), pl.BlockSpec(memory_space=pltpu.VMEM)
    ring, own_ring = (line + 12) * 4 // 5 + 1, 4
    ring_e, own_ring_e = (line + 16) // 5, (line + 5) // 5 + 1
    head = lambda m: (m, tokens, HEAD_SIZE)
    sems = 2 + 2 * (line - 1)
    outs = [struct((2, tokens, qkv_w), bf16)]
    outs += [struct((rows, w), f32) for w in (q_w, k_w, v_w)]
    outs += [struct((tokens, d_model), f32), struct((rows, out_w), f32), struct((rows, gate_w), f32), struct((rows, up_w), f32), struct((rows, down_w), f32), struct((8, 128), f32)]
    outs += [struct((d_model, 2 * tokens), bf16)]
    return pl.pallas_call(
        functools.partial(backward_kernel, line, cols, tuple(starts)),
        out_shape=outs,
        in_specs=[hbm] * 9 + [vmem] * 3 + [hbm] * 7,
        out_specs=[hbm] * 4 + [vmem] * 6 + [hbm],
        scratch_shapes=[
            V((own_ring, line, 2, 2, rows, cols), bf16),
            V((ring, line, 2, rows, cols), bf16),
            V((ring, line, rows, cols), bf16),
            V((ring, line - 1, rows, cols), bf16),
            V((ring, line - 1, rows, cols), bf16),
            V((2, d_model, 2 * tokens), bf16),
            V((2, 2, tokens, cols), bf16),
            V(head(heads), bf16),
            V(head(groups), bf16),
            V(head(groups), bf16),
            V((tokens, heads * HEAD_SIZE), bf16),
            V((tokens, heads * HEAD_SIZE), f32),
            V(head(heads), bf16),
            V((heads, tokens, 1), f32),
            V(head(heads), f32),
            V(head(groups), f32),
            V(head(groups), f32),
            V((tokens, 2 * qkv_w), bf16),
            V((2, line, 2, 2, rows, width), bf16),
            V((tokens, d_model), f32),
            V((tokens, d_model), bf16),
            V((rows, qkv_w), f32),
            V((1, d_model), f32),
            V((n, 8, 128), f32),
            V((n, 8, 128), f32),
            V((8, 128), f32),
            V((1, d_model), f32),
            V((tokens, d_model), bf16),
            V((d_model, tokens), bf16),
            V((own_ring_e, line, 2, 2, rows, cols), bf16),
            V((ring_e, 2, rows, cols), bf16),
            V((ring_e, rows, cols), bf16),
            V((ring_e, line - 1, 2, 2, rows, cols), bf16),
            V((ring_e, line - 1, 2, 2, rows, cols), bf16),
            dma((ring, sems)),
            dma((ring, sems)),
            dma((2,)),
            dma((2,)),
            dma((4,)),
            dma((2,)),
            dma((3,)),
            dma,
            dma,
            dma,
            dma((n,)),
            dma((n,)),
            dma((3,)),
            dma((2,)),
            dma((3,)),
            dma((ring_e, sems)),
            dma((ring_e, sems)),
        ],
        compiler_params=pltpu.CompilerParams(collective_id=1, has_side_effects=True, vmem_limit_bytes=64 * 2**20 - 2**17),
        name="backward_scatter",
    )(*arrays)


def finish_kernel(n, *refs):
    srcs, outs, bufs, (loads, stores) = refs[:n], refs[n : 2 * n], refs[2 * n : 3 * n], refs[3 * n :]
    for i in range(n):
        pltpu.make_async_copy(srcs[i], bufs[i], loads.at[i]).start()
    for i in range(n):
        pltpu.make_async_copy(srcs[i], bufs[i], loads.at[i]).wait()
        pltpu.make_async_copy(bufs[i], outs[i], stores.at[i]).start()
    for i in range(n):
        pltpu.make_async_copy(bufs[i], outs[i], stores.at[i]).wait()


def finish(arrays):
    n = len(arrays)
    hbm = pl.BlockSpec(memory_space=pl.ANY)
    return pl.pallas_call(
        functools.partial(finish_kernel, n),
        out_shape=[jax.ShapeDtypeStruct(a.shape, a.dtype) for a in arrays],
        in_specs=[hbm] * n,
        out_specs=[hbm] * n,
        scratch_shapes=[pltpu.VMEM(a.shape, a.dtype) for a in arrays] + [pltpu.SemaphoreType.DMA((n,)), pltpu.SemaphoreType.DMA((n,))],
        compiler_params=pltpu.CompilerParams(vmem_limit_bytes=64 * 2**20 - 2**17),
        name="finish",
    )(*arrays)


def layer(n_dp, n_tensor, hidden_in, query_weight, key_matrix, value_matrix, out_weight, gate_weight, up_weight, down_weight, attention_gain, feedforward_gain, cotangent):
    line = n_dp // 4
    rows = attention_gain.shape[0]
    block = (query_weight.shape[1] // 3) & -128
    cosine, sine = rope_tables(SEQUENCE_LENGTH, HEAD_SIZE)
    (full, _, q, k, v, mixed, n1, n2, ct, mixed_pair, middle, hidden, gate, up, hidden_out, grad_n2, gain_rows) = forward(
        line,
        (query_weight, key_matrix, value_matrix, gate_weight, up_weight, out_weight.T, down_weight.T),
        (attention_gain.reshape(1, rows), feedforward_gain.reshape(1, rows)),
        hidden_in,
        cotangent,
        cosine,
        sine,
        block,
    )
    arrays = (q, k, v, mixed, full, hidden_in, cotangent, middle, grad_n2, gain_rows, cosine, sine, n1, n2, ct, mixed_pair, hidden, gate, up)
    halves = (down_weight.shape[0], gate_weight.shape[1], up_weight.shape[1], out_weight.shape[0], query_weight.shape[1], key_matrix.shape[1], value_matrix.shape[1])
    results = backward(line, 256 if line <= 4 else 128, arrays, halves)
    g_query, g_key, g_value, grad_in, g_out, g_gate, g_up, g_down, hidden_out = finish(list(results[1:9]) + [hidden_out])
    g_gains = results[9]
    return hidden_out, grad_in, g_query, g_key, g_value, g_out.T, g_gate, g_up, g_down.T, g_gains[0, :rows], g_gains[1, :rows]


def solution(mesh):
    split = P(("dp", "tensor"), None)
    row, column, gain = P("dp", "tensor"), P("tensor", "dp"), P("dp")
    return jax.shard_map(
        functools.partial(layer, mesh.shape["dp"], mesh.shape["tensor"]),
        mesh=mesh,
        in_specs=(split, row, row, row, column, row, row, column, gain, gain, split),
        out_specs=(split, split, row, row, row, column, row, row, column, gain, gain),
        check_vma=False,
    )
```

```python
import functools
import math

import jax
import jax.numpy as jnp
from jax import lax
from jax.experimental import pallas as pl
from jax.experimental.pallas import tpu as pltpu
from jax.sharding import PartitionSpec as P

QUERY_HEADS = 16
KEY_VALUE_HEADS = 8
HEAD_SIZE = 96
SEQUENCE_LENGTH = 512

EPSILON = 1e-05
THETA_BASE = 100000.0
MESH = pl.DeviceIdType.MESH


def place():
    d = lax.axis_index("dp")
    return lax.div(d, 4), lax.rem(lax.div(d, 2), 2), lax.rem(d, 2), lax.axis_index("tensor")


def dev(z, y, x, c):
    return (z * 4 + y * 2 + x, c)


def enter(line, pos):
    z, y, x, c = pos
    barrier = pltpu.get_barrier_semaphore()

    def greet(who):
        pl.semaphore_signal(barrier, inc=1, device_id=who, device_id_type=MESH)

    greet(dev(z, y, x, 1 - c))
    greet(dev(z, y, 1 - x, c))
    greet(dev(z, 1 - y, x, c))

    @pl.when(z > 0)
    def _():
        greet(dev(z - 1, y, x, c))

    @pl.when(z < line - 1)
    def _():
        greet(dev(z + 1, y, x, c))

    pl.semaphore_wait(barrier, 3 + (z > 0).astype(jnp.int32) + (z < line - 1).astype(jnp.int32))


def remote(src, dst, send, recv, who):
    return pltpu.make_async_remote_copy(src_ref=src, dst_ref=dst, send_sem=send, recv_sem=recv, device_id=who, device_id_type=MESH)


class Gather:
    def __init__(self, line, pos, shard, full, width, orders, paired, send, recv):
        self.line, self.pos, self.shard, self.full, self.width = line, pos, shard, full, width
        self.orders, self.paired, self.send, self.recv = orders, paired, send, recv
        self.count = shard.shape[-1] // width
        self.depth = line + 1 + paired

    def columns(self, t, sub):
        return t * self.width + sub[1], sub[2]

    def region(self, t, sub, have, z=None):
        first, part = self.columns(t, sub)
        pz, py, px, c = self.pos
        if self.paired:
            first = first + c * self.shard.shape[-1]
        every = slice(None)
        zi = z if z is not None else (every if "z" in have else pz)
        cols = pl.ds(pl.multiple_of(first, 128), part)
        return self.full.at[zi, every if "y" in have else py, every if "x" in have else px, :, cols]

    def own(self, t, sub):
        first, part = self.columns(t, sub)
        return self.shard.at[:, pl.ds(pl.multiple_of(first, 128), part)]

    def copy(self, t, sub, slot, src, dst, who):
        return remote(src, dst, self.send.at[t, sub[0], slot], self.recv.at[t, sub[0], slot], who)

    def hop(self, t, sub, h, up, have, what):
        z, y, x, c = self.pos
        slot = (h - 1) * 2 + up
        if up:
            block, incoming, who = z - (h - 1), z - h, dev(z + 1, y, x, c)
            there, here = (z + 1 < self.line) & (z >= h - 1), z >= h
        else:
            block, incoming, who = z + (h - 1), z + h, dev(z - 1, y, x, c)
            there, here = (z > 0) & (z + h - 1 < self.line), z + h < self.line

        @pl.when(here if what == "recv" else there)
        def _():
            if what == "recv":
                r = self.region(t, sub, have, incoming)
                self.copy(t, sub, slot, r, r, dev(z, y, x, 1 - c)).wait_recv()
                return
            r = self.region(t, sub, have, block)
            cp = self.copy(t, sub, slot, self.own(t, sub) if h == 1 and not have else r, r, who)
            cp.start() if what == "start" else cp.wait_send()

    def act(self, t, sub, order, i, what):
        z, y, x, c = self.pos
        moves, have = [], ""
        for axis in order:
            moves += [(axis, h, have) for h in (range(1, self.line) if axis == "z" else (0,))]
            have += axis
        if self.paired:
            moves.append(("c", 0, have))
        axis, h, have = moves[i]
        if axis == "z":
            for up in (1, 0):
                self.hop(t, sub, h, up, have, what)
            return
        who = {"y": dev(z, 1 - y, x, c), "x": dev(z, y, 1 - x, c), "c": dev(z, y, x, 1 - c)}[axis]
        land = self.region(t, sub, have)
        cp = self.copy(t, sub, 2 * (self.line - 1) + "yxc".index(axis), land if have else self.own(t, sub), land, who)
        {"start": cp.start, "recv": cp.wait_recv, "sent": cp.wait_send}[what]()

    def each(self, t, fn):
        there = (t >= 0) & (t < self.count)
        for v, orders in enumerate(self.orders):
            turn_of = there if len(self.orders) == 1 else there & ((lax.rem(t + 3, 3) == 0) == (v == 1))

            @pl.when(turn_of)
            def _():
                for sub, (order, first, columns) in enumerate(orders):
                    fn((sub, first, columns), order)

    def step(self, t, s):
        def go(sub, order):
            if s > 0:
                self.act(t, sub, order, s - 1, "recv")
            if s < self.depth:
                self.act(t, sub, order, s, "start")

        self.each(t, go)

    def advance(self, p):
        for s in range(self.depth + 1):
            self.step(p - s, s)

    def finish(self):
        @pl.loop(0, self.count)
        def _(t):
            self.each(t, lambda sub, order: [self.act(t, sub, order, i, "sent") for i in range(self.depth)])


def own_copy(g, sem):
    z, y, x, c = g.pos
    first = c * g.shard.shape[-1] if g.paired else 0
    return pltpu.make_async_copy(g.shard, g.full.at[z, y, x, :, pl.ds(pl.multiple_of(first, 128), g.shard.shape[-1])], sem)


def rope_tables(length, width):
    half_width = width // 2
    inverse = THETA_BASE ** (-(jnp.arange(half_width, dtype=jnp.float32) * 2.0 / width))
    angles = jnp.arange(length, dtype=jnp.float32)[:, None] * inverse[None, :]
    cosine, sine = jnp.cos(angles), jnp.sin(angles)
    return jnp.concatenate([cosine, cosine], axis=1), jnp.concatenate([-sine, sine], axis=1)


def turn(x, cosine, sine):
    half = x.shape[-1] // 2
    return x * cosine + jnp.concatenate([x[:, half:], x[:, :half]], axis=1) * sine


def dot_nt(a, b):
    return lax.dot_general(a, b, (((1,), (1,)), ((), ())), preferred_element_type=jnp.float32)


def dot_tn(a, b):
    return lax.dot_general(a, b, (((0,), (0,)), ((), ())), preferred_element_type=jnp.float32)


def dot_nn(a, b):
    return jnp.dot(a, b, preferred_element_type=jnp.float32)


BLOCK = 128


def causal_weights(q, k, b, heads):
    scores = dot_nt(q, k) * (1.0 / math.sqrt(HEAD_SIZE))
    n = scores.shape[1]
    row = lax.broadcasted_iota(jnp.int32, scores.shape, 0) % BLOCK + b * BLOCK
    keep = row >= lax.broadcasted_iota(jnp.int32, scores.shape, 1)
    scores = jnp.where(keep, scores, -jnp.inf)
    log_total = jnp.log(jnp.sum(jnp.exp(scores), axis=1, keepdims=True))
    return jnp.exp(scores - log_total)


def rows_of(ref, first, heads, rows):
    return jnp.concatenate([ref[first + i, rows] for i in range(heads)], axis=0)


ROWS = 128


def each_rows(tokens, step, fn):
    @pl.loop(0, tokens // step)
    def _(r):
        fn(pl.ds(pl.multiple_of(r * step, step), step))


def forward_kernel(line, width, block, *refs):
    refs = list(refs)
    take = lambda n: [refs.pop(0) for _ in range(n)]
    query_in, key_in, value_in, gate_in, up_in, out_in, down_in, gain_a, gain_b, hid, ct, cosine, sine = take(13)
    full, gains_full, q_out, k_out, v_out, mixed_out, n1_pair, n2_pair, ct_pair, mixed_pair, middle_out = take(11)
    tile_pairs = take(3)
    hidden_out, grad_n2, gain = take(3)
    wbuf, gain_buf, n1, n2, flat, qh, kh, vh, mh, mixed, middle, acc, act, tiles, shard, gains, turned = take(17)
    send, recv, gsend, grecv, own_sem, load_sem, gain_sem, local_sem, pair_send, pair_recv, tile_local, tile_send, tile_recv, shard_sem = take(14)

    pos = place()
    z, y, x, c = pos
    tokens, d_model = hid.shape
    half = shard.shape[-1]
    heads, groups = qh.shape[0] // 2, kh.shape[0] // 2
    sibling = dev(z, y, x, 1 - c)
    bf16, f32 = jnp.bfloat16, jnp.float32

    third, half_w = width // 3, width // 2
    mixes = (
        (("zyx", 0, third), ("zxy", third, third), ("xyz", 2 * third, third // 2), ("yxz", 2 * third + third // 2, third // 2)),
        (("zyx", 0, half_w), ("zxy", half_w, half_w)),
    )
    g = Gather(line, pos, shard, full, width, mixes, 1, send, recv)
    gg = Gather(line, pos, gains, gains_full, gains.shape[-1], ((("zyx", 0, gains.shape[-1]),),), 0, gsend, grecv)
    g_own, gg_own = own_copy(g, own_sem.at[0]), own_copy(gg, own_sem.at[1])
    steps = (half // width) - 3
    fills, at = [], 0
    for src in (query_in, key_in, value_in):
        fills.append((src, at, src.shape[1]))
        at += src.shape[1]
    fills.append((out_in, at, out_in.shape[1]))
    at += out_in.shape[1]
    for j in range(steps):
        for i, src in enumerate((gate_in, up_in, down_in)):
            fills.append((src.at[:, pl.ds(j * block, block)], at + j * width + i * block, block))
    fills = [pltpu.make_async_copy(src, shard.at[:, pl.ds(to, n)], shard_sem.at[i]) for i, (src, to, n) in enumerate(fills)]
    for cp in fills:
        cp.start()
    gains[...] = jnp.zeros_like(gains)
    top = lax.broadcasted_iota(jnp.int32, (gains.shape[0], gain_a.shape[1]), 0) == 0
    gains[:, : gain_a.shape[1]] = jnp.where(top, gain_a[...].astype(f32), gain_b[...].astype(f32)).astype(bf16)
    enter(line, pos)
    for cp in fills:
        cp.wait()
    g_own.start()
    gg_own.start()

    def load(t, hh):
        cols = pl.ds(pl.multiple_of(hh * half + t * width, 128), width)
        return pltpu.make_async_copy(full.at[:, :, :, :, cols], wbuf.at[hh], load_sem.at[hh])

    def weight(hh):
        return wbuf[hh].reshape(d_model, width)

    def share(i, own_src, own_dst, other_src, other_dst):
        return pltpu.make_async_copy(own_src, own_dst, local_sem.at[i]), remote(other_src, other_dst, pair_send.at[i], pair_recv.at[i], sibling)

    ends = (pl.ds(0, tokens), pl.ds(tokens, tokens))
    lefts = ((ct, ct_pair), (n1, n1_pair), (n2, n2_pair))
    shares = [share(i, turned.at[i], pair.at[:, ends[0]], turned.at[i], pair.at[:, ends[1]]) for i, (_, pair) in enumerate(lefts)]
    hw = mixed.shape[1] // 2
    side = lambda ref, s, w: ref.at[:, pl.ds(pl.multiple_of(s * w, 128), w)]
    shares.append(share(3, side(mixed, c, hw), mixed_pair.at[0], side(mixed, 1 - c, hw), mixed_pair.at[1]))
    keeps = [pltpu.make_async_copy(src, dst, local_sem.at[4 + i]) for i, (src, dst) in enumerate(((qh, q_out), (kh, k_out), (vh, v_out), (mixed, mixed_out), (middle, middle_out)))]

    def begin(i):
        if i < len(lefts):
            span = 256

            @pl.loop(0, d_model // span)
            def _(e):
                at = pl.ds(pl.multiple_of(e * span, span), span)
                turned[i, at, :] = lefts[i][0][:, at].T

        for cp in shares[i]:
            cp.start()

    def end(i):
        for cp in shares[i]:
            cp.wait()

    def tile_copies(j, hh):
        slot = lax.rem(j, 2)
        cols = pl.ds(pl.multiple_of(j * block, 128), block)
        own = [pltpu.make_async_copy(tiles.at[slot, hh, i], pair.at[0, :, cols], tile_local.at[j, i]) for i, pair in enumerate(tile_pairs)]
        out = [remote(tiles.at[slot, hh, i], pair.at[1, :, cols], tile_send.at[j, i], tile_recv.at[j, i], sibling) for i, pair in enumerate(tile_pairs)]
        return own, out

    def tile_act(j, hh, what):
        @pl.when(hh == c)
        def _():
            for cp in tile_copies(j, hh)[0]:
                cp.start() if what == "start" else cp.wait()

        @pl.when(hh != c)
        def _():
            for cp in tile_copies(j, hh)[1]:
                cp.start() if what == "start" else cp.wait_send()

    def normalize():
        loaded = pltpu.make_async_copy(gains_full, gain_buf, gain_sem)
        loaded.start()
        loaded.wait()
        n = d_model // (gain_buf.shape[0] * 4)
        table = gain_buf[...].astype(f32)
        for i in range(2):
            gain[i : i + 1, :] = jnp.concatenate([table[a, b, e, i : i + 1, :n] for a in range(gain_buf.shape[0]) for b in range(2) for e in range(2)], axis=1)

        def rows_of_norm(rows):
            v = hid[rows, :].astype(f32)
            v = v * lax.rsqrt(jnp.mean(v * v, axis=1, keepdims=True) + EPSILON)
            n1[rows, :] = (v * gain[0:1, :]).astype(bf16)

        each_rows(tokens, ROWS, rows_of_norm)
        begin(1)

    def project(hh, outs):
        flat[...] = dot_nn(n1[...], weight(hh))

        def to_heads(rows):
            cos, sin = cosine[rows, :], sine[rows, :]
            first = 0
            for n, target, turned in outs:
                for h in range(n):
                    v = flat[rows, (first + h) * HEAD_SIZE : (first + h + 1) * HEAD_SIZE]
                    target[hh * n + h, rows] = (turn(v, cos, sin) if turned else v).astype(bf16)
                first += n

        each_rows(tokens, ROWS, to_heads)

    def attend_half(hh):
        per = heads // groups
        blocks = tokens // BLOCK

        @pl.loop(0, groups)
        def _(i):
            kv = hh * groups + i
            for b in range(blocks):
                rows, n = pl.ds(b * BLOCK, BLOCK), (b + 1) * BLOCK
                w = causal_weights(rows_of(qh, kv * per, per, rows), kh[kv, :n], b, per).astype(bf16)
                m = dot_nn(w, vh[kv, :n]).astype(bf16)
                for e in range(per):
                    mh[kv * per + e, rows] = m[e * BLOCK : (e + 1) * BLOCK]

        lanes = pl.ds(pl.multiple_of(hh * hw, 128), hw)

        def join(rows):
            mixed[rows, lanes] = jnp.concatenate([mh[hh * heads + h, rows] for h in range(heads)], axis=1)

        each_rows(tokens, ROWS, join)

    def leave_attention(hh):
        part = dot_nt(mixed[:, pl.ds(pl.multiple_of(hh * hw, 128), hw)], weight(hh))

        @pl.when(hh == c)
        def _():
            middle[...] = hid[...].astype(f32) + part

        @pl.when(hh != c)
        def _():
            middle[...] += part
            begin(3)
            for cp in keeps:
                cp.start()

            def rows_of_norm(rows):
                v = middle[rows, :]
                acc[rows, :] = v
                v = v * lax.rsqrt(jnp.mean(v * v, axis=1, keepdims=True) + EPSILON)
                n2[rows, :] = (v * gain[1:2, :]).astype(bf16)
                grad_n2[rows, :] = jnp.zeros_like(v)

            each_rows(tokens, ROWS, rows_of_norm)
            begin(2)

    def feed_forward(j, hh):
        @pl.when(j >= 2)
        def _():
            tile_act(j - 2, hh, "wait")

        part = lax.rem(j, 2)
        act[0] = dot_nn(n2[...], weight(hh)[:, :block])
        act[1] = dot_nn(n2[...], weight(hh)[:, block : 2 * block])
        act[2] = dot_nn(ct[...], weight(hh)[:, 2 * block :])

        def gated(rows):
            gate, up, grad = act[0, rows], act[1, rows], act[2, rows]
            sigma = jax.nn.sigmoid(gate)
            tiles[part, hh, 0, rows] = (gate * sigma * up).astype(bf16)
            tiles[part, hh, 1, rows] = (grad * up * sigma * (1.0 + gate * (1.0 - sigma))).astype(bf16)
            tiles[part, hh, 2, rows] = (grad * gate * sigma).astype(bf16)

        each_rows(tokens, ROWS // 2, gated)
        tile_act(j, hh, "start")
        acc[...] += dot_nt(tiles[part, hh, 0], weight(hh)[:, 2 * block :])
        both = jnp.concatenate([tiles[part, hh, 1], tiles[part, hh, 2]], axis=1)
        grad_n2[...] += dot_nt(both, weight(hh)[:, : 2 * block])

    count = g.count

    @pl.loop(0, count + g.depth)
    def _(p):
        gg.advance(p)
        g.advance(p)

        @pl.when(p == 0)
        def _():
            g_own.wait()
            gg_own.wait()

        @pl.when(p == 1)
        def _():
            begin(0)

        chunk_of = lambda hh: jnp.where(hh == c, p - g.depth + 1, p - g.depth)
        for hh in range(2):
            u = chunk_of(hh)

            @pl.when((u >= 0) & (u < count))
            def _():
                load(u, hh).start()

        @pl.loop(0, 2)
        def _(i):
            hh = jnp.where(i == 0, 1 - c, c)
            u = chunk_of(hh)

            @pl.when((u >= 0) & (u < count))
            def _():
                load(u, hh).wait()

                @pl.when((u == 0) & (hh == c))
                def _():
                    normalize()

                @pl.when(u == 0)
                def _():
                    project(hh, ((heads, qh, True),))

                @pl.when(u == 1)
                def _():
                    project(hh, ((groups, kh, True), (groups, vh, False)))
                    attend_half(hh)

                @pl.when(u == 2)
                def _():
                    leave_attention(hh)

                @pl.when(u >= 3)
                def _():
                    feed_forward(u - 3, hh)

    def rows_out(rows):
        hidden_out[rows, :] = acc[rows, :].astype(bf16)

    each_rows(tokens, ROWS, rows_out)
    for i in range(len(shares)):
        end(i)
    for cp in keeps:
        cp.wait()
    for j in range(max(steps - 2, 0), steps):
        for hh in range(2):
            tile_act(j, hh, "wait")

    @pl.loop(0, steps)
    def _(j):
        for cp in tile_copies(j, 0)[1]:
            cp.wait_recv()

    g.finish()
    gg.finish()


def forward(line, shards, gain_pair, hidden_in, cotangent, cosine, sine, block):
    tokens, d_model = hidden_in.shape
    rows = gain_pair[0].shape[1]
    half = sum(s.shape[1] for s in shards)
    gains = jax.ShapeDtypeStruct((8, 128), jnp.bfloat16)
    width = 3 * block
    count = half // width
    steps = count - 3
    heads, groups = QUERY_HEADS // 2, KEY_VALUE_HEADS // 2
    bf16, f32 = jnp.bfloat16, jnp.float32
    struct = jax.ShapeDtypeStruct
    hbm, vmem = pl.BlockSpec(memory_space=pl.ANY), pl.BlockSpec(memory_space=pltpu.VMEM)
    dma = pltpu.SemaphoreType.DMA
    pair = struct((d_model, 2 * tokens), bf16)
    tile_pair = struct((2, tokens, steps * block), bf16)
    head_shape = lambda n: (n, tokens, HEAD_SIZE)
    slots = 2 * (line - 1) + 3
    outs = [
        struct((line, 2, 2, rows, 2 * half), bf16),
        struct((line, 2, 2) + gains.shape, bf16),
        struct(head_shape(2 * heads), bf16),
        struct(head_shape(2 * groups), bf16),
        struct(head_shape(2 * groups), bf16),
        struct((tokens, 2 * heads * HEAD_SIZE), bf16),
        pair,
        pair,
        pair,
        struct((2, tokens, heads * HEAD_SIZE), bf16),
        struct((tokens, d_model), f32),
        tile_pair,
        tile_pair,
        tile_pair,
        struct((tokens, d_model), bf16),
        struct((tokens, d_model), f32),
        struct((8, d_model), f32),
    ]
    V = pltpu.VMEM
    return pl.pallas_call(
        functools.partial(forward_kernel, line, width, block),
        out_shape=outs,
        in_specs=[hbm] * 7 + [vmem] * 6,
        out_specs=[hbm] * 14 + [vmem] * 3,
        scratch_shapes=[
            V((2, line, 2, 2, rows, width), bf16),
            V((line, 2, 2) + gains.shape, bf16),
            V((tokens, d_model), bf16),
            V((tokens, d_model), bf16),
            V((tokens, width), f32),
            V(head_shape(2 * heads), bf16),
            V(head_shape(2 * groups), bf16),
            V(head_shape(2 * groups), bf16),
            V(head_shape(2 * heads), bf16),
            V((tokens, 2 * heads * HEAD_SIZE), bf16),
            V((tokens, d_model), f32),
            V((tokens, d_model), f32),
            V((3, tokens, block), f32),
            V((2, 2, 3, tokens, block), bf16),
            V((rows, half), bf16),
            V(gains.shape, bf16),
            V((3, d_model, tokens), bf16),
            dma((count, 4, slots)),
            dma((count, 4, slots)),
            dma((1, 1, slots)),
            dma((1, 1, slots)),
            dma((2,)),
            dma((2,)),
            dma,
            dma((9,)),
            dma((4,)),
            dma((4,)),
            dma((steps, 3)),
            dma((steps, 3)),
            dma((steps, 3)),
            dma((4 + 3 * steps,)),
        ],
        compiler_params=pltpu.CompilerParams(collective_id=0, has_side_effects=True, vmem_limit_bytes=64 * 2**20 - 2**17),
        name="gather_forward",
    )(*shards, *gain_pair, hidden_in, cotangent, cosine, sine)


class Scatter:
    def __init__(self, line, pos, count, plain, early, final):
        self.line, self.pos, self.count, self.final = line, pos, count, final
        self.own, self.first, self.second, self.up, self.down, self.send, self.recv = plain
        self.early = early
        self.lags = [0, 2, 4, 5, 4 + line, 5 + line]
        self.depth = self.lags[-1]

    def is_early(self, t):
        return lax.rem(t + 5, 5) == 4

    def plain_number(self, t):
        return t - lax.div(t, 5)

    def parts(self, t, early):
        if early:
            i, (own, first, second, up, down, send, recv) = lax.div(t, 5), self.early
        else:
            i, own, first, second, up, down, send, recv = self.plain_number(t), self.own, self.first, self.second, self.up, self.down, self.send, self.recv
        o, r = lax.rem(i, own.shape[0]), lax.rem(i, first.shape[0])
        return own.at[o], first.at[r], second.at[r], up.at[r], down.at[r], send.at[r], recv.at[r]

    def place_of(self, t, early):
        return self.parts(t, early)[0]

    def merge(self, dst, a, b, loops):
        def go(lead, rest):
            if not rest:
                dst[lead] = a[lead] + b[lead]
            elif rest[0] > 2:
                @pl.loop(0, rest[0])
                def _(i):
                    go(lead + (i,), rest[1:])
            else:
                for i in range(rest[0]):
                    go(lead + (i,), rest[1:])

        go((), loops)

    def pair_moves(self, t, v):
        z, y, x, c = self.pos
        early = v >= 2
        own, first, second, _, _, send, recv = self.parts(t, early)
        over_x, over_y = dev(z, y, 1 - x, c), dev(z, 1 - y, x, c)
        lead = (z,) if early else (slice(None),)
        if v % 2 == 0:
            give, keep, who = own.at[lead + (slice(None), 1 - x)], own.at[lead + (slice(None), x)], (over_x, over_y)
        else:
            give, keep, who = own.at[lead + (1 - y,)], own.at[lead + (y,)], (over_y, over_x)
        a, b = (1 - y, y) if v % 2 == 0 else (1 - x, x)
        lead = () if early else (slice(None),)
        one = remote(give, first, send.at[0], recv.at[0], who[0])
        two = remote(first.at[lead + (a,)], second, send.at[1], recv.at[1], who[1])
        return one, two, keep, first, second, first.at[lead + (b,)]

    def hop(self, p, j, way, early):
        z, y, x, c = self.pos
        last = self.line - 1
        travelled = z if way == 0 else last - z
        t = p - (0 if early else self.lags[3]) - j - travelled
        target = last - j if way == 0 else j
        passes = (target > z) if way == 0 else (target < z)

        def go():
            own, _, second, up, down, send, recv = self.parts(t, early)
            cur, ref = own if early else second, (up if way == 0 else down).at[j]
            nxt = dev(z + 1, y, x, c) if way == 0 else dev(z - 1, y, x, c)
            slot = 2 + 2 * j + way

            @pl.when(travelled == 0)
            def _():
                remote(cur.at[target], ref, send.at[slot], recv.at[slot], nxt).start()

            @pl.when(travelled > 0)
            def _():
                cp = remote(ref, ref, send.at[slot], recv.at[slot], nxt)
                cp.wait_recv()
                self.merge(ref, ref, cur.at[target], (2, 2) if early else ())
                cp.start()

        @pl.when(passes & (t >= 0) & (t < self.count) & (self.is_early(t) == early))
        def _():
            go()

    def arrive(self, t, early):
        z, y, x, c = self.pos
        _, _, _, up, down, send, recv = self.parts(t, early)
        last = self.line - 1
        ends = []
        for way, ref, has, k in ((0, up, z > 0, last - z), (1, down, z < last, z)):

            @pl.when(has)
            def _():
                slot = 2 + 2 * k + way
                remote(ref.at[k], ref.at[k], send.at[slot], recv.at[slot], dev(z, y, x, 1 - c)).wait_recv()

            ends.append((has, ref.at[jnp.minimum(k, last - 1)]))
        return ends

    def close(self, t):
        f32 = jnp.float32
        total = self.parts(t, False)[2][self.pos[0]].astype(f32)
        for has, ref in self.arrive(t, False):
            total = total + jnp.where(has, ref[...].astype(f32), 0.0)
        self.final(t, total)

    def close_early(self, t, v):
        z = self.pos[0]
        mine = self.place_of(t, True).at[z]
        ends = self.arrive(t, True)
        for i in range(2):
            for k in range(2):
                total = mine[i, k].astype(jnp.float32)
                for has, ref in ends:
                    total = total + jnp.where(has, ref[i, k].astype(jnp.float32), 0.0)
                mine[i, k] = total.astype(mine.dtype)
        self.pair_moves(t, v)[0].start()

    def drain(self, t, early):
        z, y, x, c = self.pos
        _, _, _, up, down, send, recv = self.parts(t, early)
        if early:
            self.pair_moves(t, 2)[0].wait_send()
        self.pair_moves(t, 2 * early)[1].wait_send()
        for j in range(self.line - 1):
            for way, ref, target in ((0, up, self.line - 1 - j), (1, down, j)):

                @pl.when((target > z) if way == 0 else (target < z))
                def _():
                    slot = 2 + 2 * j + way
                    remote(ref.at[j], ref.at[j], send.at[slot], recv.at[slot], dev(z, y, x, 1 - c)).wait_send()

    def plain(self, t, fn):
        @pl.when((t >= 0) & (t < self.count) & ~self.is_early(t))
        def _():
            fn()

    def sorts(self, t, fn, early):
        number = lax.div(t, 5) if early else self.plain_number(t)
        for v in range(2):
            @pl.when((t >= 0) & (t < self.count) & (self.is_early(t) == early) & (lax.rem(number + 2, 2) == v))
            def _():
                fn(v + 2 * early)

    def begin(self, t):
        self.sorts(t, lambda v: self.pair_moves(t, v)[0].start(), False)

    def release(self, p):
        t = p - self.own.shape[0] * 5 // 4
        self.plain(t, lambda: self.pair_moves(t, 0)[0].wait_send())

    def advance(self, p):
        line = self.line

        def one(t, v):
            first_copy, second_copy, keep, first, second, _ = self.pair_moves(t, v)
            first_copy.wait_recv()
            self.merge(first, first, keep, (2,) if v >= 2 else (line, 2))
            second_copy.start()

        def two(t, v):
            _, second_copy, _, _, second, keep = self.pair_moves(t, v)
            second_copy.wait_recv()
            if v >= 2:
                self.final(t, keep[...].astype(jnp.float32) + second[...].astype(jnp.float32))
            else:
                self.merge(second, second, keep, (line,))

        for j in range(line - 1):
            for way in range(2):
                self.hop(p, j, way, True)
        for step, lag, early in ((one, self.lags[1], False), (two, self.lags[2], False), (self.close_early, line, True), (one, line + 2, True), (two, line + 4, True)):
            t = p - lag
            self.sorts(t, lambda v, t=t, step=step: step(t, v), early)
        for j in range(line - 1):
            for way in range(2):
                self.hop(p, j, way, False)
        t = p - self.lags[-2]
        self.plain(t, lambda t=t: self.close(t))
        t = p - self.lags[-1]
        self.plain(t, lambda t=t: self.drain(t, False))

        @pl.when((t >= 0) & (t < self.count) & self.is_early(t))
        def _():
            self.drain(t, True)


def greet_all(n, pos):
    z, y, x, c = pos
    d = z * 4 + y * 2 + x
    barrier = pltpu.get_barrier_semaphore()

    @pl.loop(1, n)
    def _(i):
        pl.semaphore_signal(barrier, inc=1, device_id=(lax.rem(d + i, n), c), device_id_type=MESH)

    pl.semaphore_signal(barrier, inc=1, device_id=(d, 1 - c), device_id_type=MESH)
    pl.semaphore_wait(barrier, n)


def backward_kernel(line, cols, starts, *refs):
    refs = list(refs)
    take = lambda n: [refs.pop(0) for _ in range(n)]
    q, k, v, mixed, full, hid, ct, middle, grad_n2, gains, cosine, sine = take(12)
    n1_pair, n2_pair, ct_pair, mixed_pair, hidden_pair, gate_pair, up_pair = take(7)
    qkv_pair, grad_query, grad_key, grad_value, grad_in_out, out_out, out_gate, out_up, out_down, out_gains, gm_pair = take(11)
    own, first, second, up, down, xt, ybuf, qh, kh, vh, mh, gh, gm, dots, dq, dk, dv, dqkv, wbuf, gmid, hbuf, out_qkv, gain_one, part, parts_in, pair_in, gain_two, gmb, turned, own_e, first_e, second_e, up_e, down_e, grad_in = take(35)
    send, recv, xsem, ysem, half_sem, wsem, msem, qkv_local, qkv_send, qkv_recv, part_send, part_recv, out_sem, swap_sem, gm_sem, send_e, recv_e = take(17)

    pos = place()
    z, y, x, c = pos
    d = z * 4 + y * 2 + x
    n = line * 4
    tokens, d_model = hid.shape
    count = starts[-1]
    heads, groups = qh.shape[0], kh.shape[0]
    share = heads // groups
    blocks = tokens // BLOCK
    width = wbuf.shape[-1]
    half_width = dqkv.shape[1] // 2
    scale = 1.0 / math.sqrt(HEAD_SIZE)
    bf16, f32 = jnp.bfloat16, jnp.float32
    sources = (hidden_pair, gate_pair, up_pair, mixed_pair, qkv_pair)
    lefts = ((0, ct_pair), (starts[1], n2_pair), (starts[3], gm_pair), (starts[4], n1_pair))

    def final(t, total):
        for i, out in enumerate((out_down, out_gate, out_up, out_out, out_qkv)):
            at = pl.ds(pl.multiple_of((t - starts[i]) * cols, 128), cols)

            @pl.when((t >= starts[i]) & (t < starts[i + 1]))
            def _():
                out[:, at] = total

    s = Scatter(line, pos, count, (own, first, second, up, down, send, recv), (own_e, first_e, second_e, up_e, down_e, send_e, recv_e), final)

    def load_left(i):
        return pltpu.make_async_copy(lefts[i][1], xt.at[i % 2], xsem.at[i % 2])

    def load_right(t, act):
        slot = lax.rem(t, 2)
        for i, src in enumerate(sources):
            at = pl.ds(pl.multiple_of((t - starts[i]) * cols, 128), cols)

            @pl.when((t >= starts[i]) & (t < starts[i + 1]))
            def _():
                cp = pltpu.make_async_copy(src.at[:, :, at], ybuf.at[slot], ysem.at[slot])
                cp.start() if act == "start" else cp.wait()

    def half_loads(hh):
        take_heads = lambda ref, m: ref.at[pl.ds(hh * m, m)]
        lanes = pl.ds(pl.multiple_of(hh * mh.shape[1], 128), mh.shape[1])
        pairs = ((take_heads(q, heads), qh), (take_heads(k, groups), kh), (take_heads(v, groups), vh), (mixed.at[:, lanes], mh))
        return [pltpu.make_async_copy(src, dst, half_sem.at[i]) for i, (src, dst) in enumerate(pairs)]

    def half_load(hh, act):
        for cp in half_loads(hh):
            cp.start() if act == "start" else cp.wait()

    each = half_width // width
    half_columns = full.shape[-1] // 2

    def weights(i):
        at = (i * half_columns + each * width) if i < 2 else ((i - 2) // each * half_columns + (i - 2) % each * width)
        return pltpu.make_async_copy(full.at[:, :, :, :, pl.ds(at, width)], wbuf.at[i % 2], wsem.at[i % 2])

    def weight(i):
        return wbuf[i % 2].reshape(d_model, width)

    middle_in = pltpu.make_async_copy(middle, grad_in, msem.at[0])
    grad_n2_in = pltpu.make_async_copy(grad_n2, gmid, msem.at[1])
    ct_in, hid_in = (pltpu.make_async_copy(src, hbuf, msem.at[2]) for src in (ct, hid))

    own_half = lambda ref, which: ref.at[:, pl.ds(pl.multiple_of(which * half_width, 128), half_width)]

    def qkv_copies():
        return (
            pltpu.make_async_copy(own_half(dqkv, c), qkv_pair.at[0], qkv_local),
            remote(own_half(dqkv, 1 - c), qkv_pair.at[1], qkv_send, qkv_recv, (d, 1 - c)),
        )

    def gm_copies():
        return (
            pltpu.make_async_copy(turned, gm_pair.at[:, pl.ds(0, tokens)], gm_sem.at[0]),
            remote(turned, gm_pair.at[:, pl.ds(tokens, tokens)], gm_sem.at[1], gm_sem.at[2], (d, 1 - c)),
        )

    def norm_two_back():
        for cp in (middle_in, grad_n2_in, ct_in):
            cp.wait()
        gain_two[...] = jnp.zeros_like(gain_two)

        def rows_back(rows):
            a, grad = grad_in[rows, :], gmid[rows, :]
            inverse = lax.rsqrt(jnp.mean(a * a, axis=1, keepdims=True) + EPSILON)
            unit = a * inverse
            scaled = grad * gains[1:2, :]
            inner = jnp.mean(scaled * unit, axis=1, keepdims=True)
            total = hbuf[rows, :].astype(f32) + inverse * (scaled - unit * inner)
            gmid[rows, :] = total
            gmb[rows, :] = total.astype(bf16)
            gain_two[...] += jnp.sum(grad * unit, axis=0, keepdims=True)

        each_rows(tokens, ROWS, rows_back)
        hid_in.start()
        span = 256

        @pl.loop(0, d_model // span)
        def _(e):
            at = pl.ds(pl.multiple_of(e * span, span), span)
            turned[at, :] = gmb[:, at].T

        for cp in gm_copies():
            cp.start()

    def through_out(i):
        weights(i).wait()
        gh[...] = dot_nn(gmb[...], weight(i))
        weights(i + 2).start()

    def prepare(hh):
        half_load(hh, "wait")

        def rows_of_dots(rows):
            for h in range(heads):
                lanes = slice(h * HEAD_SIZE, (h + 1) * HEAD_SIZE)
                g = gh[rows, lanes]
                dots[h, rows] = jnp.sum(g * mh[rows, lanes].astype(f32), axis=1, keepdims=True)
                gm[h, rows] = g.astype(bf16)

        each_rows(tokens, ROWS, rows_of_dots)
        dk[...] = jnp.zeros_like(dk)
        dv[...] = jnp.zeros_like(dv)

    def group_back(g, which):
        for b in which:
            rows, m = pl.ds(b * BLOCK, BLOCK), (b + 1) * BLOCK
            qb, gb, db = (rows_of(ref, g * share, share, rows) for ref in (qh, gm, dots))
            kb, vb = kh[g, :m], vh[g, :m]
            p = causal_weights(qb, kb, b, share)
            ds = (p * (dot_nt(gb, vb) - db)).astype(bf16)
            dv[g, :m] += dot_tn(p.astype(bf16), gb)
            dk[g, :m] += dot_tn(ds, qb)
            r = dot_nn(ds, kb) * scale
            for i in range(share):
                dq[g * share + i, rows] = r[i * BLOCK : (i + 1) * BLOCK]

    def join(hh):
        def rows_of_join(rows):
            cos, sin = cosine[rows, :], -sine[rows, :]
            parts = [turn(dq[h, rows], cos, sin) for h in range(heads)]
            parts += [turn(dk[g, rows] * scale, cos, sin) for g in range(groups)]
            parts += [dv[g, rows] for g in range(groups)]
            dqkv[rows, pl.ds(pl.multiple_of(hh * half_width, 128), half_width)] = jnp.concatenate([a.astype(bf16) for a in parts], axis=1)

        each_rows(tokens, ROWS, rows_of_join)

    def against(i):
        weights(i + 2).wait()
        r = dot_nt(dqkv[:, i * width : (i + 1) * width], weight(i))
        if i == 0:
            grad_in[...] = r
        else:
            grad_in[...] += r
        if i + 2 < 2 * each:
            weights(i + 4).start()

    def norm_one_back():
        hid_in.wait()
        gain_one[...] = jnp.zeros_like(gain_one)

        def rows_back(rows):
            a = hbuf[rows, :].astype(f32)
            inverse = lax.rsqrt(jnp.mean(a * a, axis=1, keepdims=True) + EPSILON)
            unit, grad = a * inverse, grad_in[rows, :]
            scaled = grad * gains[0:1, :]
            inner = jnp.mean(scaled * unit, axis=1, keepdims=True)
            grad_in[rows, :] = gmid[rows, :] + inverse * (scaled - unit * inner)
            gain_one[...] += jnp.sum(grad * unit, axis=0, keepdims=True)

        each_rows(tokens, ROWS, rows_back)
        size = d_model // n
        part[...] = jnp.zeros_like(part)
        for i in range(n):
            for row, ref in enumerate((gain_one, gain_two)):
                part[i, row : row + 1, :size] = ref[:, i * size : (i + 1) * size]

    def part_copy(i):
        to = lax.rem(d + i, n)
        return remote(part.at[to], parts_in.at[i], part_send.at[i], part_recv.at[i], (to, c))

    load_left(0).start()
    load_left(1).start()
    load_right(0, "start")
    half_load(0, "start")
    for cp in (middle_in, grad_n2_in, ct_in):
        cp.start()
    for i in range(2):
        weights(i).start()
    greet_all(n, pos)

    swap = remote(out_gains, pair_in, swap_sem.at[0], swap_sem.at[1], (d, 1 - c))
    grad_in_copy = pltpu.make_async_copy(grad_in, grad_in_out, out_sem.at[3])
    stages = 2 * groups + 3
    chain = 1
    turns = chain + 2 * stages
    norm_at = turns + 2 * each

    @pl.loop(0, count + s.depth)
    def _(p):
        s.release(p)
        for i, (at, _) in enumerate(lefts):

            @pl.when(p == at)
            def _():
                load_left(i).wait()
                if 1 <= i < len(lefts) - 1:
                    load_left(i + 1).start()

        @pl.when(p == starts[1] - 1)
        def _():
            for cp in gm_copies():
                cp.wait()

        @pl.when(p == starts[4] - 2)
        def _():
            for cp in qkv_copies():
                cp.wait()

        @pl.when(p < count)
        def _():
            load_right(p, "wait")

            @pl.when(p + 1 < count)
            def _():
                load_right(p + 1, "start")

            side = lax.rem(sum((p >= at).astype(jnp.int32) for at, _ in lefts[1:]), 2)
            right = ybuf[lax.rem(p, 2)].reshape(2 * tokens, cols)
            for early in (False, True):

                @pl.when(s.is_early(p) == early)
                def _():
                    s.place_of(p, early)[...] = dot_nn(xt[side], right).reshape(own.shape[1:]).astype(bf16)

            s.begin(p)

        s.advance(p)

        @pl.when(p == chain - 1)
        def _():
            norm_two_back()

        for i in range(2):

            @pl.when(p == chain + i * stages)
            def _():
                through_out(i)

        @pl.when((p >= chain) & (p < turns))
        def _():
            hh, r = lax.div(p - chain, stages), lax.rem(p - chain, stages) - 1

            @pl.when(r == 0)
            def _():
                prepare(hh)

            for e, which in enumerate((range(blocks - 1), range(blocks - 1, blocks))):

                @pl.when((r > 0) & (r <= 2 * groups) & (lax.rem(r + 1, 2) == e))
                def _():
                    group_back(lax.div(r - 1, 2), which)

            @pl.when(r == stages - 2)
            def _():
                join(hh)

                @pl.when(hh == 0)
                def _():
                    half_load(1, "start")

                @pl.when(hh == 1)
                def _():
                    for cp in qkv_copies():
                        cp.start()

        for i in range(2 * each):

            @pl.when(p == turns + i)
            def _():
                against(i)

        @pl.when(p == norm_at)
        def _():
            norm_one_back()

        @pl.when(p == norm_at + 1)
        def _():
            grad_in_copy.start()

            @pl.loop(1, n)
            def _(i):
                part_copy(i).start()

        @pl.when(p == count + s.depth - 2)
        def _():
            @pl.loop(1, n)
            def _(i):
                part_copy(i).wait()

            out_gains[...] = part[d] + jnp.sum(parts_in[1:], axis=0)
            swap.start()

    ends, first_column = [grad_in_copy], 0
    for i, out in enumerate((grad_query, grad_key, grad_value)):
        cp = pltpu.make_async_copy(out_qkv.at[:, pl.ds(first_column, out.shape[1])], out, out_sem.at[i])
        cp.start()
        ends.append(cp)
        first_column += out.shape[1]
    swap.wait()
    out_gains[...] += pair_in[...]
    for cp in ends:
        cp.wait()


def backward(line, cols, arrays, halves):
    q, k, v, mixed, full, hid = arrays[:6]
    tokens, d_model = hid.shape
    rows = full.shape[3]
    n = line * 4
    down_w, gate_w, up_w, out_w, q_w, k_w, v_w = halves
    qkv_w = q_w + k_w + v_w
    starts = [0]
    for w in (down_w, gate_w, up_w, out_w, qkv_w):
        starts.append(starts[-1] + w // cols)
    heads, groups = q.shape[0] // 2, k.shape[0] // 2
    width = q_w
    bf16, f32 = jnp.bfloat16, jnp.float32
    struct, V, dma = jax.ShapeDtypeStruct, pltpu.VMEM, pltpu.SemaphoreType.DMA
    hbm, vmem = pl.BlockSpec(memory_space=pl.ANY), pl.BlockSpec(memory_space=pltpu.VMEM)
    ring, own_ring = (line + 12) * 4 // 5 + 1, 4
    ring_e, own_ring_e = (line + 16) // 5, (line + 5) // 5 + 1
    head = lambda m: (m, tokens, HEAD_SIZE)
    sems = 2 + 2 * (line - 1)
    outs = [struct((2, tokens, qkv_w), bf16)]
    outs += [struct((rows, w), f32) for w in (q_w, k_w, v_w)]
    outs += [struct((tokens, d_model), f32), struct((rows, out_w), f32), struct((rows, gate_w), f32), struct((rows, up_w), f32), struct((rows, down_w), f32), struct((8, 128), f32)]
    outs += [struct((d_model, 2 * tokens), bf16)]
    return pl.pallas_call(
        functools.partial(backward_kernel, line, cols, tuple(starts)),
        out_shape=outs,
        in_specs=[hbm] * 9 + [vmem] * 3 + [hbm] * 7,
        out_specs=[hbm] * 5 + [vmem] * 5 + [hbm],
        scratch_shapes=[
            V((own_ring, line, 2, 2, rows, cols), bf16),
            V((ring, line, 2, rows, cols), bf16),
            V((ring, line, rows, cols), bf16),
            V((ring, line - 1, rows, cols), bf16),
            V((ring, line - 1, rows, cols), bf16),
            V((2, d_model, 2 * tokens), bf16),
            V((2, 2, tokens, cols), bf16),
            V(head(heads), bf16),
            V(head(groups), bf16),
            V(head(groups), bf16),
            V((tokens, heads * HEAD_SIZE), bf16),
            V((tokens, heads * HEAD_SIZE), f32),
            V(head(heads), bf16),
            V((heads, tokens, 1), f32),
            V(head(heads), f32),
            V(head(groups), f32),
            V(head(groups), f32),
            V((tokens, 2 * qkv_w), bf16),
            V((2, line, 2, 2, rows, width), bf16),
            V((tokens, d_model), f32),
            V((tokens, d_model), bf16),
            V((rows, qkv_w), f32),
            V((1, d_model), f32),
            V((n, 8, 128), f32),
            V((n, 8, 128), f32),
            V((8, 128), f32),
            V((1, d_model), f32),
            V((tokens, d_model), bf16),
            V((d_model, tokens), bf16),
            V((own_ring_e, line, 2, 2, rows, cols), bf16),
            V((ring_e, 2, rows, cols), bf16),
            V((ring_e, rows, cols), bf16),
            V((ring_e, line - 1, 2, 2, rows, cols), bf16),
            V((ring_e, line - 1, 2, 2, rows, cols), bf16),
            V((tokens, d_model), f32),
            dma((ring, sems)),
            dma((ring, sems)),
            dma((2,)),
            dma((2,)),
            dma((4,)),
            dma((2,)),
            dma((3,)),
            dma,
            dma,
            dma,
            dma((n,)),
            dma((n,)),
            dma((4,)),
            dma((2,)),
            dma((3,)),
            dma((ring_e, sems)),
            dma((ring_e, sems)),
        ],
        compiler_params=pltpu.CompilerParams(collective_id=1, has_side_effects=True, vmem_limit_bytes=64 * 2**20 - 2**17),
        name="backward_scatter",
    )(*arrays)


def finish_kernel(n, *refs):
    srcs, outs, bufs, (loads, stores) = refs[:n], refs[n : 2 * n], refs[2 * n : 3 * n], refs[3 * n :]
    for i in range(n):
        pltpu.make_async_copy(srcs[i], bufs[i], loads.at[i]).start()
    for i in range(n):
        pltpu.make_async_copy(srcs[i], bufs[i], loads.at[i]).wait()
        pltpu.make_async_copy(bufs[i], outs[i], stores.at[i]).start()
    for i in range(n):
        pltpu.make_async_copy(bufs[i], outs[i], stores.at[i]).wait()


def finish(arrays):
    n = len(arrays)
    hbm = pl.BlockSpec(memory_space=pl.ANY)
    return pl.pallas_call(
        functools.partial(finish_kernel, n),
        out_shape=[jax.ShapeDtypeStruct(a.shape, a.dtype) for a in arrays],
        in_specs=[hbm] * n,
        out_specs=[hbm] * n,
        scratch_shapes=[pltpu.VMEM(a.shape, a.dtype) for a in arrays] + [pltpu.SemaphoreType.DMA((n,)), pltpu.SemaphoreType.DMA((n,))],
        compiler_params=pltpu.CompilerParams(vmem_limit_bytes=64 * 2**20 - 2**17),
        name="finish",
    )(*arrays)


def layer(n_dp, n_tensor, hidden_in, query_weight, key_matrix, value_matrix, out_weight, gate_weight, up_weight, down_weight, attention_gain, feedforward_gain, cotangent):
    line = n_dp // 4
    rows = attention_gain.shape[0]
    block = (query_weight.shape[1] // 3) & -128
    cosine, sine = rope_tables(SEQUENCE_LENGTH, HEAD_SIZE)
    (full, _, q, k, v, mixed, n1, n2, ct, mixed_pair, middle, hidden, gate, up, hidden_out, grad_n2, gain_rows) = forward(
        line,
        (query_weight, key_matrix, value_matrix, gate_weight, up_weight, out_weight.T, down_weight.T),
        (attention_gain.reshape(1, rows), feedforward_gain.reshape(1, rows)),
        hidden_in,
        cotangent,
        cosine,
        sine,
        block,
    )
    arrays = (q, k, v, mixed, full, hidden_in, cotangent, middle, grad_n2, gain_rows, cosine, sine, n1, n2, ct, mixed_pair, hidden, gate, up)
    halves = (down_weight.shape[0], gate_weight.shape[1], up_weight.shape[1], out_weight.shape[0], query_weight.shape[1], key_matrix.shape[1], value_matrix.shape[1])
    results = backward(line, 256 if line <= 4 else 128, arrays, halves)
    g_query, g_key, g_value, grad_in, g_out, g_gate, g_up, g_down, hidden_out = finish(list(results[1:9]) + [hidden_out])
    g_gains = results[9]
    return hidden_out, grad_in, g_query, g_key, g_value, g_out.T, g_gate, g_up, g_down.T, g_gains[0, :rows], g_gains[1, :rows]


def solution(mesh):
    split = P(("dp", "tensor"), None)
    row, column, gain = P("dp", "tensor"), P("tensor", "dp"), P("dp")
    return jax.shard_map(
        functools.partial(layer, mesh.shape["dp"], mesh.shape["tensor"]),
        mesh=mesh,
        in_specs=(split, row, row, row, column, row, row, column, gain, gain, split),
        out_specs=(split, split, row, row, row, column, row, row, column, gain, gain),
        check_vma=False,
    )
```

```python
import functools
import math

import jax
import jax.numpy as jnp
import numpy as np
from jax import lax
from jax.experimental import pallas as pl
from jax.experimental.pallas import tpu as pltpu
from jax.sharding import PartitionSpec as P

QUERY_HEADS = 16
KEY_VALUE_HEADS = 8
HEAD_SIZE = 96
SEQUENCE_LENGTH = 512

EPSILON = 1e-05
THETA_BASE = 100000.0
MESH = pl.DeviceIdType.MESH


def place():
    d = lax.axis_index("dp")
    return lax.div(d, 4), lax.rem(lax.div(d, 2), 2), lax.rem(d, 2), lax.axis_index("tensor")


def dev(z, y, x, c):
    return (z * 4 + y * 2 + x, c)


def enter(line, pos):
    z, y, x, c = pos
    barrier = pltpu.get_barrier_semaphore()

    def greet(who):
        pl.semaphore_signal(barrier, inc=1, device_id=who, device_id_type=MESH)

    greet(dev(z, y, x, 1 - c))
    greet(dev(z, y, 1 - x, c))
    greet(dev(z, 1 - y, x, c))

    @pl.when(z > 0)
    def _():
        greet(dev(z - 1, y, x, c))

    @pl.when(z < line - 1)
    def _():
        greet(dev(z + 1, y, x, c))

    pl.semaphore_wait(barrier, 3 + (z > 0).astype(jnp.int32) + (z < line - 1).astype(jnp.int32))


def remote(src, dst, send, recv, who):
    return pltpu.make_async_remote_copy(src_ref=src, dst_ref=dst, send_sem=send, recv_sem=recv, device_id=who, device_id_type=MESH)


class Gather:
    def __init__(self, line, pos, shard, full, width, orders, paired, send, recv):
        self.line, self.pos, self.shard, self.full, self.width = line, pos, shard, full, width
        self.orders, self.paired, self.send, self.recv = orders, paired, send, recv
        self.count = shard.shape[-1] // width
        self.depth = line + 1 + paired

    def columns(self, t, sub):
        return t * self.width + sub[1], sub[2]

    def region(self, t, sub, have, z=None):
        first, part = self.columns(t, sub)
        pz, py, px, c = self.pos
        if self.paired:
            first = first + c * self.shard.shape[-1]
        every = slice(None)
        zi = z if z is not None else (every if "z" in have else pz)
        cols = pl.ds(pl.multiple_of(first, 128), part)
        return self.full.at[zi, every if "y" in have else py, every if "x" in have else px, :, cols]

    def own(self, t, sub):
        first, part = self.columns(t, sub)
        return self.shard.at[:, pl.ds(pl.multiple_of(first, 128), part)]

    def copy(self, t, sub, slot, src, dst, who):
        return remote(src, dst, self.send.at[t, sub[0], slot], self.recv.at[t, sub[0], slot], who)

    def hop(self, t, sub, h, up, have, what):
        z, y, x, c = self.pos
        slot = (h - 1) * 2 + up
        if up:
            block, incoming, who = z - (h - 1), z - h, dev(z + 1, y, x, c)
            there, here = (z + 1 < self.line) & (z >= h - 1), z >= h
        else:
            block, incoming, who = z + (h - 1), z + h, dev(z - 1, y, x, c)
            there, here = (z > 0) & (z + h - 1 < self.line), z + h < self.line

        @pl.when(here if what == "recv" else there)
        def _():
            if what == "recv":
                r = self.region(t, sub, have, incoming)
                self.copy(t, sub, slot, r, r, dev(z, y, x, 1 - c)).wait_recv()
                return
            r = self.region(t, sub, have, block)
            cp = self.copy(t, sub, slot, self.own(t, sub) if h == 1 and not have else r, r, who)
            cp.start() if what == "start" else cp.wait_send()

    def act(self, t, sub, order, i, what):
        z, y, x, c = self.pos
        moves, have = [], ""
        for axis in order:
            moves += [(axis, h, have) for h in (range(1, self.line) if axis == "z" else (0,))]
            have += axis
        if self.paired:
            moves.append(("c", 0, have))
        axis, h, have = moves[i]
        if axis == "z":
            for up in (1, 0):
                self.hop(t, sub, h, up, have, what)
            return
        who = {"y": dev(z, 1 - y, x, c), "x": dev(z, y, 1 - x, c), "c": dev(z, y, x, 1 - c)}[axis]
        land = self.region(t, sub, have)
        cp = self.copy(t, sub, 2 * (self.line - 1) + "yxc".index(axis), land if have else self.own(t, sub), land, who)
        {"start": cp.start, "recv": cp.wait_recv, "sent": cp.wait_send}[what]()

    def each(self, t, fn):
        there = (t >= 0) & (t < self.count)
        for v, orders in enumerate(self.orders):
            turn_of = there if len(self.orders) == 1 else there & (((t == 0) | (t == 2) | (t == 5)) == (v == 1))

            @pl.when(turn_of)
            def _():
                for sub, (order, first, columns) in enumerate(orders):
                    fn((sub, first, columns), order)

    def step(self, t, s):
        def go(sub, order):
            if s > 0:
                self.act(t, sub, order, s - 1, "recv")
            if s < self.depth:
                self.act(t, sub, order, s, "start")

        self.each(t, go)

    def advance(self, p):
        for s in range(self.depth + 1):
            self.step(p - s, s)

    def finish(self):
        @pl.loop(0, self.count)
        def _(t):
            self.each(t, lambda sub, order: [self.act(t, sub, order, i, "sent") for i in range(self.depth)])


def own_copy(g, sem):
    z, y, x, c = g.pos
    first = c * g.shard.shape[-1] if g.paired else 0
    return pltpu.make_async_copy(g.shard, g.full.at[z, y, x, :, pl.ds(pl.multiple_of(first, 128), g.shard.shape[-1])], sem)


def rope_tables(length, width):
    inverse = np.float32(THETA_BASE) ** (-(np.arange(width // 2, dtype=np.float32) * np.float32(2.0 / width)))
    angles = np.arange(length, dtype=np.float32)[:, None] * inverse[None, :]
    cosine, sine = np.cos(angles), np.sin(angles)
    return jnp.asarray(np.concatenate([cosine, cosine], axis=1)), jnp.asarray(np.concatenate([-sine, sine], axis=1))


def turn(x, cosine, sine):
    half = x.shape[-1] // 2
    return x * cosine + jnp.concatenate([x[:, half:], x[:, :half]], axis=1) * sine


def dot_nt(a, b):
    return lax.dot_general(a, b, (((1,), (1,)), ((), ())), preferred_element_type=jnp.float32)


def dot_tn(a, b):
    return lax.dot_general(a, b, (((0,), (0,)), ((), ())), preferred_element_type=jnp.float32)


def dot_nn(a, b):
    return jnp.dot(a, b, preferred_element_type=jnp.float32)


BLOCK = 128


def causal_weights(q, k, b, heads):
    scores = dot_nt(q, k) * (1.0 / math.sqrt(HEAD_SIZE))
    n = scores.shape[1]
    row = lax.broadcasted_iota(jnp.int32, scores.shape, 0) % BLOCK + b * BLOCK
    keep = row >= lax.broadcasted_iota(jnp.int32, scores.shape, 1)
    scores = jnp.where(keep, scores, -jnp.inf)
    log_total = jnp.log(jnp.sum(jnp.exp(scores), axis=1, keepdims=True))
    return jnp.exp(scores - log_total)


def rows_of(ref, first, heads, rows):
    return jnp.concatenate([ref[first + i, rows] for i in range(heads)], axis=0)


ROWS = 128


def each_rows(tokens, step, fn):
    @pl.loop(0, tokens // step)
    def _(r):
        fn(pl.ds(pl.multiple_of(r * step, step), step))


def forward_kernel(line, width, block, *refs):
    refs = list(refs)
    take = lambda n: [refs.pop(0) for _ in range(n)]
    query_in, key_in, value_in, gate_in, up_in, out_in, down_in, gain_a, gain_b, hid, ct, cosine, sine = take(13)
    full, gains_full, q_out, k_out, v_out, mixed_out, n1_pair, n2_pair, ct_pair, mixed_pair, middle_out = take(11)
    tile_pairs = take(3)
    hidden_out, grad_n2, gain = take(3)
    wbuf, gain_buf, n1, n2, flat, qh, kh, vh, mh, mixed, middle, acc, act, tiles, shard, gains, turned = take(17)
    send, recv, gsend, grecv, own_sem, load_sem, gain_sem, local_sem, pair_send, pair_recv, tile_local, tile_send, tile_recv, shard_sem = take(14)

    pos = place()
    z, y, x, c = pos
    tokens, d_model = hid.shape
    half = shard.shape[-1]
    heads, groups = qh.shape[0] // 2, kh.shape[0] // 2
    sibling = dev(z, y, x, 1 - c)
    bf16, f32 = jnp.bfloat16, jnp.float32

    third, half_w = width // 3, width // 2
    mixes = (
        (("zyx", 0, third), ("zxy", third, third), ("xyz", 2 * third, third // 2), ("yxz", 2 * third + third // 2, third // 2)),
        (("zyx", 0, half_w), ("zxy", half_w, half_w)),
    )
    g = Gather(line, pos, shard, full, width, mixes, 1, send, recv)
    gg = Gather(line, pos, gains, gains_full, gains.shape[-1], ((("zyx", 0, gains.shape[-1]),),), 0, gsend, grecv)
    g_own, gg_own = own_copy(g, own_sem.at[0]), own_copy(gg, own_sem.at[1])
    steps = (half // width) - 3
    fills, at = [], 0
    for src in (query_in, key_in, value_in):
        fills.append((src, at, src.shape[1]))
        at += src.shape[1]
    fills.append((out_in, at, out_in.shape[1]))
    at += out_in.shape[1]
    for j in range(steps):
        for i, src in enumerate((gate_in, up_in, down_in)):
            fills.append((src.at[:, pl.ds(j * block, block)], at + j * width + i * block, block))
    fills = [pltpu.make_async_copy(src, shard.at[:, pl.ds(to, n)], shard_sem.at[i]) for i, (src, to, n) in enumerate(fills)]
    for cp in fills:
        cp.start()
    gains[...] = jnp.zeros_like(gains)
    top = lax.broadcasted_iota(jnp.int32, (gains.shape[0], gain_a.shape[1]), 0) == 0
    gains[:, : gain_a.shape[1]] = jnp.where(top, gain_a[...].astype(f32), gain_b[...].astype(f32)).astype(bf16)
    enter(line, pos)
    for cp in fills:
        cp.wait()
    g_own.start()
    gg_own.start()

    def load(t, hh):
        cols = pl.ds(pl.multiple_of(hh * half + t * width, 128), width)
        return pltpu.make_async_copy(full.at[:, :, :, :, cols], wbuf.at[hh], load_sem.at[hh])

    def weight(hh):
        return wbuf[hh].reshape(d_model, width)

    def share(i, own_src, own_dst, other_src, other_dst):
        return pltpu.make_async_copy(own_src, own_dst, local_sem.at[i]), remote(other_src, other_dst, pair_send.at[i], pair_recv.at[i], sibling)

    ends = (pl.ds(0, tokens), pl.ds(tokens, tokens))
    lefts = ((ct, ct_pair), (n1, n1_pair), (n2, n2_pair))
    shares = [share(i, turned.at[i], pair.at[:, ends[0]], turned.at[i], pair.at[:, ends[1]]) for i, (_, pair) in enumerate(lefts)]
    hw = mixed.shape[1] // 2
    side = lambda ref, s, w: ref.at[:, pl.ds(pl.multiple_of(s * w, 128), w)]
    shares.append(share(3, side(mixed, c, hw), mixed_pair.at[0], side(mixed, 1 - c, hw), mixed_pair.at[1]))
    keeps = [pltpu.make_async_copy(src, dst, local_sem.at[4 + i]) for i, (src, dst) in enumerate(((qh, q_out), (kh, k_out), (vh, v_out), (mixed, mixed_out), (middle, middle_out)))]

    def begin(i):
        if i < len(lefts):
            span = 256

            @pl.loop(0, d_model // span)
            def _(e):
                at = pl.ds(pl.multiple_of(e * span, span), span)
                turned[i, at, :] = lefts[i][0][:, at].T

        for cp in shares[i]:
            cp.start()

    def end(i):
        for cp in shares[i]:
            cp.wait()

    def tile_copies(j, hh):
        slot = lax.rem(j, 2)
        cols = pl.ds(pl.multiple_of(j * block, 128), block)
        own = [pltpu.make_async_copy(tiles.at[slot, hh, i], pair.at[0, :, cols], tile_local.at[j, i]) for i, pair in enumerate(tile_pairs)]
        out = [remote(tiles.at[slot, hh, i], pair.at[1, :, cols], tile_send.at[j, i], tile_recv.at[j, i], sibling) for i, pair in enumerate(tile_pairs)]
        return own, out

    def tile_act(j, hh, what):
        @pl.when(hh == c)
        def _():
            for cp in tile_copies(j, hh)[0]:
                cp.start() if what == "start" else cp.wait()

        @pl.when(hh != c)
        def _():
            for cp in tile_copies(j, hh)[1]:
                cp.start() if what == "start" else cp.wait_send()

    def normalize():
        loaded = pltpu.make_async_copy(gains_full, gain_buf, gain_sem)
        loaded.start()
        loaded.wait()
        n = d_model // (gain_buf.shape[0] * 4)
        table = gain_buf[...].astype(f32)
        for i in range(2):
            gain[i : i + 1, :] = jnp.concatenate([table[a, b, e, i : i + 1, :n] for a in range(gain_buf.shape[0]) for b in range(2) for e in range(2)], axis=1)

        def rows_of_norm(rows):
            v = hid[rows, :].astype(f32)
            v = v * lax.rsqrt(jnp.mean(v * v, axis=1, keepdims=True) + EPSILON)
            n1[rows, :] = (v * gain[0:1, :]).astype(bf16)

        each_rows(tokens, ROWS, rows_of_norm)
        begin(1)

    def project(hh, outs):
        flat[...] = dot_nn(n1[...], weight(hh))

        def to_heads(rows):
            cos, sin = cosine[rows, :], sine[rows, :]
            first = 0
            for n, target, turned in outs:
                for h in range(n):
                    v = flat[rows, (first + h) * HEAD_SIZE : (first + h + 1) * HEAD_SIZE]
                    target[hh * n + h, rows] = (turn(v, cos, sin) if turned else v).astype(bf16)
                first += n

        each_rows(tokens, ROWS, to_heads)

    def attend_half(hh):
        per = heads // groups
        blocks = tokens // BLOCK

        @pl.loop(0, groups)
        def _(i):
            kv = hh * groups + i
            for b in range(blocks):
                rows, n = pl.ds(b * BLOCK, BLOCK), (b + 1) * BLOCK
                w = causal_weights(rows_of(qh, kv * per, per, rows), kh[kv, :n], b, per).astype(bf16)
                m = dot_nn(w, vh[kv, :n]).astype(bf16)
                for e in range(per):
                    mh[kv * per + e, rows] = m[e * BLOCK : (e + 1) * BLOCK]

        lanes = pl.ds(pl.multiple_of(hh * hw, 128), hw)

        def join(rows):
            mixed[rows, lanes] = jnp.concatenate([mh[hh * heads + h, rows] for h in range(heads)], axis=1)

        each_rows(tokens, ROWS, join)

    def leave_attention(hh):
        part = dot_nt(mixed[:, pl.ds(pl.multiple_of(hh * hw, 128), hw)], weight(hh))

        @pl.when(hh == c)
        def _():
            middle[...] = hid[...].astype(f32) + part

        @pl.when(hh != c)
        def _():
            middle[...] += part
            begin(3)
            for cp in keeps:
                cp.start()

            def rows_of_norm(rows):
                v = middle[rows, :]
                acc[rows, :] = v
                v = v * lax.rsqrt(jnp.mean(v * v, axis=1, keepdims=True) + EPSILON)
                n2[rows, :] = (v * gain[1:2, :]).astype(bf16)
                grad_n2[rows, :] = jnp.zeros_like(v)

            each_rows(tokens, ROWS, rows_of_norm)
            begin(2)

    def feed_forward(j, hh):
        @pl.when(j >= 2)
        def _():
            tile_act(j - 2, hh, "wait")

        part = lax.rem(j, 2)
        act[0] = dot_nn(n2[...], weight(hh)[:, :block])
        act[1] = dot_nn(n2[...], weight(hh)[:, block : 2 * block])
        act[2] = dot_nn(ct[...], weight(hh)[:, 2 * block :])

        def gated(rows):
            gate, up, grad = act[0, rows], act[1, rows], act[2, rows]
            sigma = jax.nn.sigmoid(gate)
            tiles[part, hh, 0, rows] = (gate * sigma * up).astype(bf16)
            tiles[part, hh, 1, rows] = (grad * up * sigma * (1.0 + gate * (1.0 - sigma))).astype(bf16)
            tiles[part, hh, 2, rows] = (grad * gate * sigma).astype(bf16)

        each_rows(tokens, ROWS // 2, gated)
        tile_act(j, hh, "start")
        acc[...] += dot_nt(tiles[part, hh, 0], weight(hh)[:, 2 * block :])
        both = jnp.concatenate([tiles[part, hh, 1], tiles[part, hh, 2]], axis=1)
        grad_n2[...] += dot_nt(both, weight(hh)[:, : 2 * block])

    count = g.count

    @pl.loop(0, count + g.depth)
    def _(p):
        gg.advance(p)
        g.advance(p)

        @pl.when(p == 0)
        def _():
            g_own.wait()
            gg_own.wait()

        @pl.when(p == 1)
        def _():
            begin(0)

        chunk_of = lambda hh: jnp.where(hh == c, p - g.depth + 1, p - g.depth)
        for hh in range(2):
            u = chunk_of(hh)

            @pl.when((u >= 0) & (u < count))
            def _():
                load(u, hh).start()

        @pl.loop(0, 2)
        def _(i):
            hh = jnp.where(i == 0, 1 - c, c)
            u = chunk_of(hh)

            @pl.when((u >= 0) & (u < count))
            def _():
                load(u, hh).wait()

                @pl.when((u == 0) & (hh == c))
                def _():
                    normalize()

                @pl.when(u == 0)
                def _():
                    project(hh, ((heads, qh, True),))

                @pl.when(u == 1)
                def _():
                    project(hh, ((groups, kh, True), (groups, vh, False)))
                    attend_half(hh)

                @pl.when(u == 2)
                def _():
                    leave_attention(hh)

                @pl.when(u >= 3)
                def _():
                    feed_forward(u - 3, hh)

    def rows_out(rows):
        hidden_out[rows, :] = acc[rows, :].astype(bf16)

    each_rows(tokens, ROWS, rows_out)
    for i in range(len(shares)):
        end(i)
    for cp in keeps:
        cp.wait()
    for j in range(max(steps - 2, 0), steps):
        for hh in range(2):
            tile_act(j, hh, "wait")

    @pl.loop(0, steps)
    def _(j):
        for cp in tile_copies(j, 0)[1]:
            cp.wait_recv()

    g.finish()
    gg.finish()


def forward(line, shards, gain_pair, hidden_in, cotangent, cosine, sine, block):
    tokens, d_model = hidden_in.shape
    rows = gain_pair[0].shape[1]
    half = sum(s.shape[1] for s in shards)
    gains = jax.ShapeDtypeStruct((8, 128), jnp.bfloat16)
    width = 3 * block
    count = half // width
    steps = count - 3
    heads, groups = QUERY_HEADS // 2, KEY_VALUE_HEADS // 2
    bf16, f32 = jnp.bfloat16, jnp.float32
    struct = jax.ShapeDtypeStruct
    hbm, vmem = pl.BlockSpec(memory_space=pl.ANY), pl.BlockSpec(memory_space=pltpu.VMEM)
    dma = pltpu.SemaphoreType.DMA
    pair = struct((d_model, 2 * tokens), bf16)
    tile_pair = struct((2, tokens, steps * block), bf16)
    head_shape = lambda n: (n, tokens, HEAD_SIZE)
    slots = 2 * (line - 1) + 3
    outs = [
        struct((line, 2, 2, rows, 2 * half), bf16),
        struct((line, 2, 2) + gains.shape, bf16),
        struct(head_shape(2 * heads), bf16),
        struct(head_shape(2 * groups), bf16),
        struct(head_shape(2 * groups), bf16),
        struct((tokens, 2 * heads * HEAD_SIZE), bf16),
        pair,
        pair,
        pair,
        struct((2, tokens, heads * HEAD_SIZE), bf16),
        struct((tokens, d_model), f32),
        tile_pair,
        tile_pair,
        tile_pair,
        struct((tokens, d_model), bf16),
        struct((tokens, d_model), f32),
        struct((8, d_model), f32),
    ]
    V = pltpu.VMEM
    return pl.pallas_call(
        functools.partial(forward_kernel, line, width, block),
        out_shape=outs,
        in_specs=[hbm] * 7 + [vmem] * 6,
        out_specs=[hbm] * 14 + [vmem] * 3,
        scratch_shapes=[
            V((2, line, 2, 2, rows, width), bf16),
            V((line, 2, 2) + gains.shape, bf16),
            V((tokens, d_model), bf16),
            V((tokens, d_model), bf16),
            V((tokens, width), f32),
            V(head_shape(2 * heads), bf16),
            V(head_shape(2 * groups), bf16),
            V(head_shape(2 * groups), bf16),
            V(head_shape(2 * heads), bf16),
            V((tokens, 2 * heads * HEAD_SIZE), bf16),
            V((tokens, d_model), f32),
            V((tokens, d_model), f32),
            V((3, tokens, block), f32),
            V((2, 2, 3, tokens, block), bf16),
            V((rows, half), bf16),
            V(gains.shape, bf16),
            V((3, d_model, tokens), bf16),
            dma((count, 4, slots)),
            dma((count, 4, slots)),
            dma((1, 1, slots)),
            dma((1, 1, slots)),
            dma((2,)),
            dma((2,)),
            dma,
            dma((9,)),
            dma((4,)),
            dma((4,)),
            dma((steps, 3)),
            dma((steps, 3)),
            dma((steps, 3)),
            dma((4 + 3 * steps,)),
        ],
        compiler_params=pltpu.CompilerParams(collective_id=0, has_side_effects=True, vmem_limit_bytes=64 * 2**20 - 2**17),
        name="gather_forward",
    )(*shards, *gain_pair, hidden_in, cotangent, cosine, sine)


class Scatter:
    def __init__(self, line, pos, count, plain, early, final):
        self.line, self.pos, self.count, self.final = line, pos, count, final
        self.own, self.first, self.second, self.up, self.down, self.send, self.recv = plain
        self.early = early
        self.lags = [0, 2, 4, 5, 4 + line, 5 + line]
        self.depth = self.lags[-1]

    def is_early(self, t):
        return lax.rem(t + 5, 5) == 4

    def plain_number(self, t):
        return t - lax.div(t, 5)

    def parts(self, t, early):
        if early:
            i, (own, first, second, up, down, send, recv) = lax.div(t, 5), self.early
        else:
            i, own, first, second, up, down, send, recv = self.plain_number(t), self.own, self.first, self.second, self.up, self.down, self.send, self.recv
        o, r = lax.rem(i, own.shape[0]), lax.rem(i, first.shape[0])
        return own.at[o], first.at[r], second.at[r], up.at[r], down.at[r], send.at[r], recv.at[r]

    def place_of(self, t, early):
        return self.parts(t, early)[0]

    def merge(self, dst, a, b, loops):
        def go(lead, rest):
            if not rest:
                dst[lead] = a[lead] + b[lead]
            elif rest[0] > 2:
                @pl.loop(0, rest[0])
                def _(i):
                    go(lead + (i,), rest[1:])
            else:
                for i in range(rest[0]):
                    go(lead + (i,), rest[1:])

        go((), loops)

    def pair_moves(self, t, v):
        z, y, x, c = self.pos
        early = v >= 2
        own, first, second, _, _, send, recv = self.parts(t, early)
        over_x, over_y = dev(z, y, 1 - x, c), dev(z, 1 - y, x, c)
        lead = (z,) if early else (slice(None),)
        if v % 2 == 0:
            give, keep, who = own.at[lead + (slice(None), 1 - x)], own.at[lead + (slice(None), x)], (over_x, over_y)
        else:
            give, keep, who = own.at[lead + (1 - y,)], own.at[lead + (y,)], (over_y, over_x)
        a, b = (1 - y, y) if v % 2 == 0 else (1 - x, x)
        lead = () if early else (slice(None),)
        one = remote(give, first, send.at[0], recv.at[0], who[0])
        two = remote(first.at[lead + (a,)], second, send.at[1], recv.at[1], who[1])
        return one, two, keep, first, second, first.at[lead + (b,)]

    def hop(self, p, j, way, early):
        z, y, x, c = self.pos
        last = self.line - 1
        travelled = z if way == 0 else last - z
        t = p - (0 if early else self.lags[3]) - j - travelled
        target = last - j if way == 0 else j
        passes = (target > z) if way == 0 else (target < z)

        def go():
            own, _, second, up, down, send, recv = self.parts(t, early)
            cur, ref = own if early else second, (up if way == 0 else down).at[j]
            nxt = dev(z + 1, y, x, c) if way == 0 else dev(z - 1, y, x, c)
            slot = 2 + 2 * j + way

            @pl.when(travelled == 0)
            def _():
                remote(cur.at[target], ref, send.at[slot], recv.at[slot], nxt).start()

            @pl.when(travelled > 0)
            def _():
                cp = remote(ref, ref, send.at[slot], recv.at[slot], nxt)
                cp.wait_recv()
                self.merge(ref, ref, cur.at[target], (2, 2) if early else ())
                cp.start()

        @pl.when(passes & (t >= 0) & (t < self.count) & (self.is_early(t) == early))
        def _():
            go()

    def arrive(self, t, early):
        z, y, x, c = self.pos
        _, _, _, up, down, send, recv = self.parts(t, early)
        last = self.line - 1
        ends = []
        for way, ref, has, k in ((0, up, z > 0, last - z), (1, down, z < last, z)):

            @pl.when(has)
            def _():
                slot = 2 + 2 * k + way
                remote(ref.at[k], ref.at[k], send.at[slot], recv.at[slot], dev(z, y, x, 1 - c)).wait_recv()

            ends.append((has, ref.at[jnp.minimum(k, last - 1)]))
        return ends

    def close(self, t):
        f32 = jnp.float32
        total = self.parts(t, False)[2][self.pos[0]].astype(f32)
        for has, ref in self.arrive(t, False):
            total = total + jnp.where(has, ref[...].astype(f32), 0.0)
        self.final(t, total)

    def close_early(self, t, v):
        z = self.pos[0]
        mine = self.place_of(t, True).at[z]
        ends = self.arrive(t, True)
        for i in range(2):
            for k in range(2):
                total = mine[i, k].astype(jnp.float32)
                for has, ref in ends:
                    total = total + jnp.where(has, ref[i, k].astype(jnp.float32), 0.0)
                mine[i, k] = total.astype(mine.dtype)
        self.pair_moves(t, v)[0].start()

    def drain(self, t, early):
        z, y, x, c = self.pos
        _, _, _, up, down, send, recv = self.parts(t, early)
        if early:
            self.pair_moves(t, 2)[0].wait_send()
        self.pair_moves(t, 2 * early)[1].wait_send()
        for j in range(self.line - 1):
            for way, ref, target in ((0, up, self.line - 1 - j), (1, down, j)):

                @pl.when((target > z) if way == 0 else (target < z))
                def _():
                    slot = 2 + 2 * j + way
                    remote(ref.at[j], ref.at[j], send.at[slot], recv.at[slot], dev(z, y, x, 1 - c)).wait_send()

    def plain(self, t, fn):
        @pl.when((t >= 0) & (t < self.count) & ~self.is_early(t))
        def _():
            fn()

    def sorts(self, t, fn, early):
        number = lax.div(t, 5) if early else self.plain_number(t)
        for v in range(2):
            @pl.when((t >= 0) & (t < self.count) & (self.is_early(t) == early) & (lax.rem(number + 2, 2) == v))
            def _():
                fn(v + 2 * early)

    def begin(self, t):
        self.sorts(t, lambda v: self.pair_moves(t, v)[0].start(), False)

    def release(self, p):
        t = p - self.own.shape[0] * 5 // 4
        self.plain(t, lambda: self.pair_moves(t, 0)[0].wait_send())

    def advance(self, p):
        line = self.line

        def one(t, v):
            first_copy, second_copy, keep, first, second, _ = self.pair_moves(t, v)
            first_copy.wait_recv()
            self.merge(first, first, keep, (2,) if v >= 2 else (line, 2))
            second_copy.start()

        def two(t, v):
            _, second_copy, _, _, second, keep = self.pair_moves(t, v)
            second_copy.wait_recv()
            if v >= 2:
                self.final(t, keep[...].astype(jnp.float32) + second[...].astype(jnp.float32))
            else:
                self.merge(second, second, keep, (line,))

        for j in range(line - 1):
            for way in range(2):
                self.hop(p, j, way, True)
        for step, lag, early in ((one, self.lags[1], False), (two, self.lags[2], False), (self.close_early, line, True), (one, line + 2, True), (two, line + 4, True)):
            t = p - lag
            self.sorts(t, lambda v, t=t, step=step: step(t, v), early)
        for j in range(line - 1):
            for way in range(2):
                self.hop(p, j, way, False)
        t = p - self.lags[-2]
        self.plain(t, lambda t=t: self.close(t))
        t = p - self.lags[-1]
        self.plain(t, lambda t=t: self.drain(t, False))

        @pl.when((t >= 0) & (t < self.count) & self.is_early(t))
        def _():
            self.drain(t, True)


def greet_all(n, pos):
    z, y, x, c = pos
    d = z * 4 + y * 2 + x
    barrier = pltpu.get_barrier_semaphore()

    @pl.loop(1, n)
    def _(i):
        pl.semaphore_signal(barrier, inc=1, device_id=(lax.rem(d + i, n), c), device_id_type=MESH)

    pl.semaphore_signal(barrier, inc=1, device_id=(d, 1 - c), device_id_type=MESH)
    pl.semaphore_wait(barrier, n)


def backward_kernel(line, cols, starts, *refs):
    refs = list(refs)
    take = lambda n: [refs.pop(0) for _ in range(n)]
    q, k, v, mixed, full, hid, ct, middle, grad_n2, gains, cosine, sine = take(12)
    n1_pair, n2_pair, ct_pair, mixed_pair, hidden_pair, gate_pair, up_pair = take(7)
    qkv_pair, grad_query, grad_key, grad_value, grad_in_out, out_out, out_gate, out_up, out_down, out_gains, gm_pair = take(11)
    own, first, second, up, down, xt, ybuf, qh, kh, vh, mh, gh, gm, dots, dq, dk, dv, dqkv, wbuf, gmid, hbuf, out_qkv, gain_one, part, parts_in, pair_in, gain_two, gmb, turned, own_e, first_e, second_e, up_e, down_e, grad_in = take(35)
    send, recv, xsem, ysem, half_sem, wsem, msem, qkv_local, qkv_send, qkv_recv, part_send, part_recv, out_sem, swap_sem, gm_sem, send_e, recv_e = take(17)

    pos = place()
    z, y, x, c = pos
    d = z * 4 + y * 2 + x
    n = line * 4
    tokens, d_model = hid.shape
    count = starts[-1]
    heads, groups = qh.shape[0], kh.shape[0]
    share = heads // groups
    blocks = tokens // BLOCK
    width = wbuf.shape[-1]
    half_width = dqkv.shape[1] // 2
    scale = 1.0 / math.sqrt(HEAD_SIZE)
    bf16, f32 = jnp.bfloat16, jnp.float32
    sources = (hidden_pair, gate_pair, up_pair, mixed_pair, qkv_pair)
    lefts = ((0, ct_pair), (starts[1], n2_pair), (starts[3], gm_pair), (starts[4], n1_pair))

    def final(t, total):
        for i, out in enumerate((out_down, out_gate, out_up, out_out, out_qkv)):
            at = pl.ds(pl.multiple_of((t - starts[i]) * cols, 128), cols)

            @pl.when((t >= starts[i]) & (t < starts[i + 1]))
            def _():
                out[:, at] = total

    s = Scatter(line, pos, count, (own, first, second, up, down, send, recv), (own_e, first_e, second_e, up_e, down_e, send_e, recv_e), final)

    def load_left(i):
        return pltpu.make_async_copy(lefts[i][1], xt.at[i % 2], xsem.at[i % 2])

    def load_right(t, act):
        slot = lax.rem(t, 2)
        for i, src in enumerate(sources):
            at = pl.ds(pl.multiple_of((t - starts[i]) * cols, 128), cols)

            @pl.when((t >= starts[i]) & (t < starts[i + 1]))
            def _():
                cp = pltpu.make_async_copy(src.at[:, :, at], ybuf.at[slot], ysem.at[slot])
                cp.start() if act == "start" else cp.wait()

    def half_loads(hh):
        take_heads = lambda ref, m: ref.at[pl.ds(hh * m, m)]
        lanes = pl.ds(pl.multiple_of(hh * mh.shape[1], 128), mh.shape[1])
        pairs = ((take_heads(q, heads), qh), (take_heads(k, groups), kh), (take_heads(v, groups), vh), (mixed.at[:, lanes], mh))
        return [pltpu.make_async_copy(src, dst, half_sem.at[i]) for i, (src, dst) in enumerate(pairs)]

    def half_load(hh, act):
        for cp in half_loads(hh):
            cp.start() if act == "start" else cp.wait()

    each = half_width // width
    half_columns = full.shape[-1] // 2

    def weights(i):
        at = (i * half_columns + each * width) if i < 2 else ((i - 2) // each * half_columns + (i - 2) % each * width)
        return pltpu.make_async_copy(full.at[:, :, :, :, pl.ds(at, width)], wbuf.at[i % 2], wsem.at[i % 2])

    def weight(i):
        return wbuf[i % 2].reshape(d_model, width)

    middle_in = pltpu.make_async_copy(middle, grad_in, msem.at[0])
    grad_n2_in = pltpu.make_async_copy(grad_n2, gmid, msem.at[1])
    ct_in, hid_in = (pltpu.make_async_copy(src, hbuf, msem.at[2]) for src in (ct, hid))

    own_half = lambda ref, which: ref.at[:, pl.ds(pl.multiple_of(which * half_width, 128), half_width)]

    def qkv_copies():
        return (
            pltpu.make_async_copy(own_half(dqkv, c), qkv_pair.at[0], qkv_local),
            remote(own_half(dqkv, 1 - c), qkv_pair.at[1], qkv_send, qkv_recv, (d, 1 - c)),
        )

    def gm_copies():
        return (
            pltpu.make_async_copy(turned, gm_pair.at[:, pl.ds(0, tokens)], gm_sem.at[0]),
            remote(turned, gm_pair.at[:, pl.ds(tokens, tokens)], gm_sem.at[1], gm_sem.at[2], (d, 1 - c)),
        )

    def norm_two_back():
        for cp in (middle_in, grad_n2_in, ct_in):
            cp.wait()
        gain_two[...] = jnp.zeros_like(gain_two)

        def rows_back(rows):
            a, grad = grad_in[rows, :], gmid[rows, :]
            inverse = lax.rsqrt(jnp.mean(a * a, axis=1, keepdims=True) + EPSILON)
            unit = a * inverse
            scaled = grad * gains[1:2, :]
            inner = jnp.mean(scaled * unit, axis=1, keepdims=True)
            total = hbuf[rows, :].astype(f32) + inverse * (scaled - unit * inner)
            gmid[rows, :] = total
            gmb[rows, :] = total.astype(bf16)
            gain_two[...] += jnp.sum(grad * unit, axis=0, keepdims=True)

        each_rows(tokens, ROWS, rows_back)
        hid_in.start()
        span = 256

        @pl.loop(0, d_model // span)
        def _(e):
            at = pl.ds(pl.multiple_of(e * span, span), span)
            turned[at, :] = gmb[:, at].T

        for cp in gm_copies():
            cp.start()

    def through_out(i):
        weights(i).wait()
        gh[...] = dot_nn(gmb[...], weight(i))
        weights(i + 2).start()

    def prepare(hh):
        half_load(hh, "wait")

        def rows_of_dots(rows):
            for h in range(heads):
                lanes = slice(h * HEAD_SIZE, (h + 1) * HEAD_SIZE)
                g = gh[rows, lanes]
                dots[h, rows] = jnp.sum(g * mh[rows, lanes].astype(f32), axis=1, keepdims=True)
                gm[h, rows] = g.astype(bf16)

        each_rows(tokens, ROWS, rows_of_dots)
        dk[...] = jnp.zeros_like(dk)
        dv[...] = jnp.zeros_like(dv)

    def group_back(g, which):
        for b in which:
            rows, m = pl.ds(b * BLOCK, BLOCK), (b + 1) * BLOCK
            qb, gb, db = (rows_of(ref, g * share, share, rows) for ref in (qh, gm, dots))
            kb, vb = kh[g, :m], vh[g, :m]
            p = causal_weights(qb, kb, b, share)
            ds = (p * (dot_nt(gb, vb) - db)).astype(bf16)
            dv[g, :m] += dot_tn(p.astype(bf16), gb)
            dk[g, :m] += dot_tn(ds, qb)
            r = dot_nn(ds, kb) * scale
            for i in range(share):
                dq[g * share + i, rows] = r[i * BLOCK : (i + 1) * BLOCK]

    def join(hh):
        def rows_of_join(rows):
            cos, sin = cosine[rows, :], -sine[rows, :]
            parts = [turn(dq[h, rows], cos, sin) for h in range(heads)]
            parts += [turn(dk[g, rows] * scale, cos, sin) for g in range(groups)]
            parts += [dv[g, rows] for g in range(groups)]
            dqkv[rows, pl.ds(pl.multiple_of(hh * half_width, 128), half_width)] = jnp.concatenate([a.astype(bf16) for a in parts], axis=1)

        each_rows(tokens, ROWS, rows_of_join)

    def against(i):
        weights(i + 2).wait()
        r = dot_nt(dqkv[:, i * width : (i + 1) * width], weight(i))
        if i == 0:
            grad_in[...] = r
        else:
            grad_in[...] += r
        if i + 2 < 2 * each:
            weights(i + 4).start()

    def norm_one_back():
        hid_in.wait()
        gain_one[...] = jnp.zeros_like(gain_one)

        def rows_back(rows):
            a = hbuf[rows, :].astype(f32)
            inverse = lax.rsqrt(jnp.mean(a * a, axis=1, keepdims=True) + EPSILON)
            unit, grad = a * inverse, grad_in[rows, :]
            scaled = grad * gains[0:1, :]
            inner = jnp.mean(scaled * unit, axis=1, keepdims=True)
            grad_in[rows, :] = gmid[rows, :] + inverse * (scaled - unit * inner)
            gain_one[...] += jnp.sum(grad * unit, axis=0, keepdims=True)

        each_rows(tokens, ROWS, rows_back)
        size = d_model // n
        part[...] = jnp.zeros_like(part)
        for i in range(n):
            for row, ref in enumerate((gain_one, gain_two)):
                part[i, row : row + 1, :size] = ref[:, i * size : (i + 1) * size]

    def part_copy(i):
        to = lax.rem(d + i, n)
        return remote(part.at[to], parts_in.at[i], part_send.at[i], part_recv.at[i], (to, c))

    load_left(0).start()
    load_left(1).start()
    load_right(0, "start")
    half_load(0, "start")
    for cp in (middle_in, grad_n2_in, ct_in):
        cp.start()
    for i in range(2):
        weights(i).start()
    greet_all(n, pos)

    swap = remote(out_gains, pair_in, swap_sem.at[0], swap_sem.at[1], (d, 1 - c))
    grad_in_copy = pltpu.make_async_copy(grad_in, grad_in_out, out_sem.at[3])
    stages = 2 * groups + 3
    chain = 1
    turns = chain + 2 * stages
    norm_at = turns + 2 * each

    @pl.loop(0, count + s.depth)
    def _(p):
        s.release(p)
        for i, (at, _) in enumerate(lefts):

            @pl.when(p == at)
            def _():
                load_left(i).wait()
                if 1 <= i < len(lefts) - 1:
                    load_left(i + 1).start()

        @pl.when(p == starts[1] - 1)
        def _():
            for cp in gm_copies():
                cp.wait()

        @pl.when(p == starts[4] - 2)
        def _():
            for cp in qkv_copies():
                cp.wait()

        @pl.when(p < count)
        def _():
            load_right(p, "wait")

            @pl.when(p + 1 < count)
            def _():
                load_right(p + 1, "start")

            side = lax.rem(sum((p >= at).astype(jnp.int32) for at, _ in lefts[1:]), 2)
            right = ybuf[lax.rem(p, 2)].reshape(2 * tokens, cols)
            for early in (False, True):

                @pl.when(s.is_early(p) == early)
                def _():
                    s.place_of(p, early)[...] = dot_nn(xt[side], right).reshape(own.shape[1:]).astype(bf16)

            s.begin(p)

        s.advance(p)

        @pl.when(p == chain - 1)
        def _():
            norm_two_back()

        for i in range(2):

            @pl.when(p == chain + i * stages)
            def _():
                through_out(i)

        @pl.when((p >= chain) & (p < turns))
        def _():
            hh, r = lax.div(p - chain, stages), lax.rem(p - chain, stages) - 1

            @pl.when(r == 0)
            def _():
                prepare(hh)

            for e, which in enumerate((range(blocks - 1), range(blocks - 1, blocks))):

                @pl.when((r > 0) & (r <= 2 * groups) & (lax.rem(r + 1, 2) == e))
                def _():
                    group_back(lax.div(r - 1, 2), which)

            @pl.when(r == stages - 2)
            def _():
                join(hh)

                @pl.when(hh == 0)
                def _():
                    half_load(1, "start")

                @pl.when(hh == 1)
                def _():
                    for cp in qkv_copies():
                        cp.start()

        for i in range(2 * each):

            @pl.when(p == turns + i)
            def _():
                against(i)

        @pl.when(p == norm_at)
        def _():
            norm_one_back()

        @pl.when(p == norm_at + 1)
        def _():
            grad_in_copy.start()

            @pl.loop(1, n)
            def _(i):
                part_copy(i).start()

        @pl.when(p == count + s.depth - 2)
        def _():
            @pl.loop(1, n)
            def _(i):
                part_copy(i).wait()

            out_gains[...] = part[d] + jnp.sum(parts_in[1:], axis=0)
            swap.start()

    ends, first_column = [grad_in_copy], 0
    for i, out in enumerate((grad_query, grad_key, grad_value)):
        cp = pltpu.make_async_copy(out_qkv.at[:, pl.ds(first_column, out.shape[1])], out, out_sem.at[i])
        cp.start()
        ends.append(cp)
        first_column += out.shape[1]
    swap.wait()
    out_gains[...] += pair_in[...]
    for cp in ends:
        cp.wait()


def backward(line, cols, arrays, halves):
    q, k, v, mixed, full, hid = arrays[:6]
    tokens, d_model = hid.shape
    rows = full.shape[3]
    n = line * 4
    down_w, gate_w, up_w, out_w, q_w, k_w, v_w = halves
    qkv_w = q_w + k_w + v_w
    starts = [0]
    for w in (down_w, gate_w, up_w, out_w, qkv_w):
        starts.append(starts[-1] + w // cols)
    heads, groups = q.shape[0] // 2, k.shape[0] // 2
    width = q_w
    bf16, f32 = jnp.bfloat16, jnp.float32
    struct, V, dma = jax.ShapeDtypeStruct, pltpu.VMEM, pltpu.SemaphoreType.DMA
    hbm, vmem = pl.BlockSpec(memory_space=pl.ANY), pl.BlockSpec(memory_space=pltpu.VMEM)
    ring, own_ring = (line + 12) * 4 // 5 + 1, 4
    ring_e, own_ring_e = (line + 16) // 5, (line + 5) // 5 + 1
    head = lambda m: (m, tokens, HEAD_SIZE)
    sems = 2 + 2 * (line - 1)
    outs = [struct((2, tokens, qkv_w), bf16)]
    outs += [struct((rows, w), f32) for w in (q_w, k_w, v_w)]
    outs += [struct((tokens, d_model), f32), struct((rows, out_w), f32), struct((rows, gate_w), f32), struct((rows, up_w), f32), struct((rows, down_w), f32), struct((8, 128), f32)]
    outs += [struct((d_model, 2 * tokens), bf16)]
    return pl.pallas_call(
        functools.partial(backward_kernel, line, cols, tuple(starts)),
        out_shape=outs,
        in_specs=[hbm] * 9 + [vmem] * 3 + [hbm] * 7,
        out_specs=[hbm] * 5 + [vmem] * 5 + [hbm],
        scratch_shapes=[
            V((own_ring, line, 2, 2, rows, cols), bf16),
            V((ring, line, 2, rows, cols), bf16),
            V((ring, line, rows, cols), bf16),
            V((ring, line - 1, rows, cols), bf16),
            V((ring, line - 1, rows, cols), bf16),
            V((2, d_model, 2 * tokens), bf16),
            V((2, 2, tokens, cols), bf16),
            V(head(heads), bf16),
            V(head(groups), bf16),
            V(head(groups), bf16),
            V((tokens, heads * HEAD_SIZE), bf16),
            V((tokens, heads * HEAD_SIZE), f32),
            V(head(heads), bf16),
            V((heads, tokens, 1), f32),
            V(head(heads), f32),
            V(head(groups), f32),
            V(head(groups), f32),
            V((tokens, 2 * qkv_w), bf16),
            V((2, line, 2, 2, rows, width), bf16),
            V((tokens, d_model), f32),
            V((tokens, d_model), bf16),
            V((rows, qkv_w), f32),
            V((1, d_model), f32),
            V((n, 8, 128), f32),
            V((n, 8, 128), f32),
            V((8, 128), f32),
            V((1, d_model), f32),
            V((tokens, d_model), bf16),
            V((d_model, tokens), bf16),
            V((own_ring_e, line, 2, 2, rows, cols), bf16),
            V((ring_e, 2, rows, cols), bf16),
            V((ring_e, rows, cols), bf16),
            V((ring_e, line - 1, 2, 2, rows, cols), bf16),
            V((ring_e, line - 1, 2, 2, rows, cols), bf16),
            V((tokens, d_model), f32),
            dma((ring, sems)),
            dma((ring, sems)),
            dma((2,)),
            dma((2,)),
            dma((4,)),
            dma((2,)),
            dma((3,)),
            dma,
            dma,
            dma,
            dma((n,)),
            dma((n,)),
            dma((4,)),
            dma((2,)),
            dma((3,)),
            dma((ring_e, sems)),
            dma((ring_e, sems)),
        ],
        compiler_params=pltpu.CompilerParams(collective_id=1, has_side_effects=True, vmem_limit_bytes=64 * 2**20 - 2**17),
        name="backward_scatter",
    )(*arrays)


def finish_kernel(n, *refs):
    srcs, gains, outs, gain_outs, bufs, (loads, stores) = refs[:n], refs[n], refs[n + 1 : 2 * n + 1], refs[2 * n + 1 : 2 * n + 3], refs[2 * n + 3 : 3 * n + 3], refs[3 * n + 3 :]
    for i in range(n):
        pltpu.make_async_copy(srcs[i], bufs[i], loads.at[i]).start()
    for row, out in enumerate(gain_outs):
        out[...] = gains[row : row + 1, : out.shape[1]]
    for i in range(n):
        pltpu.make_async_copy(srcs[i], bufs[i], loads.at[i]).wait()
        pltpu.make_async_copy(bufs[i], outs[i], stores.at[i]).start()
    for i in range(n):
        pltpu.make_async_copy(bufs[i], outs[i], stores.at[i]).wait()


def finish(arrays, gains, rows):
    n = len(arrays)
    hbm, vmem = pl.BlockSpec(memory_space=pl.ANY), pl.BlockSpec(memory_space=pltpu.VMEM)
    return pl.pallas_call(
        functools.partial(finish_kernel, n),
        out_shape=[jax.ShapeDtypeStruct(a.shape, a.dtype) for a in arrays] + [jax.ShapeDtypeStruct((1, rows), gains.dtype)] * 2,
        in_specs=[hbm] * n + [vmem],
        out_specs=[hbm] * n + [vmem] * 2,
        scratch_shapes=[pltpu.VMEM(a.shape, a.dtype) for a in arrays] + [pltpu.SemaphoreType.DMA((n,)), pltpu.SemaphoreType.DMA((n,))],
        compiler_params=pltpu.CompilerParams(vmem_limit_bytes=64 * 2**20 - 2**17),
        name="finish",
    )(*arrays, gains)


def layer(n_dp, n_tensor, hidden_in, query_weight, key_matrix, value_matrix, out_weight, gate_weight, up_weight, down_weight, attention_gain, feedforward_gain, cotangent):
    line = n_dp // 4
    rows = attention_gain.shape[0]
    block = (query_weight.shape[1] // 3) & -128
    cosine, sine = rope_tables(SEQUENCE_LENGTH, HEAD_SIZE)
    (full, _, q, k, v, mixed, n1, n2, ct, mixed_pair, middle, hidden, gate, up, hidden_out, grad_n2, gain_rows) = forward(
        line,
        (query_weight, key_matrix, value_matrix, gate_weight, up_weight, out_weight.T, down_weight.T),
        (attention_gain.reshape(1, rows), feedforward_gain.reshape(1, rows)),
        hidden_in,
        cotangent,
        cosine,
        sine,
        block,
    )
    arrays = (q, k, v, mixed, full, hidden_in, cotangent, middle, grad_n2, gain_rows, cosine, sine, n1, n2, ct, mixed_pair, hidden, gate, up)
    halves = (down_weight.shape[0], gate_weight.shape[1], up_weight.shape[1], out_weight.shape[0], query_weight.shape[1], key_matrix.shape[1], value_matrix.shape[1])
    results = backward(line, 256 if line <= 4 else 128, arrays, halves)
    g_query, g_key, g_value, grad_in, g_out, g_gate, g_up, g_down, hidden_out, first_gain, second_gain = finish(list(results[1:9]) + [hidden_out], results[9], rows)
    return hidden_out, grad_in, g_query, g_key, g_value, g_out.T, g_gate, g_up, g_down.T, first_gain.reshape(rows), second_gain.reshape(rows)


def solution(mesh):
    split = P(("dp", "tensor"), None)
    row, column, gain = P("dp", "tensor"), P("tensor", "dp"), P("dp")
    return jax.shard_map(
        functools.partial(layer, mesh.shape["dp"], mesh.shape["tensor"]),
        mesh=mesh,
        in_specs=(split, row, row, row, column, row, row, column, gain, gain, split),
        out_specs=(split, split, row, row, row, column, row, row, column, gain, gain),
        check_vma=False,
    )
```
